16 devices in a mesh: stage: 2 (over z), expert: 8 (over y, x, core).
Axes of the slice: x: 2, y: 2, z: 2, core: 2. Of those that a mesh axis runs over, the one named last changes fastest.
Arguments:
- x_acts: bfloat16 [2, 2, 8192, 640], P(None, 'stage', 'expert')
- expert_ids: int32 [2, 2, 8192, 4], P(None, 'stage', 'expert')
- gate_wts: float32 [2, 2, 8192, 4], P(None, 'stage', 'expert')
- w_in: bfloat16 [2, 32, 640, 640], P('stage', 'expert')
- w_up: bfloat16 [2, 32, 640, 640], P('stage', 'expert')
- w_out: bfloat16 [2, 32, 640, 640], P('stage', 'expert')
- d_out: bfloat16 [2, 8192, 640], P('stage', 'expert')
Outputs:
- output 1: bfloat16 [2, 8192, 640], P('stage', 'expert')
- output 2: bfloat16 [2, 8192, 640], P('stage', 'expert')
- output 3: bfloat16 [2, 32, 640, 640], P('stage', 'expert')
- output 4: bfloat16 [2, 32, 640, 640], P('stage', 'expert')
- output 5: bfloat16 [2, 32, 640, 640], P('stage', 'expert')
All inputs are finite; a program needn't handle non-finite values.
Results may differ from the reference program's by a relative error of at most 0.001.
Values are sent between devices in bfloat16 or wider.
A program may use at most 1 GiB of HBM per device.

```python
import jax
import jax.numpy as jnp
from jax import lax

NUM_STAGES = 2
GROUP_SIZE = 8
TOKENS_DEV = 1024
MODEL_DIM = 640
FFN_DIM = 640
NUM_EXPERTS = 32
TOP_K = 4
CAPACITY = 3 * TOP_K * TOKENS_DEV // (2 * NUM_EXPERTS)
SLOTS = NUM_EXPERTS * CAPACITY


def device_routing(dev_key):
    key_order, key_pos = jax.random.split(dev_key)
    block_expert = jax.random.permutation(key_order, NUM_EXPERTS)
    token_pos = jax.random.permutation(key_pos, TOKENS_DEV)
    spacing = TOKENS_DEV // TOP_K
    cold_len = TOKENS_DEV // (2 * NUM_EXPERTS)
    slot_pos = (token_pos[:, None] + spacing * jnp.arange(TOP_K)[None, :]) % TOKENS_DEV
    within = slot_pos % (4 * cold_len)
    block_idx = 2 * (slot_pos // (4 * cold_len)) + (within >= 3 * cold_len).astype(jnp.int32)
    return block_expert[block_idx].astype(jnp.int32)


def draw_routing(route_key):
    sub_keys = jax.random.split(route_key, 2 * NUM_STAGES * GROUP_SIZE)
    choices = jax.vmap(device_routing)(sub_keys)
    return choices.reshape(2, NUM_STAGES, GROUP_SIZE * TOKENS_DEV, TOP_K)


def setup_inputs(seed: int = 0) -> dict:
    sub_keys = jax.random.split(jax.random.key(seed), 7)
    tok_shape = (2, NUM_STAGES, GROUP_SIZE * TOKENS_DEV)
    w_shape = (NUM_STAGES, NUM_EXPERTS, MODEL_DIM, FFN_DIM)
    x_acts = jax.random.normal(sub_keys[0], tok_shape + (MODEL_DIM,), jnp.float32)
    expert_ids = draw_routing(sub_keys[1])
    gate_wts = jax.random.uniform(sub_keys[2], tok_shape + (TOP_K,), jnp.float32, 0.5, 1.5) / TOP_K
    w_in = jax.random.normal(sub_keys[3], w_shape, jnp.float32) * MODEL_DIM ** -0.5
    w_up = jax.random.normal(sub_keys[4], w_shape, jnp.float32) * MODEL_DIM ** -0.5
    w_out = jax.random.normal(sub_keys[5], (NUM_STAGES, NUM_EXPERTS, FFN_DIM, MODEL_DIM), jnp.float32) * FFN_DIM ** -0.5
    d_out = jax.random.normal(sub_keys[6], (NUM_STAGES, GROUP_SIZE * TOKENS_DEV, MODEL_DIM), jnp.float32)
    return dict(x_acts=x_acts.astype(jnp.bfloat16), expert_ids=expert_ids, gate_wts=gate_wts,
                w_in=w_in.astype(jnp.bfloat16), w_up=w_up.astype(jnp.bfloat16),
                w_out=w_out.astype(jnp.bfloat16), d_out=d_out.astype(jnp.bfloat16))


def bf16_cast(raw_value):
    return raw_value.astype(jnp.bfloat16).astype(jnp.float32)


def slot_index(choices):
    chosen = choices[:, :, None] == jnp.arange(NUM_EXPERTS)[None, None, :]
    taken = jnp.any(chosen, axis=1).astype(jnp.int32)
    slot_rank = jnp.cumsum(taken, axis=0) - 1
    return choices * CAPACITY + jnp.take_along_axis(slot_rank, choices, axis=1)


def gather_slots(slot_idx, gates):
    flat_idx = slot_idx.reshape(-1)
    owner = jnp.zeros((SLOTS,), jnp.int32).at[flat_idx].set(jnp.repeat(jnp.arange(TOKENS_DEV), TOP_K))
    slot_gate = jnp.zeros((SLOTS,), jnp.float32).at[flat_idx].set(gates.reshape(-1))
    return owner, slot_gate.reshape(NUM_EXPERTS, CAPACITY)


def stage_layer(stage_args):
    x_two, choice_two, gate_two, w_in_s, w_up_s, w_out_s, dy_stage = stage_args
    w_in_f = w_in_s.astype(jnp.float32)
    w_up_f = w_up_s.astype(jnp.float32)
    w_out_f = w_out_s.astype(jnp.float32)

    def per_device(tensor):
        return tensor.reshape((GROUP_SIZE, TOKENS_DEV) + tensor.shape[1:])

    def device_step(grad_acc, dev_block):
        x_fw, ch_fw, g_fw, x_bw, ch_bw, g_bw, dy_bw = dev_block
        idx_fw = slot_index(ch_fw)
        owner_fw, gate_fw = gather_slots(idx_fw, g_fw)
        rows_fw = x_fw.astype(jnp.float32)[owner_fw].reshape(NUM_EXPERTS, CAPACITY, MODEL_DIM)
        pre_in = jnp.einsum('ecd,edf->ecf', rows_fw, w_in_f)
        pre_up = jnp.einsum('ecd,edf->ecf', rows_fw, w_up_f)
        hidden = bf16_cast(jax.nn.silu(pre_in) * pre_up)
        expert_out = jnp.einsum('ecf,efd->ecd', hidden, w_out_f)
        contrib = bf16_cast(gate_fw[:, :, None] * expert_out).reshape(SLOTS, MODEL_DIM)
        y_dev = jnp.sum(contrib[idx_fw], axis=1).astype(jnp.bfloat16)

        idx_bw = slot_index(ch_bw)
        owner_bw, gate_bw = gather_slots(idx_bw, g_bw)
        rows_bw = x_bw.astype(jnp.float32)[owner_bw].reshape(NUM_EXPERTS, CAPACITY, MODEL_DIM)
        dy_rows = dy_bw.astype(jnp.float32)[owner_bw].reshape(NUM_EXPERTS, CAPACITY, MODEL_DIM)
        pre_in = jnp.einsum('ecd,edf->ecf', rows_bw, w_in_f)
        pre_up = jnp.einsum('ecd,edf->ecf', rows_bw, w_up_f)
        sig_in = jax.nn.sigmoid(pre_in)
        act_in = pre_in * sig_in
        hidden = bf16_cast(act_in * pre_up)
        gated_dy = bf16_cast(gate_bw[:, :, None] * dy_rows)
        d_hidden = jnp.einsum('ecd,efd->ecf', gated_dy, w_out_f)
        d_pre_in = bf16_cast(d_hidden * pre_up * sig_in * (1.0 + pre_in * (1.0 - sig_in)))
        d_pre_up = bf16_cast(d_hidden * act_in)
        dx_slot = bf16_cast(jnp.einsum('ecf,edf->ecd', d_pre_in, w_in_f) + jnp.einsum('ecf,edf->ecd', d_pre_up, w_up_f))
        dx_dev = jnp.sum(dx_slot.reshape(SLOTS, MODEL_DIM)[idx_bw], axis=1).astype(jnp.bfloat16)
        acc_in, acc_up, acc_out = grad_acc
        new_acc = (acc_in + jnp.einsum('ecd,ecf->edf', rows_bw, d_pre_in),
                   acc_up + jnp.einsum('ecd,ecf->edf', rows_bw, d_pre_up),
                   acc_out + jnp.einsum('ecf,ecd->efd', hidden, gated_dy))
        return new_acc, (y_dev, dx_dev)

    zero_acc = (jnp.zeros(w_in_s.shape, jnp.float32), jnp.zeros(w_up_s.shape, jnp.float32),
                jnp.zeros(w_out_s.shape, jnp.float32))
    blocks = (per_device(x_two[1]), per_device(choice_two[1]), per_device(gate_two[1]),
              per_device(x_two[0]), per_device(choice_two[0]), per_device(gate_two[0]),
              per_device(dy_stage))
    grads, outs = lax.scan(device_step, zero_acc, blocks)
    tok_total = GROUP_SIZE * TOKENS_DEV
    return (outs[0].reshape(tok_total, MODEL_DIM), outs[1].reshape(tok_total, MODEL_DIM),
            grads[0].astype(jnp.bfloat16), grads[1].astype(jnp.bfloat16), grads[2].astype(jnp.bfloat16))


def reference(x_acts, expert_ids, gate_wts, w_in, w_up, w_out, d_out):
    x_prev = jnp.moveaxis(jnp.roll(x_acts, 1, axis=1), 1, 0)
    ids_prev = jnp.moveaxis(jnp.roll(expert_ids, 1, axis=1), 1, 0)
    gate_prev = jnp.moveaxis(jnp.roll(gate_wts, 1, axis=1), 1, 0)
    y_out, dx_next, d_w_in, d_w_up, d_w_out = lax.map(
        stage_layer, (x_prev, ids_prev, gate_prev, w_in, w_up, w_out, d_out))
    d_x = jnp.roll(dx_next, -1, axis=0)
    return (y_out, d_x, d_w_in, d_w_up, d_w_out)
```

```python
import functools

import jax
import jax.numpy as jnp
from jax import lax
from jax.experimental import pallas as pl
from jax.experimental.pallas import tpu as pltpu
from jax.sharding import PartitionSpec as P

MESH = pl.DeviceIdType.MESH
F32, BF16 = jnp.float32, jnp.bfloat16
DY, XF, XB, TAB = 0, 1, 2, 3
NG, NE, CAP = 8, 4, 192


def dot(lhs, rhs, dims=((1,), (0,))):
    return lax.dot_general(lhs, rhs, (dims, ((), ())), preferred_element_type=F32)


def slot_hits(code_rows, tokens):
    slot = lax.broadcasted_iota(jnp.int32, (CAP, tokens), 0).astype(F32)
    return [slot == code_rows[e:e + 1, :] for e in range(NE)]


def dispatch_kernel(x_ref, dy_ref, tab_ref, win_ref, wup_ref, wout_ref,
                    c_ref, xb_ref, q_ref, code_ref,
                    buf, tabs, codes, gates, gslot, xs, st, cst, wbuf,
                    ssem, rsem, lsem, wsem, stsem, csem):
    stage = lax.axis_index('stage')
    me = lax.axis_index('expert')
    other = 1 - stage
    sib = me + 1 - 2 * (me % 2)
    xn = me + 2 - 4 * ((me // 2) % 2)
    yn = me + 4 - 8 * (me // 4)
    dg = xn + 4 - 8 * (xn // 4)
    sib_of = lambda h: h + 1 - 2 * (h % 2)
    tokens = x_ref.shape[2]
    half = tokens // 2
    sends = []

    barrier = pltpu.get_barrier_semaphore()
    for peer in ((other, me), (stage, sib), (stage, xn), (stage, yn)):
        pl.semaphore_signal(barrier, inc=1, device_id=peer, device_id_type=MESH)
    pl.semaphore_wait(barrier, 4)

    def place(arr, h, part):
        if arr == TAB:
            return tabs.at[h]
        if arr == XB:
            return xb_ref.at[h, pl.ds(part * half, half)]
        return buf.at[arr, h, pl.ds(part * half, half)]

    def remote(arr, h, part, slot, peer, src=None):
        return pltpu.make_async_remote_copy(
            src_ref=place(arr, h, part) if src is None else src, dst_ref=place(arr, h, part),
            send_sem=ssem.at[arr, slot], recv_sem=rsem.at[arr, h, part],
            device_id=peer, device_id_type=MESH)

    def send(arr, h, part, slot, peer, src=None):
        copy = remote(arr, h, part, slot, peer, src)
        copy.start()
        sends.append(copy)

    def arrived(arr, h, part):
        remote(arr, h, part, 0, (stage, sib)).wait_recv()

    to_x, to_y, to_sib, to_z = (stage, xn), (stage, yn), (stage, sib), (other, me)

    send(TAB, me, 0, 14, to_z, tab_ref)
    for part in range(2):
        send(XF, me, part, 14 + part, to_z, x_ref.at[1, 0, pl.ds(part * half, half)])
    for part in range(2):
        send(XB, me, part, 14 + part, to_z, x_ref.at[0, 0, pl.ds(part * half, half)])
    dy_half = lambda part: dy_ref.at[0, pl.ds(part * half, half)]
    send(DY, me, 0, 0, to_x, dy_half(0))
    send(DY, me, 1, 2, to_y, dy_half(1))
    send(DY, me, 0, 4, to_sib, dy_half(0))
    send(DY, me, 1, 5, to_sib, dy_half(1))
    own_dy = pltpu.make_async_copy(dy_ref.at[0], buf.at[DY, me], lsem)
    own_dy.start()

    def weights(e):
        return [pltpu.make_async_copy(w.at[0, e], wbuf.at[e % 2, k], wsem.at[e % 2, k])
                for k, w in enumerate((win_ref, wup_ref, wout_ref))]

    for e in range(2):
        for copy in weights(e):
            copy.start()

    arrived(TAB, me, 0)
    send(TAB, me, 0, 0, to_x)
    send(TAB, me, 0, 2, to_y)
    send(TAB, me, 0, 4, to_sib)
    send(DY, me, 1, 1, to_x, dy_half(1))
    send(DY, me, 0, 3, to_y, dy_half(0))

    def first_halves(arr):
        arrived(arr, xn, 0)
        arrived(arr, yn, 1)
        send(arr, xn, 0, 6, to_y)
        send(arr, yn, 1, 7, to_x)
        send(arr, xn, 0, 8, to_sib)
        send(arr, yn, 1, 11, to_sib)

    def second_halves(arr):
        arrived(arr, xn, 1)
        arrived(arr, yn, 0)
        send(arr, xn, 1, 9, to_sib)
        send(arr, yn, 0, 10, to_sib)

    def diagonal(arr):
        for part in range(2):
            arrived(arr, dg, part)
            send(arr, dg, part, 12 + part, to_sib)

    def own_sends(arr):
        for part in range(2):
            arrived(arr, me, part)
        send(arr, me, 0, 0, to_x)
        send(arr, me, 1, 2, to_y)
        send(arr, me, 1, 1, to_x)
        send(arr, me, 0, 3, to_y)
        send(arr, me, 0, 4, to_sib)
        send(arr, me, 1, 5, to_sib)

    arrived(TAB, xn, 0)
    arrived(TAB, yn, 0)
    send(TAB, xn, 0, 6, to_y)
    first_halves(DY)
    send(TAB, xn, 0, 8, to_sib)
    send(TAB, yn, 0, 10, to_sib)
    own_sends(XF)
    second_halves(DY)
    arrived(TAB, dg, 0)
    send(TAB, dg, 0, 12, to_sib)
    for h in (sib, sib_of(xn), sib_of(yn), sib_of(dg)):
        arrived(TAB, h, 0)

    upper = (lax.broadcasted_iota(jnp.int32, (tokens, tokens), 0)
             <= lax.broadcasted_iota(jnp.int32, (tokens, tokens), 1)).astype(F32).astype(BF16)
    top_k = 4
    for kind in range(2):
        taken = []
        for h in range(NG):
            ids = tabs[h, 8 * kind:8 * kind + top_k, :]
            gts = tabs[h, 8 * kind + top_k:8 * kind + 2 * top_k, :]
            for e in range(NE):
                eq = ids == (me * NE + e).astype(F32)
                taken.append(jnp.sum(jnp.where(eq, 1.0, 0.0), axis=0, keepdims=True))
                gates[kind, h, e:e + 1, :] = jnp.sum(jnp.where(eq, gts, 0.0), axis=0, keepdims=True)
        taken = jnp.concatenate(taken, axis=0)
        rank = dot(taken.astype(BF16), upper) - 1.0
        code = jnp.where(taken > 0.5, rank, -1.0)
        for h in range(NG):
            codes[kind, h, 0:NE, :] = code[h * NE:(h + 1) * NE, :]
            codes[kind, h, NE:8, :] = jnp.full((8 - NE, tokens), -1.0, F32)
    code_copy = pltpu.make_async_copy(codes.at[1], code_ref, lsem)

    def gather(kind, h, tok_rows):
        hits = slot_hits(codes[kind, h], tokens)
        gate_rows = gates[kind, h]
        onehot = jnp.concatenate([jnp.where(hit, 1.0, 0.0).astype(BF16) for hit in hits], axis=0)
        slot_gate = [jnp.sum(jnp.where(hits[e], gate_rows[e:e + 1, :], 0.0), axis=1, keepdims=True)
                     for e in range(NE)]
        return dot(onehot, tok_rows), slot_gate

    def q_copy(slot, h):
        return pltpu.make_async_copy(st.at[slot], q_ref.at[:, h], stsem.at[slot])

    def gather_dy(n, h, wait_slot):
        slot = n % 2
        if wait_slot:
            q_copy(slot, h).wait()
        rows, slot_gate = gather(1, h, buf[DY, h])
        for e in range(NE):
            st[slot, e] = (slot_gate[e] * rows[e * CAP:(e + 1) * CAP]).astype(BF16)
        q_copy(slot, h).start()

    def gather_xf(h):
        rows, slot_gate = gather(0, h, buf[XF, h])
        for e in range(NE):
            xs[e, h] = rows[e * CAP:(e + 1) * CAP].astype(BF16)
            gslot[e, h] = jnp.broadcast_to(slot_gate[e], (CAP, 128))

    own_dy.wait()
    code_copy.start()
    code_copy.wait()

    def pick(i, *choices):
        out = choices[-1]
        for k in range(len(choices) - 2, -1, -1):
            out = jnp.where(i == k, choices[k], out)
        return out

    def dy_pair(i, h, wait_slot):
        gather_dy(0, h, wait_slot)
        h2 = sib_of(h)
        arrived(DY, h2, 0)
        arrived(DY, h2, 1)
        gather_dy(1, h2, wait_slot)

    dy_pair(0, me, False)

    @pl.loop(0, 2)
    def _(i):
        dy_pair(0, xn + i * (yn - xn), True)

    diagonal(DY)
    dy_pair(0, dg, True)
    first_halves(XF)
    own_sends(XB)

    def xf_pair(h):
        gather_xf(h)
        h2 = sib_of(h)
        arrived(XF, h2, 0)
        arrived(XF, h2, 1)
        gather_xf(h2)

    xf_pair(me)
    second_halves(XF)

    @pl.loop(0, 2)
    def _(i):
        xf_pair(xn + i * (yn - xn))

    diagonal(XF)
    xf_pair(dg)

    chunk = 2
    rows_chunk = chunk * CAP

    def c_copy(slot, e, h0):
        return pltpu.make_async_copy(cst.at[slot], c_ref.at[pl.ds(h0, chunk), e], csem.at[slot])

    def ffn(e, first):
        for copy in weights(e):
            copy.wait()

        def body(i, wait_slot):
            slot = i % 2
            h0 = i * chunk
            rows = xs[e, pl.ds(h0, chunk)].reshape(rows_chunk, -1)
            pre = dot(rows, wbuf[e % 2, 0])
            act = pre * jax.nn.sigmoid(pre)
            hidden = (act * dot(rows, wbuf[e % 2, 1])).astype(BF16)
            out = dot(hidden, wbuf[e % 2, 2])
            gate = gslot[e, pl.ds(h0, chunk)].reshape(rows_chunk, 128)[:, 0:1]
            if wait_slot:
                c_copy(slot, e, h0).wait()
            cst[slot] = (gate * out).astype(BF16).reshape(chunk, CAP, -1)
            c_copy(slot, e, h0).start()

        if first:
            body(0, False)
            body(1, False)
            pl.loop(2, NG // chunk)(lambda i: body(i, True))
        else:
            pl.loop(0, NG // chunk)(lambda i: body(i, True))
        if e + 2 < NE:
            for copy in weights(e + 2):
                copy.start()

    ffn(0, True)
    first_halves(XB)
    ffn(1, False)
    ffn(2, False)
    second_halves(XB)
    ffn(3, False)
    diagonal(XB)
    for h in (sib, sib_of(xn), sib_of(yn), sib_of(dg)):
        arrived(XB, h, 0)
        arrived(XB, h, 1)
    for slot in range(2):
        c_copy(slot, NE - 1, 0).wait()
        q_copy(slot, 0).wait()
    for copy in sends:
        copy.wait_send()


def run_dispatch(x_acts, d_out, table, w_in, w_up, w_out):
    tokens, dim = x_acts.shape[2:]
    hid = w_in.shape[3]
    any_spec = pl.BlockSpec(memory_space=pl.ANY)
    flops = 2 * NG * NE * CAP * (2 * tokens * dim + 3 * dim * hid)
    return pl.pallas_call(
        dispatch_kernel,
        name='dispatch',
        out_shape=(jax.ShapeDtypeStruct((NG, NE, CAP, dim), BF16),
                   jax.ShapeDtypeStruct((NG, tokens, dim), BF16),
                   jax.ShapeDtypeStruct((NE, NG, CAP, dim), BF16),
                   jax.ShapeDtypeStruct((NG, 8, tokens), F32)),
        in_specs=[any_spec] * 6,
        out_specs=[any_spec] * 4,
        scratch_shapes=[
            pltpu.VMEM((2, NG, tokens, dim), BF16),
            pltpu.VMEM((NG, 16, tokens), F32),
            pltpu.VMEM((2, NG, 8, tokens), F32),
            pltpu.VMEM((2, NG, 8, tokens), F32),
            pltpu.VMEM((NE, NG, CAP, 128), F32),
            pltpu.VMEM((NE, NG, CAP, dim), BF16),
            pltpu.VMEM((2, NE, CAP, dim), BF16),
            pltpu.VMEM((2, 2, CAP, dim), BF16),
            pltpu.VMEM((2, 3, dim, hid), BF16),
            pltpu.SemaphoreType.DMA((4, 16)),
            pltpu.SemaphoreType.DMA((4, NG, 2)),
            pltpu.SemaphoreType.DMA,
            pltpu.SemaphoreType.DMA((2, 3)),
            pltpu.SemaphoreType.DMA((2,)),
            pltpu.SemaphoreType.DMA((2,)),
        ],
        cost_estimate=pl.CostEstimate(flops=flops, bytes_accessed=60_000_000, transcendentals=0),
        compiler_params=pltpu.CompilerParams(collective_id=0, has_side_effects=True,
                                             vmem_limit_bytes=67_043_328),
    )(x_acts, d_out, table, w_in, w_up, w_out)


def backward_kernel(code_ref, xb_ref, q_ref, win_ref, wup_ref, wout_ref,
                    dx_ref, dwin_ref, dwup_ref, dwout_ref,
                    xs, acc_in, acc_up, acc_out):
    step = pl.program_id(0)
    tokens, dim = xb_ref.shape[1:]

    @pl.when(step < NG)
    def _():
        hits = slot_hits(code_ref[0], tokens)
        onehot = jnp.concatenate([jnp.where(hit, 1.0, 0.0).astype(BF16) for hit in hits], axis=0)
        rows = dot(onehot, xb_ref[0]).astype(BF16)
        for e in range(NE):
            xs[e, step] = rows[e * CAP:(e + 1) * CAP]

    @pl.when(step >= NG)
    def _():
        e = step - NG
        chunk = 4
        rows_chunk = chunk * CAP

        def body(i):
            hs = pl.ds(i * chunk, chunk)
            x = xs[e, hs].reshape(rows_chunk, dim)
            q = q_ref[0, hs].reshape(rows_chunk, dim)
            pre_in = dot(x, win_ref[0, 0])
            pre_up = dot(x, wup_ref[0, 0])
            d_hid = dot(q, wout_ref[0, 0], ((1,), (1,)))
            sig = jax.nn.sigmoid(pre_in)
            act = pre_in * sig
            hidden = (act * pre_up).astype(BF16)
            d_in = (d_hid * pre_up * sig * (1.0 + pre_in * (1.0 - sig))).astype(BF16)
            d_up = (d_hid * act).astype(BF16)
            dx = dot(d_in, win_ref[0, 0], ((1,), (1,))) + dot(d_up, wup_ref[0, 0], ((1,), (1,)))
            dx_ref[hs, 0] = dx.astype(BF16).reshape(chunk, CAP, dim)
            return (dot(x, d_in, ((0,), (0,))), dot(x, d_up, ((0,), (0,))),
                    dot(hidden, q, ((0,), (0,))))

        steps = NG // chunk

        def loop(i, carry):
            parts = body(i)
            first = i == 0
            for acc, part in zip((acc_in, acc_up, acc_out), parts):
                acc[...] = jnp.where(first, part, acc[...] + part)
            return carry

        lax.fori_loop(0, steps, loop, 0)
        dwin_ref[0, 0] = acc_in[...].astype(BF16)
        dwup_ref[0, 0] = acc_up[...].astype(BF16)
        dwout_ref[0, 0] = acc_out[...].astype(BF16)


def run_backward(code, xb, q, w_in, w_up, w_out):
    tokens, dim = xb.shape[1:]
    hid = w_in.shape[3]
    exp = lambda i: jnp.maximum(i - NG, 0)
    src = lambda i: jnp.minimum(i, NG - 1)
    w_spec = lambda rows, cols: pl.BlockSpec((1, 1, rows, cols), lambda i: (0, exp(i), 0, 0))
    flops = 2 * NG * NE * CAP * (tokens * dim + 8 * dim * hid)
    return pl.pallas_call(
        backward_kernel,
        name='backward',
        grid=(NG + NE,),
        out_shape=(jax.ShapeDtypeStruct((NG, NE, CAP, dim), BF16),
                   jax.ShapeDtypeStruct(w_in.shape, BF16),
                   jax.ShapeDtypeStruct(w_up.shape, BF16),
                   jax.ShapeDtypeStruct(w_out.shape, BF16)),
        in_specs=[pl.BlockSpec((1, 8, tokens), lambda i: (src(i), 0, 0)),
                  pl.BlockSpec((1, tokens, dim), lambda i: (src(i), 0, 0)),
                  pl.BlockSpec((1, NG, CAP, dim), lambda i: (exp(i), 0, 0, 0)),
                  w_spec(dim, hid), w_spec(dim, hid), w_spec(hid, dim)],
        out_specs=[pl.BlockSpec((NG, 1, CAP, dim), lambda i: (0, exp(i), 0, 0)),
                   w_spec(dim, hid), w_spec(dim, hid), w_spec(hid, dim)],
        scratch_shapes=[pltpu.VMEM((NE, NG, CAP, dim), BF16),
                        pltpu.VMEM((dim, hid), F32), pltpu.VMEM((dim, hid), F32),
                        pltpu.VMEM((hid, dim), F32)],
        cost_estimate=pl.CostEstimate(flops=flops, bytes_accessed=60_000_000, transcendentals=0),
        compiler_params=pltpu.CompilerParams(dimension_semantics=('arbitrary',),
                                             vmem_limit_bytes=64_000_000),
    )(code, xb, q, w_in, w_up, w_out)


def token_codes(ids, num_experts):
    tokens, top_k = ids.shape
    experts = lax.broadcasted_iota(jnp.int32, (tokens, num_experts), 1)
    taken = jnp.zeros((tokens, num_experts), F32)
    for j in range(top_k):
        taken += jnp.where(ids[:, j:j + 1] == experts, 1.0, 0.0)
    lower = (lax.broadcasted_iota(jnp.int32, (tokens, tokens), 0)
             >= lax.broadcasted_iota(jnp.int32, (tokens, tokens), 1)).astype(F32).astype(BF16)
    rank = dot(lower, taken.astype(BF16)) - 1.0
    return jnp.where(taken > 0.5, rank, -10000.0)


def slot_matrix(code):
    tokens = code.shape[0]
    lane = lax.broadcasted_iota(jnp.int32, (tokens, 128), 1).astype(F32)
    blocks = []
    for b in range(NE * CAP // 128):
        hit = None
        for e in range(NE):
            if e * CAP < (b + 1) * 128 and (e + 1) * CAP > b * 128:
                eq = lane == code[:, e:e + 1] + float(e * CAP - b * 128)
                hit = eq if hit is None else hit | eq
        blocks.append(jnp.where(hit, 1.0, 0.0).astype(BF16))
    return jnp.concatenate(blocks, axis=1)


def combine_kernel(ids_ref, rows_ref, out_ref, acc, codes):
    step = pl.program_id(0)

    @pl.when(step == 0)
    def _():
        code = token_codes(ids_ref[...], NG * NE)
        for s in range(NG):
            codes[s] = code[:, s * NE:(s + 1) * NE]

    part = dot(slot_matrix(codes[step]), rows_ref[0])

    @pl.when(step == 0)
    def _():
        acc[...] = part

    @pl.when(step > 0)
    def _():
        acc[...] += part

    @pl.when(step == NG - 1)
    def _():
        out_ref[...] = acc[...].astype(BF16)


def run_combine(ids, rows):
    tokens, top_k = ids.shape
    dim = rows.shape[2]
    return pl.pallas_call(
        combine_kernel,
        name='combine',
        grid=(NG,),
        out_shape=jax.ShapeDtypeStruct((tokens, dim), BF16),
        in_specs=[pl.BlockSpec((tokens, top_k), lambda i: (0, 0)),
                  pl.BlockSpec((1, NE * CAP, dim), lambda i: (i, 0, 0))],
        out_specs=pl.BlockSpec((tokens, dim), lambda i: (0, 0)),
        scratch_shapes=[pltpu.VMEM((tokens, dim), F32), pltpu.VMEM((NG, tokens, NE), F32)],
        cost_estimate=pl.CostEstimate(flops=2 * tokens * NG * NE * CAP * dim,
                                      bytes_accessed=10_000_000, transcendentals=0),
        compiler_params=pltpu.CompilerParams(dimension_semantics=('arbitrary',),
                                             vmem_limit_bytes=48_000_000),
    )(ids, rows)


def solution(mesh):
    to_next = [(0, 1), (1, 0)]

    def device_fn(x_acts, expert_ids, gate_wts, w_in, w_up, w_out, d_out):
        dim = x_acts.shape[3]
        ids_t = jnp.swapaxes(expert_ids[:, 0], 1, 2).astype(F32)
        gates_t = jnp.swapaxes(gate_wts[:, 0], 1, 2)
        table = jnp.concatenate([ids_t[1], gates_t[1], ids_t[0], gates_t[0]], axis=0)
        ids_here = lax.ppermute(expert_ids[:, 0], 'stage', to_next)

        c_rows, xb, q_rows, code = run_dispatch(x_acts, d_out, table, w_in, w_up, w_out)

        def give_back(rows):
            return lax.all_to_all(rows.reshape(NG, NE * CAP, dim), 'expert', 0, 0, tiled=True)

        y_back = give_back(c_rows)
        dx_rows, dw_in, dw_up, dw_out = run_backward(code, xb, q_rows, w_in, w_up, w_out)
        dx_back = give_back(dx_rows)
        y_dev = run_combine(ids_here[1], y_back)
        dx_here = run_combine(ids_here[0], dx_back)
        dx_dev = lax.ppermute(dx_here, 'stage', to_next)
        return y_dev[None], dx_dev[None], dw_in, dw_up, dw_out

    tok_spec = P(None, 'stage', 'expert', None)
    w_spec = P('stage', 'expert', None, None)
    row_spec = P('stage', 'expert', None)
    return jax.shard_map(device_fn, mesh=mesh,
                         in_specs=(tok_spec, tok_spec, tok_spec, w_spec, w_spec, w_spec, row_spec),
                         out_specs=(row_spec, row_spec, w_spec, w_spec, w_spec), check_vma=False)
```

```python
import jax
import jax.numpy as jnp
from jax import lax
from jax.experimental import pallas as pl
from jax.experimental.pallas import tpu as pltpu
from jax.sharding import PartitionSpec as P

MESH = pl.DeviceIdType.MESH
F32, BF16 = jnp.float32, jnp.bfloat16
DY, XF, XB, TAB = 0, 1, 2, 3
NG, NE, CAP = 8, 4, 192


def dot(lhs, rhs, dims=((1,), (0,))):
    return lax.dot_general(lhs, rhs, (dims, ((), ())), preferred_element_type=F32)


def slot_hits(code_rows, tokens):
    slot = lax.broadcasted_iota(jnp.int32, (CAP, tokens), 0).astype(F32)
    return [slot == code_rows[e:e + 1, :] for e in range(NE)]


def dispatch_kernel(x_ref, dy_ref, tab_ref, win_ref, wup_ref, wout_ref,
                    c_ref, xb_ref, q_ref, code_ref, tab_out,
                    buf, tabs, codes, gates, gslot, xs, st, cst, wbuf,
                    ssem, rsem, lsem, wsem, stsem, csem, tsem):
    stage = lax.axis_index('stage')
    me = lax.axis_index('expert')
    other = 1 - stage
    sib = me + 1 - 2 * (me % 2)
    xn = me + 2 - 4 * ((me // 2) % 2)
    yn = me + 4 - 8 * (me // 4)
    dg = xn + 4 - 8 * (xn // 4)
    sib_of = lambda h: h + 1 - 2 * (h % 2)
    tokens = x_ref.shape[2]
    half = tokens // 2
    sends = []

    barrier = pltpu.get_barrier_semaphore()
    for peer in ((other, me), (stage, sib), (stage, xn), (stage, yn)):
        pl.semaphore_signal(barrier, inc=1, device_id=peer, device_id_type=MESH)
    pl.semaphore_wait(barrier, 4)

    def place(arr, h, part):
        if arr == TAB:
            return tabs.at[h]
        if arr == XB:
            return xb_ref.at[h, pl.ds(part * half, half)]
        return buf.at[arr, h, pl.ds(part * half, half)]

    def remote(arr, h, part, slot, peer, src=None):
        return pltpu.make_async_remote_copy(
            src_ref=place(arr, h, part) if src is None else src, dst_ref=place(arr, h, part),
            send_sem=ssem.at[arr, slot], recv_sem=rsem.at[arr, h, part],
            device_id=peer, device_id_type=MESH)

    def send(arr, h, part, slot, peer, src=None):
        copy = remote(arr, h, part, slot, peer, src)
        copy.start()
        sends.append(copy)

    def arrived(arr, h, part):
        remote(arr, h, part, 0, (stage, sib)).wait_recv()

    to_x, to_y, to_sib, to_z = (stage, xn), (stage, yn), (stage, sib), (other, me)

    send(TAB, me, 0, 14, to_z, tab_ref)
    for part in range(2):
        send(XF, me, part, 14 + part, to_z, x_ref.at[1, 0, pl.ds(part * half, half)])
    for part in range(2):
        send(XB, me, part, 14 + part, to_z, x_ref.at[0, 0, pl.ds(part * half, half)])
    dy_half = lambda part: dy_ref.at[0, pl.ds(part * half, half)]
    send(DY, me, 0, 0, to_x, dy_half(0))
    send(DY, me, 1, 2, to_y, dy_half(1))
    send(DY, me, 0, 4, to_sib, dy_half(0))
    send(DY, me, 1, 5, to_sib, dy_half(1))
    own_dy = pltpu.make_async_copy(dy_ref.at[0], buf.at[DY, me], lsem)
    own_dy.start()

    def weights(e):
        return [pltpu.make_async_copy(w.at[0, e], wbuf.at[e % 2, k], wsem.at[e % 2, k])
                for k, w in enumerate((win_ref, wup_ref, wout_ref))]

    for e in range(2):
        for copy in weights(e):
            copy.start()

    arrived(TAB, me, 0)
    send(TAB, me, 0, 0, to_x)
    send(TAB, me, 0, 2, to_y)
    send(TAB, me, 0, 4, to_sib)
    send(DY, me, 1, 1, to_x, dy_half(1))
    send(DY, me, 0, 3, to_y, dy_half(0))

    def first_halves(arr):
        arrived(arr, xn, 0)
        arrived(arr, yn, 1)
        send(arr, xn, 0, 6, to_y)
        send(arr, yn, 1, 7, to_x)
        send(arr, xn, 0, 8, to_sib)
        send(arr, yn, 1, 11, to_sib)

    def second_halves(arr):
        arrived(arr, xn, 1)
        arrived(arr, yn, 0)
        send(arr, xn, 1, 9, to_sib)
        send(arr, yn, 0, 10, to_sib)

    def diagonal(arr):
        for part in range(2):
            arrived(arr, dg, part)
            send(arr, dg, part, 12 + part, to_sib)

    def own_sends(arr):
        for part in range(2):
            arrived(arr, me, part)
        send(arr, me, 0, 0, to_x)
        send(arr, me, 1, 2, to_y)
        send(arr, me, 1, 1, to_x)
        send(arr, me, 0, 3, to_y)
        send(arr, me, 0, 4, to_sib)
        send(arr, me, 1, 5, to_sib)

    arrived(TAB, xn, 0)
    arrived(TAB, yn, 0)
    send(TAB, xn, 0, 6, to_y)
    first_halves(DY)
    send(TAB, xn, 0, 8, to_sib)
    send(TAB, yn, 0, 10, to_sib)
    own_sends(XF)
    second_halves(DY)
    arrived(TAB, dg, 0)
    send(TAB, dg, 0, 12, to_sib)
    for h in (sib, sib_of(xn), sib_of(yn), sib_of(dg)):
        arrived(TAB, h, 0)
    core = me % 2
    tab_copies = [pltpu.make_async_copy(tabs.at[h], tab_out.at[k], tsem.at[k])
                  for k, h in enumerate((me, yn + core * (xn - yn)))]
    for copy in tab_copies:
        copy.start()

    upper = (lax.broadcasted_iota(jnp.int32, (tokens, tokens), 0)
             <= lax.broadcasted_iota(jnp.int32, (tokens, tokens), 1)).astype(F32).astype(BF16)
    top_k = 4
    for kind in range(2):
        taken = []
        for h in range(NG):
            ids = tabs[h, 8 * kind:8 * kind + top_k, :]
            gts = tabs[h, 8 * kind + top_k:8 * kind + 2 * top_k, :]
            for e in range(NE):
                eq = ids == (me * NE + e).astype(F32)
                taken.append(jnp.sum(jnp.where(eq, 1.0, 0.0), axis=0, keepdims=True))
                gates[kind, h, e:e + 1, :] = jnp.sum(jnp.where(eq, gts, 0.0), axis=0, keepdims=True)
        taken = jnp.concatenate(taken, axis=0)
        rank = dot(taken.astype(BF16), upper) - 1.0
        code = jnp.where(taken > 0.5, rank, -1.0)
        for h in range(NG):
            codes[kind, h, 0:NE, :] = code[h * NE:(h + 1) * NE, :]
            codes[kind, h, NE:8, :] = jnp.full((8 - NE, tokens), -1.0, F32)
    code_copy = pltpu.make_async_copy(codes.at[1], code_ref, lsem)

    def gather(kind, h, tok_rows):
        hits = slot_hits(codes[kind, h], tokens)
        gate_rows = gates[kind, h]
        onehot = jnp.concatenate([jnp.where(hit, 1.0, 0.0).astype(BF16) for hit in hits], axis=0)
        slot_gate = [jnp.sum(jnp.where(hits[e], gate_rows[e:e + 1, :], 0.0), axis=1, keepdims=True)
                     for e in range(NE)]
        return dot(onehot, tok_rows), slot_gate

    def q_copy(slot, h):
        return pltpu.make_async_copy(st.at[slot], q_ref.at[:, h], stsem.at[slot])

    def gather_dy(n, h, wait_slot):
        slot = n % 2
        if wait_slot:
            q_copy(slot, h).wait()
        rows, slot_gate = gather(1, h, buf[DY, h])
        for e in range(NE):
            st[slot, e] = (slot_gate[e] * rows[e * CAP:(e + 1) * CAP]).astype(BF16)
        q_copy(slot, h).start()

    def gather_xf(h):
        rows, slot_gate = gather(0, h, buf[XF, h])
        for e in range(NE):
            xs[e, h] = rows[e * CAP:(e + 1) * CAP].astype(BF16)
            gslot[e, h] = jnp.broadcast_to(slot_gate[e], (CAP, 128))

    own_dy.wait()
    code_copy.start()
    code_copy.wait()

    def pick(i, *choices):
        out = choices[-1]
        for k in range(len(choices) - 2, -1, -1):
            out = jnp.where(i == k, choices[k], out)
        return out

    def dy_pair(i, h, wait_slot):
        gather_dy(0, h, wait_slot)
        h2 = sib_of(h)
        arrived(DY, h2, 0)
        arrived(DY, h2, 1)
        gather_dy(1, h2, wait_slot)

    dy_pair(0, me, False)

    @pl.loop(0, 2)
    def _(i):
        dy_pair(0, xn + i * (yn - xn), True)

    diagonal(DY)
    dy_pair(0, dg, True)
    first_halves(XF)
    own_sends(XB)

    def xf_pair(h):
        gather_xf(h)
        h2 = sib_of(h)
        arrived(XF, h2, 0)
        arrived(XF, h2, 1)
        gather_xf(h2)

    xf_pair(me)
    second_halves(XF)

    @pl.loop(0, 2)
    def _(i):
        xf_pair(xn + i * (yn - xn))

    diagonal(XF)
    xf_pair(dg)

    chunk = 2
    rows_chunk = chunk * CAP

    def c_copy(slot, e, h0):
        return pltpu.make_async_copy(cst.at[slot], c_ref.at[pl.ds(h0, chunk), e], csem.at[slot])

    def ffn(e, first):
        for copy in weights(e):
            copy.wait()

        def body(i, wait_slot):
            slot = i % 2
            h0 = i * chunk
            rows = xs[e, pl.ds(h0, chunk)].reshape(rows_chunk, -1)
            pre = dot(rows, wbuf[e % 2, 0])
            act = pre * jax.nn.sigmoid(pre)
            hidden = (act * dot(rows, wbuf[e % 2, 1])).astype(BF16)
            out = dot(hidden, wbuf[e % 2, 2])
            gate = gslot[e, pl.ds(h0, chunk)].reshape(rows_chunk, 128)[:, 0:1]
            if wait_slot:
                c_copy(slot, e, h0).wait()
            cst[slot] = (gate * out).astype(BF16).reshape(chunk, CAP, -1)
            c_copy(slot, e, h0).start()

        if first:
            body(0, False)
            body(1, False)
            pl.loop(2, NG // chunk)(lambda i: body(i, True))
        else:
            pl.loop(0, NG // chunk)(lambda i: body(i, True))
        if e + 2 < NE:
            for copy in weights(e + 2):
                copy.start()

    ffn(0, True)
    first_halves(XB)
    ffn(1, False)
    ffn(2, False)
    second_halves(XB)
    ffn(3, False)
    diagonal(XB)
    for h in (sib, sib_of(xn), sib_of(yn), sib_of(dg)):
        arrived(XB, h, 0)
        arrived(XB, h, 1)
    for slot in range(2):
        c_copy(slot, NE - 1, 0).wait()
        q_copy(slot, 0).wait()
    for copy in tab_copies:
        copy.wait()
    for copy in sends:
        copy.wait_send()


def run_dispatch(x_acts, d_out, table, w_in, w_up, w_out):
    tokens, dim = x_acts.shape[2:]
    hid = w_in.shape[3]
    any_spec = pl.BlockSpec(memory_space=pl.ANY)
    flops = 2 * NG * NE * CAP * (2 * tokens * dim + 3 * dim * hid)
    return pl.pallas_call(
        dispatch_kernel,
        name='dispatch',
        out_shape=(jax.ShapeDtypeStruct((NG, NE, CAP, dim), BF16),
                   jax.ShapeDtypeStruct((NG, tokens, dim), BF16),
                   jax.ShapeDtypeStruct((NE, NG, CAP, dim), BF16),
                   jax.ShapeDtypeStruct((NG, 8, tokens), F32),
                   jax.ShapeDtypeStruct((2, 16, tokens), F32)),
        in_specs=[any_spec] * 6,
        out_specs=[any_spec] * 5,
        scratch_shapes=[
            pltpu.VMEM((2, NG, tokens, dim), BF16),
            pltpu.VMEM((NG, 16, tokens), F32),
            pltpu.VMEM((2, NG, 8, tokens), F32),
            pltpu.VMEM((2, NG, 8, tokens), F32),
            pltpu.VMEM((NE, NG, CAP, 128), F32),
            pltpu.VMEM((NE, NG, CAP, dim), BF16),
            pltpu.VMEM((2, NE, CAP, dim), BF16),
            pltpu.VMEM((2, 2, CAP, dim), BF16),
            pltpu.VMEM((2, 3, dim, hid), BF16),
            pltpu.SemaphoreType.DMA((4, 16)),
            pltpu.SemaphoreType.DMA((4, NG, 2)),
            pltpu.SemaphoreType.DMA,
            pltpu.SemaphoreType.DMA((2, 3)),
            pltpu.SemaphoreType.DMA((2,)),
            pltpu.SemaphoreType.DMA((2,)),
            pltpu.SemaphoreType.DMA((2,)),
        ],
        cost_estimate=pl.CostEstimate(flops=flops, bytes_accessed=60_000_000, transcendentals=0),
        compiler_params=pltpu.CompilerParams(collective_id=0, has_side_effects=True,
                                             vmem_limit_bytes=67_043_328),
    )(x_acts, d_out, table, w_in, w_up, w_out)


def backward_kernel(code_ref, xb_ref, q_ref, win_ref, wup_ref, wout_ref, c_ref,
                    dx_ref, dwin_ref, dwup_ref, dwout_ref, back_ref,
                    xs, acc_in, acc_up, acc_out, ssem, rsem):
    step = pl.program_id(0)
    tokens, dim = xb_ref.shape[1:]
    stage = lax.axis_index('stage')
    me = lax.axis_index('expert')

    def give(k):
        peer = (me + k) % NG
        return pltpu.make_async_remote_copy(
            src_ref=c_ref.at[peer], dst_ref=back_ref.at[me], send_sem=ssem.at[k], recv_sem=rsem.at[me],
            device_id=(stage, peer), device_id_type=MESH)

    def take(k):
        peer = (me + k) % NG
        return pltpu.make_async_remote_copy(
            src_ref=c_ref.at[peer], dst_ref=back_ref.at[peer], send_sem=ssem.at[k],
            recv_sem=rsem.at[peer], device_id=(stage, peer), device_id_type=MESH)

    @pl.when(step == 0)
    def _():
        barrier = pltpu.get_barrier_semaphore()
        for k in range(1, NG):
            pl.semaphore_signal(barrier, inc=1, device_id=(stage, (me + k) % NG), device_id_type=MESH)
        pl.semaphore_wait(barrier, NG - 1)
        for k in range(1, NG):
            give(k).start()

    @pl.when(step < NG)
    def _():
        hits = slot_hits(code_ref[0], tokens)
        onehot = jnp.concatenate([jnp.where(hit, 1.0, 0.0).astype(BF16) for hit in hits], axis=0)
        rows = dot(onehot, xb_ref[0]).astype(BF16)
        for e in range(NE):
            xs[e, step] = rows[e * CAP:(e + 1) * CAP]

    @pl.when(step >= NG)
    def _():
        e = step - NG
        chunk = 4
        rows_chunk = chunk * CAP

        def body(i):
            hs = pl.ds(i * chunk, chunk)
            x = xs[e, hs].reshape(rows_chunk, dim)
            q = q_ref[0, hs].reshape(rows_chunk, dim)
            pre_in = dot(x, win_ref[0, 0])
            pre_up = dot(x, wup_ref[0, 0])
            d_hid = dot(q, wout_ref[0, 0], ((1,), (1,)))
            sig = jax.nn.sigmoid(pre_in)
            act = pre_in * sig
            hidden = (act * pre_up).astype(BF16)
            d_in = (d_hid * pre_up * sig * (1.0 + pre_in * (1.0 - sig))).astype(BF16)
            d_up = (d_hid * act).astype(BF16)
            dx = dot(d_in, win_ref[0, 0], ((1,), (1,))) + dot(d_up, wup_ref[0, 0], ((1,), (1,)))
            dx_ref[hs, 0] = dx.astype(BF16).reshape(chunk, CAP, dim)
            return (dot(x, d_in, ((0,), (0,))), dot(x, d_up, ((0,), (0,))),
                    dot(hidden, q, ((0,), (0,))))

        steps = NG // chunk

        def loop(i, carry):
            parts = body(i)
            first = i == 0
            for acc, part in zip((acc_in, acc_up, acc_out), parts):
                acc[...] = jnp.where(first, part, acc[...] + part)
            return carry

        lax.fori_loop(0, steps, loop, 0)
        dwin_ref[0, 0] = acc_in[...].astype(BF16)
        dwup_ref[0, 0] = acc_up[...].astype(BF16)
        dwout_ref[0, 0] = acc_out[...].astype(BF16)

    @pl.when(step == NG + NE - 1)
    def _():
        for k in range(1, NG):
            take(k).wait_recv()
        for k in range(1, NG):
            give(k).wait_send()


def run_backward(code, xb, q, w_in, w_up, w_out, c_rows):
    tokens, dim = xb.shape[1:]
    hid = w_in.shape[3]
    exp = lambda i: jnp.maximum(i - NG, 0)
    src = lambda i: jnp.minimum(i, NG - 1)
    w_spec = lambda rows, cols: pl.BlockSpec((1, 1, rows, cols), lambda i: (0, exp(i), 0, 0))
    flops = 2 * NG * NE * CAP * (tokens * dim + 8 * dim * hid)
    return pl.pallas_call(
        backward_kernel,
        name='backward',
        grid=(NG + NE,),
        out_shape=(jax.ShapeDtypeStruct((NG, NE, CAP, dim), BF16),
                   jax.ShapeDtypeStruct(w_in.shape, BF16),
                   jax.ShapeDtypeStruct(w_up.shape, BF16),
                   jax.ShapeDtypeStruct(w_out.shape, BF16),
                   jax.ShapeDtypeStruct((NG, NE, CAP, dim), BF16)),
        in_specs=[pl.BlockSpec((1, 8, tokens), lambda i: (src(i), 0, 0)),
                  pl.BlockSpec((1, tokens, dim), lambda i: (src(i), 0, 0)),
                  pl.BlockSpec((1, NG, CAP, dim), lambda i: (exp(i), 0, 0, 0)),
                  w_spec(dim, hid), w_spec(dim, hid), w_spec(hid, dim),
                  pl.BlockSpec(memory_space=pl.ANY)],
        out_specs=[pl.BlockSpec((NG, 1, CAP, dim), lambda i: (0, exp(i), 0, 0)),
                   w_spec(dim, hid), w_spec(dim, hid), w_spec(hid, dim),
                   pl.BlockSpec(memory_space=pl.ANY)],
        scratch_shapes=[pltpu.VMEM((NE, NG, CAP, dim), BF16),
                        pltpu.VMEM((dim, hid), F32), pltpu.VMEM((dim, hid), F32),
                        pltpu.VMEM((hid, dim), F32),
                        pltpu.SemaphoreType.DMA((NG,)), pltpu.SemaphoreType.DMA((NG,))],
        cost_estimate=pl.CostEstimate(flops=flops, bytes_accessed=60_000_000, transcendentals=0),
        compiler_params=pltpu.CompilerParams(dimension_semantics=('arbitrary',), collective_id=1,
                                             has_side_effects=True, vmem_limit_bytes=64_000_000),
    )(code, xb, q, w_in, w_up, w_out, c_rows)


def token_codes(ids):
    tokens, top_k = ids.shape
    num_experts = NG * NE
    experts = lax.broadcasted_iota(jnp.int32, (tokens, num_experts), 1).astype(F32)
    taken = jnp.zeros((tokens, num_experts), F32)
    for j in range(top_k):
        taken += jnp.where(ids[:, j:j + 1] == experts, 1.0, 0.0)
    lower = (lax.broadcasted_iota(jnp.int32, (tokens, tokens), 0)
             >= lax.broadcasted_iota(jnp.int32, (tokens, tokens), 1)).astype(F32).astype(BF16)
    rank = dot(lower, taken.astype(BF16)) - 1.0
    return jnp.where(taken > 0.5, rank, -10000.0)


def slot_matrix(code):
    tokens = code.shape[0]
    lane = lax.broadcasted_iota(jnp.int32, (tokens, 128), 1).astype(F32)
    blocks = []
    for b in range(NE * CAP // 128):
        hit = None
        for e in range(NE):
            if e * CAP < (b + 1) * 128 and (e + 1) * CAP > b * 128:
                eq = lane == code[:, e:e + 1] + float(e * CAP - b * 128)
                hit = eq if hit is None else hit | eq
        blocks.append(jnp.where(hit, 1.0, 0.0).astype(BF16))
    return jnp.concatenate(blocks, axis=1)


def collect_kernel(tab_ref, c_ref, back_ref, rows_ref,
                   y_ref, dx_ref,
                   codes, ybuf, rbuf, acc, part_out, part_in, out_buf,
                   ysem, osem, ssem, rsem, psem, prsem, zsem, zrsem):
    stage = lax.axis_index('stage')
    me = lax.axis_index('expert')
    core = me % 2
    sib_of = lambda h: h + 1 - 2 * (h % 2)
    sib = sib_of(me)
    xn = me + 2 - 4 * ((me // 2) % 2)
    yn = me + 4 - 8 * (me // 4)
    dg = xn + 4 - 8 * (xn // 4)
    partner = yn + core * (xn - yn)
    line = xn + core * (yn - xn)
    line0 = 2 * (line // 2)
    tokens, dim = acc.shape
    chunks = part_out.shape[0]
    tchunk = tokens // chunks

    barrier = pltpu.get_barrier_semaphore()
    for peer in ((1 - stage, me), (stage, sib), (stage, xn), (stage, yn), (stage, sib_of(xn)),
                 (stage, sib_of(yn))):
        pl.semaphore_signal(barrier, inc=1, device_id=peer, device_id_type=MESH)
    pl.semaphore_wait(barrier, 6)

    targets = ((2 * (xn // 2), 2 * (dg // 2), 1 + core), (2 * (yn // 2) + 1, 2 * (dg // 2) + 1, 1 + core),
               (sib, sib_of(xn) + core * (sib_of(yn) - sib_of(xn)), 0))
    sends = []
    for role in range(2):
        for k, (target, via, slot) in enumerate(targets):
            sends.append(pltpu.make_async_remote_copy(
                src_ref=rows_ref.at[via if role == 0 else target], dst_ref=rbuf.at[role, slot],
                send_sem=ssem.at[role, k], recv_sem=rsem.at[role, slot],
                device_id=(stage, target), device_id_type=MESH))
            sends[-1].start()
    own = [pltpu.make_async_copy(rows_ref.at[h], rbuf.at[role, 3], osem.at[role])
           for role, h in enumerate((partner, me))]
    for copy in own:
        copy.start()

    def arrived(role, slot):
        pltpu.make_async_remote_copy(
            src_ref=rows_ref.at[me], dst_ref=rbuf.at[role, slot], send_sem=ssem.at[role, 0],
            recv_sem=rsem.at[role, slot], device_id=(stage, sib), device_id_type=MESH).wait_recv()

    def y_fetch(k):
        src = c_ref if k == 0 else back_ref
        return pltpu.make_async_copy(src.at[(me + k) % NG], ybuf.at[k % 2], ysem.at[k % 2])

    y_fetch(0).start()

    for n, (row, kind) in enumerate(((0, 0), (1, 1), (0, 1))):
        code = token_codes(tab_ref[row].T[:, 8 * kind:8 * kind + 4])
        for s in range(NG):
            codes[n, s] = code[:, s * NE:(s + 1) * NE]

    def rows_of(ref):
        return ref.reshape(NE * CAP, dim)

    def y_part(k):
        if k + 1 < NG:
            y_fetch(k + 1).start()
        y_fetch(k).wait()
        part = dot(slot_matrix(codes[0, (me + k) % NG]), rows_of(ybuf[k % 2]))
        acc[...] = part if k == 0 else acc[...] + part

    sources = (sib, line0, line0 + 1, me)

    def partial_copy(i):
        return pltpu.make_async_remote_copy(
            src_ref=part_out.at[i], dst_ref=part_in.at[i], send_sem=psem.at[i], recv_sem=prsem.at[i],
            device_id=(stage, partner), device_id_type=MESH)

    def z_copy(i):
        return pltpu.make_async_remote_copy(
            src_ref=out_buf.at[i], dst_ref=dx_ref.at[pl.ds(i * tchunk, tchunk)], send_sem=zsem.at[i],
            recv_sem=zrsem.at[i], device_id=(1 - stage, me), device_id_type=MESH)

    for k in range(0, 4):
        y_part(k)
    for slot in range(3):
        arrived(0, slot)
    own[0].wait()

    @pl.loop(0, chunks)
    def _(i):
        toks = pl.ds(i * tchunk, tchunk)
        total = None
        for slot, d in enumerate(sources):
            part = dot(slot_matrix(codes[1, d, toks]), rows_of(rbuf[0, slot]))
            total = part if total is None else total + part
        part_out[i] = total
        partial_copy(i).start()

    for k in range(4, NG):
        y_part(k)
    out_buf[...] = acc[...].astype(BF16).reshape(out_buf.shape)
    y_out = [pltpu.make_async_copy(out_buf.at[i], y_ref.at[pl.ds(i * tchunk, tchunk)], zsem.at[i])
             for i in range(chunks)]
    for copy in y_out:
        copy.start()
    for slot in range(3):
        arrived(1, slot)
    own[1].wait()
    for slot, d in enumerate(sources):
        part = dot(slot_matrix(codes[2, d]), rows_of(rbuf[1, slot]))
        acc[...] = part if slot == 0 else acc[...] + part
    for copy in y_out:
        copy.wait()

    for i in range(chunks):
        partial_copy(i).wait_recv()
        out_buf[i] = (acc[i * tchunk:(i + 1) * tchunk] + part_in[i]).astype(BF16)
        z_copy(i).start()
    for copy in sends:
        copy.wait_send()
    for i in range(chunks):
        partial_copy(i).wait_send()
        z_copy(i).wait()


def run_collect(tables, c_rows, y_back, dx_rows):
    tokens = tables.shape[2]
    dim = c_rows.shape[3]
    chunks = 4
    any_spec = pl.BlockSpec(memory_space=pl.ANY)
    return pl.pallas_call(
        collect_kernel,
        name='collect',
        out_shape=(jax.ShapeDtypeStruct((tokens, dim), BF16), jax.ShapeDtypeStruct((tokens, dim), BF16)),
        in_specs=[pl.BlockSpec(memory_space=pltpu.VMEM)] + [any_spec] * 3,
        out_specs=[any_spec] * 2,
        scratch_shapes=[
            pltpu.VMEM((3, NG, tokens, NE), F32),
            pltpu.VMEM((2, NE, CAP, dim), BF16),
            pltpu.VMEM((2, 4, NE, CAP, dim), BF16),
            pltpu.VMEM((tokens, dim), F32),
            pltpu.VMEM((chunks, tokens // chunks, dim), F32),
            pltpu.VMEM((chunks, tokens // chunks, dim), F32),
            pltpu.VMEM((chunks, tokens // chunks, dim), BF16),
            pltpu.SemaphoreType.DMA((2,)),
            pltpu.SemaphoreType.DMA((2,)),
            pltpu.SemaphoreType.DMA((2, 3)),
            pltpu.SemaphoreType.DMA((2, 3)),
            pltpu.SemaphoreType.DMA((chunks,)),
            pltpu.SemaphoreType.DMA((chunks,)),
            pltpu.SemaphoreType.DMA((chunks,)),
            pltpu.SemaphoreType.DMA((chunks,)),
        ],
        cost_estimate=pl.CostEstimate(flops=4 * tokens * NG * NE * CAP * dim,
                                      bytes_accessed=20_000_000, transcendentals=0),
        compiler_params=pltpu.CompilerParams(collective_id=2, has_side_effects=True,
                                             vmem_limit_bytes=64_000_000),
    )(tables, c_rows, y_back, dx_rows)


def solution(mesh):
    def device_fn(x_acts, expert_ids, gate_wts, w_in, w_up, w_out, d_out):
        ids_t = jnp.swapaxes(expert_ids[:, 0], 1, 2).astype(F32)
        gates_t = jnp.swapaxes(gate_wts[:, 0], 1, 2)
        table = jnp.concatenate([ids_t[1], gates_t[1], ids_t[0], gates_t[0]], axis=0)

        c_rows, xb, q_rows, code, tables = run_dispatch(x_acts, d_out, table, w_in, w_up, w_out)
        dx_rows, dw_in, dw_up, dw_out, y_back = run_backward(code, xb, q_rows, w_in, w_up, w_out, c_rows)
        y_dev, dx_dev = run_collect(tables, c_rows, y_back, dx_rows)
        return y_dev[None], dx_dev[None], dw_in, dw_up, dw_out

    tok_spec = P(None, 'stage', 'expert', None)
    w_spec = P('stage', 'expert', None, None)
    row_spec = P('stage', 'expert', None)
    return jax.shard_map(device_fn, mesh=mesh,
                         in_specs=(tok_spec, tok_spec, tok_spec, w_spec, w_spec, w_spec, row_spec),
                         out_specs=(row_spec, row_spec, w_spec, w_spec, w_spec), check_vma=False)
```

```python
import jax
import jax.numpy as jnp
from jax import lax
from jax.experimental import pallas as pl
from jax.experimental.pallas import tpu as pltpu
from jax.sharding import PartitionSpec as P

MESH = pl.DeviceIdType.MESH
F32, BF16 = jnp.float32, jnp.bfloat16
DY, XF, XB, TAB = 0, 1, 2, 3
NG, NE, CAP = 8, 4, 192


def dot(lhs, rhs, dims=((1,), (0,))):
    return lax.dot_general(lhs, rhs, (dims, ((), ())), preferred_element_type=F32)


def slot_hits(code_rows, tokens):
    slot = lax.broadcasted_iota(jnp.int32, (CAP, tokens), 0).astype(F32)
    return [slot == code_rows[e:e + 1, :] for e in range(NE)]


def dispatch_kernel(x_ref, dy_ref, tab_ref, win_ref, wup_ref, wout_ref,
                    c_ref, xb_ref, q_ref, code_ref, tok_ref,
                    buf, tabs, codes, gates, gslot, xs, st, cst, wbuf,
                    ssem, rsem, lsem, wsem, stsem, csem, tsem, tok):
    stage = lax.axis_index('stage')
    me = lax.axis_index('expert')
    other = 1 - stage
    sib = me + 1 - 2 * (me % 2)
    xn = me + 2 - 4 * ((me // 2) % 2)
    yn = me + 4 - 8 * (me // 4)
    dg = xn + 4 - 8 * (xn // 4)
    sib_of = lambda h: h + 1 - 2 * (h % 2)
    tokens = x_ref.shape[2]
    half = tokens // 2
    sends = []

    barrier = pltpu.get_barrier_semaphore()
    for peer in ((other, me), (stage, sib), (stage, xn), (stage, yn)):
        pl.semaphore_signal(barrier, inc=1, device_id=peer, device_id_type=MESH)
    pl.semaphore_wait(barrier, 4)

    def place(arr, h, part):
        if arr == TAB:
            return tabs.at[h]
        if arr == XB:
            return xb_ref.at[h, pl.ds(part * half, half)]
        return buf.at[arr, h, pl.ds(part * half, half)]

    def remote(arr, h, part, slot, peer, src=None):
        return pltpu.make_async_remote_copy(
            src_ref=place(arr, h, part) if src is None else src, dst_ref=place(arr, h, part),
            send_sem=ssem.at[arr, slot], recv_sem=rsem.at[arr, h, part],
            device_id=peer, device_id_type=MESH)

    def send(arr, h, part, slot, peer, src=None):
        copy = remote(arr, h, part, slot, peer, src)
        copy.start()
        sends.append(copy)

    def arrived(arr, h, part):
        remote(arr, h, part, 0, (stage, sib)).wait_recv()

    to_x, to_y, to_sib, to_z = (stage, xn), (stage, yn), (stage, sib), (other, me)

    send(TAB, me, 0, 14, to_z, tab_ref)
    for part in range(2):
        send(XF, me, part, 14 + part, to_z, x_ref.at[1, 0, pl.ds(part * half, half)])
    for part in range(2):
        send(XB, me, part, 14 + part, to_z, x_ref.at[0, 0, pl.ds(part * half, half)])
    dy_half = lambda part: dy_ref.at[0, pl.ds(part * half, half)]
    send(DY, me, 0, 0, to_x, dy_half(0))
    send(DY, me, 1, 2, to_y, dy_half(1))
    send(DY, me, 0, 4, to_sib, dy_half(0))
    send(DY, me, 1, 5, to_sib, dy_half(1))
    own_dy = pltpu.make_async_copy(dy_ref.at[0], buf.at[DY, me], lsem)
    own_dy.start()

    def weights(e):
        return [pltpu.make_async_copy(w.at[0, e], wbuf.at[e % 2, k], wsem.at[e % 2, k])
                for k, w in enumerate((win_ref, wup_ref, wout_ref))]

    for e in range(2):
        for copy in weights(e):
            copy.start()

    arrived(TAB, me, 0)
    send(TAB, me, 0, 0, to_x)
    send(TAB, me, 0, 2, to_y)
    send(TAB, me, 0, 4, to_sib)
    send(DY, me, 1, 1, to_x, dy_half(1))
    send(DY, me, 0, 3, to_y, dy_half(0))

    def first_halves(arr):
        arrived(arr, xn, 0)
        arrived(arr, yn, 1)
        send(arr, xn, 0, 6, to_y)
        send(arr, yn, 1, 7, to_x)
        send(arr, xn, 0, 8, to_sib)
        send(arr, yn, 1, 11, to_sib)

    def second_halves(arr):
        arrived(arr, xn, 1)
        arrived(arr, yn, 0)
        send(arr, xn, 1, 9, to_sib)
        send(arr, yn, 0, 10, to_sib)

    def diagonal(arr):
        for part in range(2):
            arrived(arr, dg, part)
            send(arr, dg, part, 12 + part, to_sib)

    def own_sends(arr):
        for part in range(2):
            arrived(arr, me, part)
        send(arr, me, 0, 0, to_x)
        send(arr, me, 1, 2, to_y)
        send(arr, me, 1, 1, to_x)
        send(arr, me, 0, 3, to_y)
        send(arr, me, 0, 4, to_sib)
        send(arr, me, 1, 5, to_sib)

    arrived(TAB, xn, 0)
    arrived(TAB, yn, 0)
    send(TAB, xn, 0, 6, to_y)
    first_halves(DY)
    send(TAB, xn, 0, 8, to_sib)
    send(TAB, yn, 0, 10, to_sib)
    own_sends(XF)
    second_halves(DY)
    arrived(TAB, dg, 0)
    send(TAB, dg, 0, 12, to_sib)
    for h in (sib, sib_of(xn), sib_of(yn), sib_of(dg)):
        arrived(TAB, h, 0)
    upper = (lax.broadcasted_iota(jnp.int32, (tokens, tokens), 0)
             <= lax.broadcasted_iota(jnp.int32, (tokens, tokens), 1)).astype(F32).astype(BF16)
    top_k = 4
    for kind in range(2):
        taken = []
        for h in range(NG):
            ids = tabs[h, 8 * kind:8 * kind + top_k, :]
            gts = tabs[h, 8 * kind + top_k:8 * kind + 2 * top_k, :]
            for e in range(NE):
                eq = ids == (me * NE + e).astype(F32)
                taken.append(jnp.sum(jnp.where(eq, 1.0, 0.0), axis=0, keepdims=True))
                gates[kind, h, e:e + 1, :] = jnp.sum(jnp.where(eq, gts, 0.0), axis=0, keepdims=True)
        taken = jnp.concatenate(taken, axis=0)
        rank = dot(taken.astype(BF16), upper) - 1.0
        code = jnp.where(taken > 0.5, rank, -1.0)
        for h in range(NG):
            codes[kind, h, 0:NE, :] = code[h * NE:(h + 1) * NE, :]
            codes[kind, h, NE:8, :] = jnp.full((8 - NE, tokens), -1.0, F32)
    code_copy = pltpu.make_async_copy(codes.at[1], code_ref, lsem)

    def gather(kind, h, tok_rows):
        hits = slot_hits(codes[kind, h], tokens)
        gate_rows = gates[kind, h]
        onehot = jnp.concatenate([jnp.where(hit, 1.0, 0.0).astype(BF16) for hit in hits], axis=0)
        slot_gate = [jnp.sum(jnp.where(hits[e], gate_rows[e:e + 1, :], 0.0), axis=1, keepdims=True)
                     for e in range(NE)]
        return dot(onehot, tok_rows), slot_gate

    def q_copy(slot, h):
        return pltpu.make_async_copy(st.at[slot], q_ref.at[:, h], stsem.at[slot])

    def gather_dy(n, h, wait_slot):
        slot = n % 2
        if wait_slot:
            q_copy(slot, h).wait()
        rows, slot_gate = gather(1, h, buf[DY, h])
        for e in range(NE):
            st[slot, e] = (slot_gate[e] * rows[e * CAP:(e + 1) * CAP]).astype(BF16)
        q_copy(slot, h).start()

    def gather_xf(h):
        rows, slot_gate = gather(0, h, buf[XF, h])
        for e in range(NE):
            xs[e, h] = rows[e * CAP:(e + 1) * CAP].astype(BF16)
            gslot[e, h] = jnp.broadcast_to(slot_gate[e], (CAP, 128))

    own_dy.wait()
    code_copy.start()
    code_copy.wait()

    def pick(i, *choices):
        out = choices[-1]
        for k in range(len(choices) - 2, -1, -1):
            out = jnp.where(i == k, choices[k], out)
        return out

    def dy_pair(i, h, wait_slot):
        gather_dy(0, h, wait_slot)
        h2 = sib_of(h)
        arrived(DY, h2, 0)
        arrived(DY, h2, 1)
        gather_dy(1, h2, wait_slot)

    core = me % 2
    partner = yn + core * (xn - yn)
    lower = (lax.broadcasted_iota(jnp.int32, (tokens, tokens), 0)
             >= lax.broadcasted_iota(jnp.int32, (tokens, tokens), 1)).astype(F32).astype(BF16)
    for n, (h, kind) in enumerate(((me, 0), (partner, 1), (me, 1))):
        tok[n] = token_codes(tabs[h].T[:, 8 * kind:8 * kind + top_k], lower)
    tok_copy = pltpu.make_async_copy(tok, tok_ref, tsem)
    tok_copy.start()

    dy_pair(0, me, False)

    @pl.loop(0, 2)
    def _(i):
        dy_pair(0, xn + i * (yn - xn), True)

    diagonal(DY)
    dy_pair(0, dg, True)
    first_halves(XF)
    own_sends(XB)

    def xf_pair(h):
        gather_xf(h)
        h2 = sib_of(h)
        arrived(XF, h2, 0)
        arrived(XF, h2, 1)
        gather_xf(h2)

    xf_pair(me)
    second_halves(XF)

    @pl.loop(0, 2)
    def _(i):
        xf_pair(xn + i * (yn - xn))

    diagonal(XF)
    xf_pair(dg)

    chunk = 2
    rows_chunk = chunk * CAP

    def c_copy(slot, e, h0):
        return pltpu.make_async_copy(cst.at[slot], c_ref.at[pl.ds(h0, chunk), e], csem.at[slot])

    def ffn(e, first):
        for copy in weights(e):
            copy.wait()

        def body(i, wait_slot):
            slot = i % 2
            h0 = i * chunk
            rows = xs[e, pl.ds(h0, chunk)].reshape(rows_chunk, -1)
            pre = dot(rows, wbuf[e % 2, 0])
            act = pre * jax.nn.sigmoid(pre)
            hidden = (act * dot(rows, wbuf[e % 2, 1])).astype(BF16)
            out = dot(hidden, wbuf[e % 2, 2])
            gate = gslot[e, pl.ds(h0, chunk)].reshape(rows_chunk, 128)[:, 0:1]
            if wait_slot:
                c_copy(slot, e, h0).wait()
            cst[slot] = (gate * out).astype(BF16).reshape(chunk, CAP, -1)
            c_copy(slot, e, h0).start()

        if first:
            body(0, False)
            body(1, False)
            pl.loop(2, NG // chunk)(lambda i: body(i, True))
        else:
            pl.loop(0, NG // chunk)(lambda i: body(i, True))
        if e + 2 < NE:
            for copy in weights(e + 2):
                copy.start()

    ffn(0, True)
    first_halves(XB)
    ffn(1, False)
    ffn(2, False)
    second_halves(XB)
    ffn(3, False)
    diagonal(XB)
    for h in (sib, sib_of(xn), sib_of(yn), sib_of(dg)):
        arrived(XB, h, 0)
        arrived(XB, h, 1)
    for slot in range(2):
        c_copy(slot, NE - 1, 0).wait()
        q_copy(slot, 0).wait()
    tok_copy.wait()
    for copy in sends:
        copy.wait_send()


def run_dispatch(x_acts, d_out, table, w_in, w_up, w_out):
    tokens, dim = x_acts.shape[2:]
    hid = w_in.shape[3]
    any_spec = pl.BlockSpec(memory_space=pl.ANY)
    flops = 2 * NG * NE * CAP * (2 * tokens * dim + 3 * dim * hid)
    return pl.pallas_call(
        dispatch_kernel,
        name='dispatch',
        out_shape=(jax.ShapeDtypeStruct((NG, NE, CAP, dim), BF16),
                   jax.ShapeDtypeStruct((NG, tokens, dim), BF16),
                   jax.ShapeDtypeStruct((NE, NG, CAP, dim), BF16),
                   jax.ShapeDtypeStruct((NG, 8, tokens), F32),
                   jax.ShapeDtypeStruct((3, tokens, 128), F32)),
        in_specs=[any_spec] * 6,
        out_specs=[any_spec] * 5,
        scratch_shapes=[
            pltpu.VMEM((2, NG, tokens, dim), BF16),
            pltpu.VMEM((NG, 16, tokens), F32),
            pltpu.VMEM((2, NG, 8, tokens), F32),
            pltpu.VMEM((2, NG, 8, tokens), F32),
            pltpu.VMEM((NE, NG, CAP, 128), F32),
            pltpu.VMEM((NE, NG, CAP, dim), BF16),
            pltpu.VMEM((2, NE, CAP, dim), BF16),
            pltpu.VMEM((2, 2, CAP, dim), BF16),
            pltpu.VMEM((2, 3, dim, hid), BF16),
            pltpu.SemaphoreType.DMA((4, 16)),
            pltpu.SemaphoreType.DMA((4, NG, 2)),
            pltpu.SemaphoreType.DMA,
            pltpu.SemaphoreType.DMA((2, 3)),
            pltpu.SemaphoreType.DMA((2,)),
            pltpu.SemaphoreType.DMA((2,)),
            pltpu.SemaphoreType.DMA,
            pltpu.VMEM((3, tokens, 128), F32),
        ],
        cost_estimate=pl.CostEstimate(flops=flops, bytes_accessed=60_000_000, transcendentals=0),
        compiler_params=pltpu.CompilerParams(collective_id=0, has_side_effects=True,
                                             vmem_limit_bytes=67_043_328),
    )(x_acts, d_out, table, w_in, w_up, w_out)


def backward_kernel(code_ref, xb_ref, q_ref, win_ref, wup_ref, wout_ref,
                    dx_ref, dwin_ref, dwup_ref, dwout_ref,
                    xs, acc_in, acc_up, acc_out):
    step = pl.program_id(0)
    tokens, dim = xb_ref.shape[1:]

    @pl.when(step < NG)
    def _():
        hits = slot_hits(code_ref[0], tokens)
        onehot = jnp.concatenate([jnp.where(hit, 1.0, 0.0).astype(BF16) for hit in hits], axis=0)
        rows = dot(onehot, xb_ref[0]).astype(BF16)
        for e in range(NE):
            xs[e, step] = rows[e * CAP:(e + 1) * CAP]

    @pl.when(step >= NG)
    def _():
        e = step - NG
        chunk = 4
        rows_chunk = chunk * CAP

        def body(i):
            hs = pl.ds(i * chunk, chunk)
            x = xs[e, hs].reshape(rows_chunk, dim)
            q = q_ref[0, hs].reshape(rows_chunk, dim)
            pre_in = dot(x, win_ref[0, 0])
            pre_up = dot(x, wup_ref[0, 0])
            d_hid = dot(q, wout_ref[0, 0], ((1,), (1,)))
            sig = jax.nn.sigmoid(pre_in)
            act = pre_in * sig
            hidden = (act * pre_up).astype(BF16)
            d_in = (d_hid * pre_up * sig * (1.0 + pre_in * (1.0 - sig))).astype(BF16)
            d_up = (d_hid * act).astype(BF16)
            dx = dot(d_in, win_ref[0, 0], ((1,), (1,))) + dot(d_up, wup_ref[0, 0], ((1,), (1,)))
            dx_ref[hs, 0] = dx.astype(BF16).reshape(chunk, CAP, dim)
            return (dot(x, d_in, ((0,), (0,))), dot(x, d_up, ((0,), (0,))),
                    dot(hidden, q, ((0,), (0,))))

        steps = NG // chunk

        def loop(i, carry):
            parts = body(i)
            first = i == 0
            for acc, part in zip((acc_in, acc_up, acc_out), parts):
                acc[...] = jnp.where(first, part, acc[...] + part)
            return carry

        lax.fori_loop(0, steps, loop, 0)
        dwin_ref[0, 0] = acc_in[...].astype(BF16)
        dwup_ref[0, 0] = acc_up[...].astype(BF16)
        dwout_ref[0, 0] = acc_out[...].astype(BF16)


def run_backward(code, xb, q, w_in, w_up, w_out):
    tokens, dim = xb.shape[1:]
    hid = w_in.shape[3]
    exp = lambda i: jnp.maximum(i - NG, 0)
    src = lambda i: jnp.minimum(i, NG - 1)
    w_spec = lambda rows, cols: pl.BlockSpec((1, 1, rows, cols), lambda i: (0, exp(i), 0, 0))
    flops = 2 * NG * NE * CAP * (tokens * dim + 8 * dim * hid)
    return pl.pallas_call(
        backward_kernel,
        name='backward',
        grid=(NG + NE,),
        out_shape=(jax.ShapeDtypeStruct((NG, NE, CAP, dim), BF16),
                   jax.ShapeDtypeStruct(w_in.shape, BF16),
                   jax.ShapeDtypeStruct(w_up.shape, BF16),
                   jax.ShapeDtypeStruct(w_out.shape, BF16)),
        in_specs=[pl.BlockSpec((1, 8, tokens), lambda i: (src(i), 0, 0)),
                  pl.BlockSpec((1, tokens, dim), lambda i: (src(i), 0, 0)),
                  pl.BlockSpec((1, NG, CAP, dim), lambda i: (exp(i), 0, 0, 0)),
                  w_spec(dim, hid), w_spec(dim, hid), w_spec(hid, dim)],
        out_specs=[pl.BlockSpec((NG, 1, CAP, dim), lambda i: (0, exp(i), 0, 0)),
                   w_spec(dim, hid), w_spec(dim, hid), w_spec(hid, dim)],
        scratch_shapes=[pltpu.VMEM((NE, NG, CAP, dim), BF16),
                        pltpu.VMEM((dim, hid), F32), pltpu.VMEM((dim, hid), F32),
                        pltpu.VMEM((hid, dim), F32)],
        cost_estimate=pl.CostEstimate(flops=flops, bytes_accessed=60_000_000, transcendentals=0),
        compiler_params=pltpu.CompilerParams(dimension_semantics=('arbitrary',),
                                             vmem_limit_bytes=64_000_000),
    )(code, xb, q, w_in, w_up, w_out)


def token_codes(ids, lower):
    tokens, top_k = ids.shape
    experts = lax.broadcasted_iota(jnp.int32, (tokens, 128), 1).astype(F32)
    taken = jnp.zeros((tokens, 128), F32)
    for j in range(top_k):
        taken += jnp.where(ids[:, j:j + 1] == experts, 1.0, 0.0)
    rank = dot(lower, taken.astype(BF16)) - 1.0
    return jnp.where(taken > 0.5, rank, -10000.0)


def slot_matrix(code, device):
    tokens = code.shape[0]
    code = pltpu.roll(code, (128 - NE * device) % 128, 1)
    lane = lax.broadcasted_iota(jnp.int32, (tokens, 128), 1).astype(F32)
    blocks = []
    for b in range(NE * CAP // 128):
        hit = None
        for e in range(NE):
            if e * CAP < (b + 1) * 128 and (e + 1) * CAP > b * 128:
                eq = lane == code[:, e:e + 1] + float(e * CAP - b * 128)
                hit = eq if hit is None else hit | eq
        blocks.append(jnp.where(hit, 1.0, 0.0).astype(BF16))
    return jnp.concatenate(blocks, axis=1)


def collect_kernel(tok_ref, c_ref, back_ref, rows_ref,
                   y_ref, dx_ref,
                   ybuf, rbuf, acc, part_out, part_in, out_buf, y_buf,
                   ysem, osem, ssem, rsem, psem, prsem, zsem, zrsem):
    stage = lax.axis_index('stage')
    me = lax.axis_index('expert')
    core = me % 2
    sib_of = lambda h: h + 1 - 2 * (h % 2)
    sib = sib_of(me)
    xn = me + 2 - 4 * ((me // 2) % 2)
    yn = me + 4 - 8 * (me // 4)
    dg = xn + 4 - 8 * (xn // 4)
    partner = yn + core * (xn - yn)
    line = xn + core * (yn - xn)
    line0 = 2 * (line // 2)
    tokens, dim = acc.shape
    pieces, piece = part_out.shape[:2]
    tchunk = 256
    per_chunk = tchunk // piece

    barrier = pltpu.get_barrier_semaphore()
    for peer in ((1 - stage, me), (stage, sib), (stage, xn), (stage, yn), (stage, sib_of(xn)),
                 (stage, sib_of(yn))):
        pl.semaphore_signal(barrier, inc=1, device_id=peer, device_id_type=MESH)
    pl.semaphore_wait(barrier, 6)

    targets = ((2 * (xn // 2), 2 * (dg // 2), 1 + core), (2 * (yn // 2) + 1, 2 * (dg // 2) + 1, 1 + core),
               (sib, sib_of(xn) + core * (sib_of(yn) - sib_of(xn)), 0))
    sends = []
    for role in range(2):
        for k, (target, via, slot) in enumerate(targets):
            sends.append(pltpu.make_async_remote_copy(
                src_ref=rows_ref.at[via if role == 0 else target], dst_ref=rbuf.at[role, slot],
                send_sem=ssem.at[role, k], recv_sem=rsem.at[role, slot],
                device_id=(stage, target), device_id_type=MESH))
            sends[-1].start()
    own = [pltpu.make_async_copy(rows_ref.at[h], rbuf.at[role, 3], osem.at[role])
           for role, h in enumerate((partner, me))]
    for copy in own:
        copy.start()

    def arrived(role, slot):
        pltpu.make_async_remote_copy(
            src_ref=rows_ref.at[me], dst_ref=rbuf.at[role, slot], send_sem=ssem.at[role, 0],
            recv_sem=rsem.at[role, slot], device_id=(stage, sib), device_id_type=MESH).wait_recv()

    def y_fetch(k):
        src = c_ref if k == 0 else back_ref
        return pltpu.make_async_copy(src.at[(me + k) % NG], ybuf.at[k % 2], ysem.at[k % 2])

    y_fetch(0).start()

    def rows_of(ref):
        return ref.reshape(NE * CAP, dim)

    def y_part(k):
        if k + 1 < NG:
            y_fetch(k + 1).start()
        y_fetch(k).wait()
        part = dot(slot_matrix(tok_ref[0], (me + k) % NG), rows_of(ybuf[k % 2]))
        acc[...] = part if k == 0 else acc[...] + part

    sources = (sib, line0, line0 + 1, me)

    def partial_copy(i):
        return pltpu.make_async_remote_copy(
            src_ref=part_out.at[i], dst_ref=part_in.at[i], send_sem=psem.at[i], recv_sem=prsem.at[i],
            device_id=(stage, partner), device_id_type=MESH)

    def z_copy(i):
        return pltpu.make_async_remote_copy(
            src_ref=out_buf.at[i], dst_ref=dx_ref.at[pl.ds(i * piece, piece)], send_sem=zsem.at[i],
            recv_sem=zrsem.at[i], device_id=(1 - stage, me), device_id_type=MESH)

    def combine(table, role, chunk):
        toks = pl.ds(chunk * tchunk, tchunk)
        code = tok_ref[table, toks]
        total = None
        for slot, d in enumerate(sources):
            part = dot(slot_matrix(code, d), rows_of(rbuf[role, slot]))
            total = part if total is None else total + part
        return total

    for k in range(0, 5):
        y_part(k)
    for slot in range(3):
        arrived(0, slot)
    own[0].wait()

    @pl.loop(0, tokens // tchunk)
    def _(chunk):
        total = combine(1, 0, chunk)
        for p in range(per_chunk):
            part_out[chunk * per_chunk + p] = total[p * piece:(p + 1) * piece]
        for p in range(per_chunk):
            partial_copy(chunk * per_chunk + p).start()

    for k in range(5, NG):
        y_part(k)
    y_buf[...] = acc[...].astype(BF16)
    y_out = pltpu.make_async_copy(y_buf, y_ref, osem.at[0])
    y_out.start()
    for slot in range(3):
        arrived(1, slot)
    own[1].wait()

    @pl.loop(0, tokens // tchunk)
    def _(chunk):
        total = combine(2, 1, chunk)
        for p in range(per_chunk):
            i = chunk * per_chunk + p
            partial_copy(i).wait_recv()
            out_buf[i] = (total[p * piece:(p + 1) * piece] + part_in[i]).astype(BF16)
            z_copy(i).start()

    y_out.wait()
    for copy in sends:
        copy.wait_send()

    @pl.loop(0, pieces)
    def _(i):
        partial_copy(i).wait_send()
        z_copy(i).wait()


def run_collect(tok, c_rows, y_back, dx_rows):
    tokens = tok.shape[1]
    dim = c_rows.shape[3]
    pieces = 16
    any_spec = pl.BlockSpec(memory_space=pl.ANY)
    return pl.pallas_call(
        collect_kernel,
        name='collect',
        out_shape=(jax.ShapeDtypeStruct((tokens, dim), BF16), jax.ShapeDtypeStruct((tokens, dim), BF16)),
        in_specs=[pl.BlockSpec(memory_space=pltpu.VMEM)] + [any_spec] * 3,
        out_specs=[any_spec] * 2,
        scratch_shapes=[
            pltpu.VMEM((2, NE, CAP, dim), BF16),
            pltpu.VMEM((2, 4, NE, CAP, dim), BF16),
            pltpu.VMEM((tokens, dim), F32),
            pltpu.VMEM((pieces, tokens // pieces, dim), F32),
            pltpu.VMEM((pieces, tokens // pieces, dim), F32),
            pltpu.VMEM((pieces, tokens // pieces, dim), BF16),
            pltpu.VMEM((tokens, dim), BF16),
            pltpu.SemaphoreType.DMA((2,)),
            pltpu.SemaphoreType.DMA((2,)),
            pltpu.SemaphoreType.DMA((2, 3)),
            pltpu.SemaphoreType.DMA((2, 3)),
            pltpu.SemaphoreType.DMA((pieces,)),
            pltpu.SemaphoreType.DMA((pieces,)),
            pltpu.SemaphoreType.DMA((pieces,)),
            pltpu.SemaphoreType.DMA((pieces,)),
        ],
        cost_estimate=pl.CostEstimate(flops=4 * tokens * NG * NE * CAP * dim,
                                      bytes_accessed=20_000_000, transcendentals=0),
        compiler_params=pltpu.CompilerParams(collective_id=2, has_side_effects=True,
                                             vmem_limit_bytes=64_000_000),
    )(tok, c_rows, y_back, dx_rows)


def solution(mesh):
    def device_fn(x_acts, expert_ids, gate_wts, w_in, w_up, w_out, d_out):
        dim = x_acts.shape[3]
        ids_t = jnp.swapaxes(expert_ids[:, 0], 1, 2).astype(F32)
        gates_t = jnp.swapaxes(gate_wts[:, 0], 1, 2)
        table = jnp.concatenate([ids_t[1], gates_t[1], ids_t[0], gates_t[0]], axis=0)

        c_rows, xb, q_rows, code, tok = run_dispatch(x_acts, d_out, table, w_in, w_up, w_out)
        y_back = lax.all_to_all(c_rows.reshape(NG, NE * CAP, dim), 'expert', 0, 0, tiled=True)
        dx_rows, dw_in, dw_up, dw_out = run_backward(code, xb, q_rows, w_in, w_up, w_out)
        y_back = y_back.reshape(c_rows.shape)
        y_dev, dx_dev = run_collect(tok, c_rows, y_back, dx_rows)
        return y_dev[None], dx_dev[None], dw_in, dw_up, dw_out

    tok_spec = P(None, 'stage', 'expert', None)
    w_spec = P('stage', 'expert', None, None)
    row_spec = P('stage', 'expert', None)
    return jax.shard_map(device_fn, mesh=mesh,
                         in_specs=(tok_spec, tok_spec, tok_spec, w_spec, w_spec, w_spec, row_spec),
                         out_specs=(row_spec, row_spec, w_spec, w_spec, w_spec), check_vma=False)
```

```python
import jax
import jax.numpy as jnp
from jax import lax
from jax.experimental import pallas as pl
from jax.experimental.pallas import tpu as pltpu
from jax.sharding import PartitionSpec as P

MESH = pl.DeviceIdType.MESH
F32, BF16 = jnp.float32, jnp.bfloat16
DY, XF, XB, IDS, GTS = 0, 1, 2, 3, 4
NG, NE, CAP = 8, 4, 192


def dot(lhs, rhs, dims=((1,), (0,))):
    return lax.dot_general(lhs, rhs, (dims, ((), ())), preferred_element_type=F32)


def slot_hits(code_rows, tokens):
    slot = lax.broadcasted_iota(jnp.int32, (CAP, tokens), 0).astype(F32)
    return [slot == code_rows[e:e + 1, :] for e in range(NE)]


def dispatch_kernel(x_ref, dy_ref, ids_ref, gts_ref, win_ref, wup_ref, wout_ref,
                    c_ref, xb_ref, q_ref, code_ref, tok_ref,
                    buf, tab_ids, tab_gts, codes, gates, gslot, xs, st, cst, wbuf, tok,
                    ssem, rsem, lsem, wsem, stsem, csem, tsem):
    stage = lax.axis_index('stage')
    me = lax.axis_index('expert')
    other = 1 - stage
    core = me % 2
    xn = me + 2 - 4 * ((me // 2) % 2)
    yn = me + 4 - 8 * (me // 4)
    dg = xn + 4 - 8 * (xn // 4)
    sib_of = lambda h: h + 1 - 2 * core
    sib = sib_of(me)
    tokens = x_ref.shape[2]
    half = tokens // 2
    sends = []

    barrier = pltpu.get_barrier_semaphore()
    for peer in ((other, me), (stage, sib), (stage, xn), (stage, yn)):
        pl.semaphore_signal(barrier, inc=1, device_id=peer, device_id_type=MESH)
    pl.semaphore_wait(barrier, 4)

    def place(arr, h, part):
        if arr == IDS:
            return tab_ids.at[h]
        if arr == GTS:
            return tab_gts.at[h]
        if arr == XB:
            return xb_ref.at[h, pl.ds(part * half, half)]
        return buf.at[arr, h, pl.ds(part * half, half)]

    def remote(arr, h, part, slot, peer, src=None):
        return pltpu.make_async_remote_copy(
            src_ref=place(arr, h, part) if src is None else src, dst_ref=place(arr, h, part),
            send_sem=ssem.at[arr, slot], recv_sem=rsem.at[arr, h, part],
            device_id=peer, device_id_type=MESH)

    def send(arr, h, part, slot, peer, src=None):
        remote(arr, h, part, slot, peer, src).start()
        sends.append((arr, h, part, slot, peer, src))

    def arrived(arr, h, part):
        remote(arr, h, part, 0, (stage, sib)).wait_recv()

    to_x, to_y, to_sib, to_z = (stage, xn), (stage, yn), (stage, sib), (other, me)

    send(IDS, me, 0, 14, to_z, ids_ref)
    send(GTS, me, 0, 14, to_z, gts_ref)
    for part in range(2):
        send(XF, me, part, 14 + part, to_z, x_ref.at[1, 0, pl.ds(part * half, half)])
    for part in range(2):
        send(XB, me, part, 14 + part, to_z, x_ref.at[0, 0, pl.ds(part * half, half)])
    dy_half = lambda part: dy_ref.at[0, pl.ds(part * half, half)]
    send(DY, me, 0, 0, to_x, dy_half(0))
    send(DY, me, 1, 2, to_y, dy_half(1))
    send(DY, me, 0, 4, to_sib, dy_half(0))
    send(DY, me, 1, 5, to_sib, dy_half(1))
    own_dy = pltpu.make_async_copy(dy_ref.at[0], buf.at[DY, me], lsem)
    own_dy.start()

    def weights(e):
        return [pltpu.make_async_copy(w.at[0, e], wbuf.at[e % 2, k], wsem.at[e % 2, k])
                for k, w in enumerate((win_ref, wup_ref, wout_ref))]

    for e in range(2):
        for copy in weights(e):
            copy.start()

    for arr in (IDS, GTS):
        arrived(arr, me, 0)
        send(arr, me, 0, 0, to_x)
        send(arr, me, 0, 2, to_y)
        send(arr, me, 0, 4, to_sib)
    send(DY, me, 1, 1, to_x, dy_half(1))
    send(DY, me, 0, 3, to_y, dy_half(0))

    def first_halves(arr):
        arrived(arr, xn, 0)
        arrived(arr, yn, 1)
        send(arr, xn, 0, 6, to_y)
        send(arr, yn, 1, 7, to_x)
        send(arr, xn, 0, 8, to_sib)
        send(arr, yn, 1, 11, to_sib)

    def second_halves(arr):
        arrived(arr, xn, 1)
        arrived(arr, yn, 0)
        send(arr, xn, 1, 9, to_sib)
        send(arr, yn, 0, 10, to_sib)

    def diagonal(arr):
        for part in range(2):
            arrived(arr, dg, part)
            send(arr, dg, part, 12 + part, to_sib)

    def own_sends(arr):
        for part in range(2):
            arrived(arr, me, part)
        send(arr, me, 0, 0, to_x)
        send(arr, me, 1, 2, to_y)
        send(arr, me, 1, 1, to_x)
        send(arr, me, 0, 3, to_y)
        send(arr, me, 0, 4, to_sib)
        send(arr, me, 1, 5, to_sib)

    for arr in (IDS, GTS):
        arrived(arr, xn, 0)
        arrived(arr, yn, 0)
        send(arr, xn, 0, 6, to_y)
    first_halves(DY)
    for arr in (IDS, GTS):
        send(arr, xn, 0, 8, to_sib)
        send(arr, yn, 0, 10, to_sib)
    own_sends(XF)
    second_halves(DY)
    for arr in (IDS, GTS):
        arrived(arr, dg, 0)
        send(arr, dg, 0, 12, to_sib)
        for h in (sib, sib_of(xn), sib_of(yn), sib_of(dg)):
            arrived(arr, h, 0)

    upper = (lax.broadcasted_iota(jnp.int32, (tokens, tokens), 0)
             <= lax.broadcasted_iota(jnp.int32, (tokens, tokens), 1)).astype(F32).astype(BF16)
    for kind in range(2):
        taken = []
        for h in range(NG):
            for e in range(NE):
                eq = tab_ids[h, 1 - kind] == me * NE + e
                taken.append(jnp.sum(jnp.where(eq, 1.0, 0.0), axis=0, keepdims=True))
                gates[kind, h, e:e + 1, :] = jnp.sum(jnp.where(eq, tab_gts[h, 1 - kind], 0.0), axis=0,
                                                     keepdims=True)
        taken = jnp.concatenate(taken, axis=0)
        rank = dot(taken.astype(BF16), upper) - 1.0
        code = jnp.where(taken > 0.5, rank, -1.0)
        for h in range(NG):
            codes[kind, h, 0:NE, :] = code[h * NE:(h + 1) * NE, :]
            codes[kind, h, NE:8, :] = jnp.full((8 - NE, tokens), -1.0, F32)
    code_copy = pltpu.make_async_copy(codes.at[1], code_ref, tsem.at[0])
    code_copy.start()

    partner = yn + core * (xn - yn)
    lower = (lax.broadcasted_iota(jnp.int32, (tokens, tokens), 0)
             >= lax.broadcasted_iota(jnp.int32, (tokens, tokens), 1)).astype(F32).astype(BF16)
    for n, (h, kind) in enumerate(((me, 1), (partner, 0), (me, 0))):
        both = jnp.concatenate([tab_ids[h, 0], tab_ids[h, 1]], axis=0).astype(F32)
        tok[n] = token_codes(both.T[:, 4 * kind:4 * kind + 4], lower)
    tok_copy = pltpu.make_async_copy(tok, tok_ref, tsem.at[1])
    tok_copy.start()

    def shard(i):
        j, odd = i // 2, i % 2
        return me + (j % 2) * (xn - me) + (j // 2) * (yn - me) + odd * (1 - 2 * core)

    def gather(kind, arr, h):
        hits = slot_hits(codes[kind, h], tokens)
        gate_rows = gates[kind, h]
        onehot = jnp.concatenate([jnp.where(hit, 1.0, 0.0).astype(BF16) for hit in hits], axis=0)
        slot_gate = [jnp.sum(jnp.where(hits[e], gate_rows[e:e + 1, :], 0.0), axis=1, keepdims=True)
                     for e in range(NE)]
        return dot(onehot, buf[arr, h]), slot_gate

    def q_copy(slot, h):
        return pltpu.make_async_copy(st.at[slot], q_ref.at[:, h], stsem.at[slot])

    def sibling_part(arr, i):
        @pl.when(i % 2 == 1)
        def _():
            arrived(arr, shard(i), 0)
            arrived(arr, shard(i), 1)

    own_dy.wait()

    @pl.loop(0, NG)
    def _(i):
        pl.when(i == 6)(lambda: diagonal(DY))
        sibling_part(DY, i)
        h, slot = shard(i), i % 2
        pl.when(i >= 2)(lambda: q_copy(slot, h).wait())
        rows, slot_gate = gather(1, DY, h)
        for e in range(NE):
            st[slot, e] = (slot_gate[e] * rows[e * CAP:(e + 1) * CAP]).astype(BF16)
        q_copy(slot, h).start()

    first_halves(XF)
    own_sends(XB)

    @pl.loop(0, NG)
    def _(i):
        pl.when(i == 2)(lambda: second_halves(XF))
        pl.when(i == 6)(lambda: diagonal(XF))
        sibling_part(XF, i)
        h = shard(i)
        rows, slot_gate = gather(0, XF, h)
        for e in range(NE):
            xs[e, h] = rows[e * CAP:(e + 1) * CAP].astype(BF16)
            gslot[e, h] = jnp.broadcast_to(slot_gate[e], (CAP, 128))

    chunk = 2
    steps = NG // chunk
    rows_chunk = chunk * CAP

    def c_copy(slot, e, h0):
        return pltpu.make_async_copy(cst.at[slot], c_ref.at[pl.ds(h0, chunk), e], csem.at[slot])

    @pl.loop(0, NE)
    def _(e):
        pl.when(e == 1)(lambda: first_halves(XB))
        pl.when(e == 3)(lambda: second_halves(XB))
        for copy in weights(e):
            copy.wait()

        @pl.loop(0, steps)
        def _(i):
            slot = i % 2
            h0 = i * chunk
            rows = xs[e, pl.ds(h0, chunk)].reshape(rows_chunk, -1)
            pre = dot(rows, wbuf[e % 2, 0])
            act = pre * jax.nn.sigmoid(pre)
            hidden = (act * dot(rows, wbuf[e % 2, 1])).astype(BF16)
            out = dot(hidden, wbuf[e % 2, 2])
            gate = gslot[e, pl.ds(h0, chunk)].reshape(rows_chunk, 128)[:, 0:1]
            pl.when(e * steps + i >= 2)(lambda: c_copy(slot, e, h0).wait())
            cst[slot] = (gate * out).astype(BF16).reshape(chunk, CAP, -1)
            c_copy(slot, e, h0).start()

        @pl.when(e + 2 < NE)
        def _():
            for copy in weights(e + 2):
                copy.start()

    diagonal(XB)
    for h in (sib, sib_of(xn), sib_of(yn), sib_of(dg)):
        arrived(XB, h, 0)
        arrived(XB, h, 1)
    for slot in range(2):
        c_copy(slot, NE - 1, 0).wait()
        q_copy(slot, 0).wait()
    code_copy.wait()
    tok_copy.wait()
    for args in sends:
        remote(*args).wait_send()


def run_dispatch(x_acts, d_out, ids, gts, w_in, w_up, w_out):
    tokens, dim = x_acts.shape[2:]
    hid = w_in.shape[3]
    any_spec = pl.BlockSpec(memory_space=pl.ANY)
    flops = 2 * NG * NE * CAP * (2 * tokens * dim + 3 * dim * hid)
    return pl.pallas_call(
        dispatch_kernel,
        name='dispatch',
        out_shape=(jax.ShapeDtypeStruct((NG, NE, CAP, dim), BF16),
                   jax.ShapeDtypeStruct((NG, tokens, dim), BF16),
                   jax.ShapeDtypeStruct((NE, NG, CAP, dim), BF16),
                   jax.ShapeDtypeStruct((NG, 8, tokens), F32),
                   jax.ShapeDtypeStruct((3, tokens, 128), F32)),
        in_specs=[any_spec] * 7,
        out_specs=[any_spec] * 5,
        scratch_shapes=[
            pltpu.VMEM((2, NG, tokens, dim), BF16),
            pltpu.VMEM((NG, 2, 4, tokens), jnp.int32),
            pltpu.VMEM((NG, 2, 4, tokens), F32),
            pltpu.VMEM((2, NG, 8, tokens), F32),
            pltpu.VMEM((2, NG, 8, tokens), F32),
            pltpu.VMEM((NE, NG, CAP, 128), F32),
            pltpu.VMEM((NE, NG, CAP, dim), BF16),
            pltpu.VMEM((2, NE, CAP, dim), BF16),
            pltpu.VMEM((2, 2, CAP, dim), BF16),
            pltpu.VMEM((2, 3, dim, hid), BF16),
            pltpu.VMEM((3, tokens, 128), F32),
            pltpu.SemaphoreType.DMA((5, 16)),
            pltpu.SemaphoreType.DMA((5, NG, 2)),
            pltpu.SemaphoreType.DMA,
            pltpu.SemaphoreType.DMA((2, 3)),
            pltpu.SemaphoreType.DMA((2,)),
            pltpu.SemaphoreType.DMA((2,)),
            pltpu.SemaphoreType.DMA((2,)),
        ],
        cost_estimate=pl.CostEstimate(flops=flops, bytes_accessed=60_000_000, transcendentals=0),
        compiler_params=pltpu.CompilerParams(collective_id=0, has_side_effects=True,
                                             vmem_limit_bytes=67_043_328),
    )(x_acts, d_out, ids, gts, w_in, w_up, w_out)


def backward_kernel(code_ref, xb_ref, q_ref, win_ref, wup_ref, wout_ref,
                    dx_ref, dwin_ref, dwup_ref, dwout_ref,
                    xs, acc_in, acc_up, acc_out):
    step = pl.program_id(0)
    tokens, dim = xb_ref.shape[1:]

    @pl.when(step < NG)
    def _():
        hits = slot_hits(code_ref[0], tokens)
        onehot = jnp.concatenate([jnp.where(hit, 1.0, 0.0).astype(BF16) for hit in hits], axis=0)
        rows = dot(onehot, xb_ref[0]).astype(BF16)
        for e in range(NE):
            xs[e, step] = rows[e * CAP:(e + 1) * CAP]

    @pl.when(step >= NG)
    def _():
        e = step - NG
        chunk = 4
        rows_chunk = chunk * CAP

        def body(i):
            hs = pl.ds(i * chunk, chunk)
            x = xs[e, hs].reshape(rows_chunk, dim)
            q = q_ref[0, hs].reshape(rows_chunk, dim)
            pre_in = dot(x, win_ref[0, 0])
            pre_up = dot(x, wup_ref[0, 0])
            d_hid = dot(q, wout_ref[0, 0], ((1,), (1,)))
            sig = jax.nn.sigmoid(pre_in)
            act = pre_in * sig
            hidden = (act * pre_up).astype(BF16)
            d_in = (d_hid * pre_up * sig * (1.0 + pre_in * (1.0 - sig))).astype(BF16)
            d_up = (d_hid * act).astype(BF16)
            dx = dot(d_in, win_ref[0, 0], ((1,), (1,))) + dot(d_up, wup_ref[0, 0], ((1,), (1,)))
            dx_ref[hs, 0] = dx.astype(BF16).reshape(chunk, CAP, dim)
            return (dot(x, d_in, ((0,), (0,))), dot(x, d_up, ((0,), (0,))),
                    dot(hidden, q, ((0,), (0,))))

        steps = NG // chunk

        def loop(i, carry):
            parts = body(i)
            first = i == 0
            for acc, part in zip((acc_in, acc_up, acc_out), parts):
                acc[...] = jnp.where(first, part, acc[...] + part)
            return carry

        lax.fori_loop(0, steps, loop, 0)
        dwin_ref[0, 0] = acc_in[...].astype(BF16)
        dwup_ref[0, 0] = acc_up[...].astype(BF16)
        dwout_ref[0, 0] = acc_out[...].astype(BF16)


def run_backward(code, xb, q, w_in, w_up, w_out):
    tokens, dim = xb.shape[1:]
    hid = w_in.shape[3]
    exp = lambda i: jnp.maximum(i - NG, 0)
    src = lambda i: jnp.minimum(i, NG - 1)
    w_spec = lambda rows, cols: pl.BlockSpec((1, 1, rows, cols), lambda i: (0, exp(i), 0, 0))
    flops = 2 * NG * NE * CAP * (tokens * dim + 8 * dim * hid)
    return pl.pallas_call(
        backward_kernel,
        name='backward',
        grid=(NG + NE,),
        out_shape=(jax.ShapeDtypeStruct((NG, NE, CAP, dim), BF16),
                   jax.ShapeDtypeStruct(w_in.shape, BF16),
                   jax.ShapeDtypeStruct(w_up.shape, BF16),
                   jax.ShapeDtypeStruct(w_out.shape, BF16)),
        in_specs=[pl.BlockSpec((1, 8, tokens), lambda i: (src(i), 0, 0)),
                  pl.BlockSpec((1, tokens, dim), lambda i: (src(i), 0, 0)),
                  pl.BlockSpec((1, NG, CAP, dim), lambda i: (exp(i), 0, 0, 0)),
                  w_spec(dim, hid), w_spec(dim, hid), w_spec(hid, dim)],
        out_specs=[pl.BlockSpec((NG, 1, CAP, dim), lambda i: (0, exp(i), 0, 0)),
                   w_spec(dim, hid), w_spec(dim, hid), w_spec(hid, dim)],
        scratch_shapes=[pltpu.VMEM((NE, NG, CAP, dim), BF16),
                        pltpu.VMEM((dim, hid), F32), pltpu.VMEM((dim, hid), F32),
                        pltpu.VMEM((hid, dim), F32)],
        cost_estimate=pl.CostEstimate(flops=flops, bytes_accessed=60_000_000, transcendentals=0),
        compiler_params=pltpu.CompilerParams(dimension_semantics=('arbitrary',),
                                             vmem_limit_bytes=64_000_000),
    )(code, xb, q, w_in, w_up, w_out)


def token_codes(ids, lower):
    tokens, top_k = ids.shape
    experts = lax.broadcasted_iota(jnp.int32, (tokens, 128), 1).astype(F32)
    taken = jnp.zeros((tokens, 128), F32)
    for j in range(top_k):
        taken += jnp.where(ids[:, j:j + 1] == experts, 1.0, 0.0)
    rank = dot(lower, taken.astype(BF16)) - 1.0
    return jnp.where(taken > 0.5, rank, -10000.0)


def slot_matrix(code, device):
    tokens = code.shape[0]
    code = pltpu.roll(code, (128 - NE * device) % 128, 1)
    lane = lax.broadcasted_iota(jnp.int32, (tokens, 128), 1).astype(F32)
    blocks = []
    for b in range(NE * CAP // 128):
        hit = None
        for e in range(NE):
            if e * CAP < (b + 1) * 128 and (e + 1) * CAP > b * 128:
                eq = lane == code[:, e:e + 1] + float(e * CAP - b * 128)
                hit = eq if hit is None else hit | eq
        blocks.append(jnp.where(hit, 1.0, 0.0).astype(BF16))
    return jnp.concatenate(blocks, axis=1)


def collect_kernel(tok_ref, back_ref, rows_ref,
                   y_ref, dx_ref,
                   ybuf, rbuf, acc, part_out, part_in, out_buf, y_buf,
                   ysem, osem, ssem, rsem, psem, prsem, zsem, zrsem):
    stage = lax.axis_index('stage')
    me = lax.axis_index('expert')
    core = me % 2
    sib_of = lambda h: h + 1 - 2 * (h % 2)
    sib = sib_of(me)
    xn = me + 2 - 4 * ((me // 2) % 2)
    yn = me + 4 - 8 * (me // 4)
    dg = xn + 4 - 8 * (xn // 4)
    partner = yn + core * (xn - yn)
    line = xn + core * (yn - xn)
    line0 = 2 * (line // 2)
    tokens, dim = acc.shape
    pieces, piece = part_out.shape[:2]
    tchunk = 256
    per_chunk = tchunk // piece

    barrier = pltpu.get_barrier_semaphore()
    for peer in ((1 - stage, me), (stage, sib), (stage, xn), (stage, yn), (stage, sib_of(xn)),
                 (stage, sib_of(yn))):
        pl.semaphore_signal(barrier, inc=1, device_id=peer, device_id_type=MESH)
    pl.semaphore_wait(barrier, 6)

    targets = ((2 * (xn // 2), 2 * (dg // 2), 1 + core), (2 * (yn // 2) + 1, 2 * (dg // 2) + 1, 1 + core),
               (sib, sib_of(xn) + core * (sib_of(yn) - sib_of(xn)), 0))
    sends = []
    for role in range(2):
        for k, (target, via, slot) in enumerate(targets):
            sends.append(pltpu.make_async_remote_copy(
                src_ref=rows_ref.at[via if role == 0 else target], dst_ref=rbuf.at[role, slot],
                send_sem=ssem.at[role, k], recv_sem=rsem.at[role, slot],
                device_id=(stage, target), device_id_type=MESH))
            sends[-1].start()
    own = [pltpu.make_async_copy(rows_ref.at[h], rbuf.at[role, 3], osem.at[role])
           for role, h in enumerate((partner, me))]
    for copy in own:
        copy.start()

    def arrived(role, slot):
        pltpu.make_async_remote_copy(
            src_ref=rows_ref.at[me], dst_ref=rbuf.at[role, slot], send_sem=ssem.at[role, 0],
            recv_sem=rsem.at[role, slot], device_id=(stage, sib), device_id_type=MESH).wait_recv()

    def y_fetch(k):
        return pltpu.make_async_copy(back_ref.at[(me + k) % NG], ybuf.at[k % 2], ysem.at[k % 2])

    y_fetch(0).start()
    acc[...] = jnp.zeros_like(acc)

    def rows_of(ref):
        return ref.reshape(NE * CAP, dim)

    def y_part(k):
        pl.when(k + 1 < NG)(lambda: y_fetch(k + 1).start())
        y_fetch(k).wait()
        acc[...] += dot(slot_matrix(tok_ref[0], (me + k) % NG), rows_of(ybuf[k % 2]))

    sources = (sib, line0, line0 + 1, me)

    def partial_copy(i):
        return pltpu.make_async_remote_copy(
            src_ref=part_out.at[i], dst_ref=part_in.at[i], send_sem=psem.at[i], recv_sem=prsem.at[i],
            device_id=(stage, partner), device_id_type=MESH)

    def z_copy(i):
        return pltpu.make_async_remote_copy(
            src_ref=out_buf.at[i], dst_ref=dx_ref.at[pl.ds(i * piece, piece)], send_sem=zsem.at[i],
            recv_sem=zrsem.at[i], device_id=(1 - stage, me), device_id_type=MESH)

    def combine(table, role, chunk):
        toks = pl.ds(chunk * tchunk, tchunk)
        code = tok_ref[table, toks]
        total = None
        for slot, d in enumerate(sources):
            part = dot(slot_matrix(code, d), rows_of(rbuf[role, slot]))
            total = part if total is None else total + part
        return total

    pl.loop(0, 5)(y_part)
    for slot in range(3):
        arrived(0, slot)
    own[0].wait()

    @pl.loop(0, tokens // tchunk)
    def _(chunk):
        total = combine(1, 0, chunk)
        for p in range(per_chunk):
            part_out[chunk * per_chunk + p] = total[p * piece:(p + 1) * piece]
        for p in range(per_chunk):
            partial_copy(chunk * per_chunk + p).start()

    pl.loop(5, NG)(y_part)
    y_buf[...] = acc[...].astype(BF16)
    y_out = pltpu.make_async_copy(y_buf, y_ref, osem.at[0])
    y_out.start()
    for slot in range(3):
        arrived(1, slot)
    own[1].wait()

    @pl.loop(0, tokens // tchunk)
    def _(chunk):
        total = combine(2, 1, chunk)
        for p in range(per_chunk):
            i = chunk * per_chunk + p
            partial_copy(i).wait_recv()
            out_buf[i] = (total[p * piece:(p + 1) * piece] + part_in[i]).astype(BF16)
            z_copy(i).start()

    y_out.wait()
    for copy in sends:
        copy.wait_send()

    @pl.loop(0, pieces)
    def _(i):
        partial_copy(i).wait_send()
        z_copy(i).wait()


def run_collect(tok, y_back, dx_rows):
    tokens = tok.shape[1]
    dim = dx_rows.shape[3]
    pieces = 16
    any_spec = pl.BlockSpec(memory_space=pl.ANY)
    return pl.pallas_call(
        collect_kernel,
        name='collect',
        out_shape=(jax.ShapeDtypeStruct((tokens, dim), BF16), jax.ShapeDtypeStruct((tokens, dim), BF16)),
        in_specs=[pl.BlockSpec(memory_space=pltpu.VMEM)] + [any_spec] * 2,
        out_specs=[any_spec] * 2,
        scratch_shapes=[
            pltpu.VMEM((2, NE, CAP, dim), BF16),
            pltpu.VMEM((2, 4, NE, CAP, dim), BF16),
            pltpu.VMEM((tokens, dim), F32),
            pltpu.VMEM((pieces, tokens // pieces, dim), F32),
            pltpu.VMEM((pieces, tokens // pieces, dim), F32),
            pltpu.VMEM((pieces, tokens // pieces, dim), BF16),
            pltpu.VMEM((tokens, dim), BF16),
            pltpu.SemaphoreType.DMA((2,)),
            pltpu.SemaphoreType.DMA((2,)),
            pltpu.SemaphoreType.DMA((2, 3)),
            pltpu.SemaphoreType.DMA((2, 3)),
            pltpu.SemaphoreType.DMA((pieces,)),
            pltpu.SemaphoreType.DMA((pieces,)),
            pltpu.SemaphoreType.DMA((pieces,)),
            pltpu.SemaphoreType.DMA((pieces,)),
        ],
        cost_estimate=pl.CostEstimate(flops=4 * tokens * NG * NE * CAP * dim,
                                      bytes_accessed=20_000_000, transcendentals=0),
        compiler_params=pltpu.CompilerParams(collective_id=2, has_side_effects=True,
                                             vmem_limit_bytes=64_000_000),
    )(tok, y_back, dx_rows)


def solution(mesh):
    def device_fn(x_acts, expert_ids, gate_wts, w_in, w_up, w_out, d_out):
        dim = x_acts.shape[3]
        ids_t = jnp.swapaxes(expert_ids[:, 0], 1, 2)
        gates_t = jnp.swapaxes(gate_wts[:, 0], 1, 2)
        c_rows, xb, q_rows, code, tok = run_dispatch(x_acts, d_out, ids_t, gates_t, w_in, w_up, w_out)
        y_back = lax.all_to_all(c_rows.reshape(NG, NE * CAP, dim), 'expert', 0, 0, tiled=True)
        dx_rows, dw_in, dw_up, dw_out = run_backward(code, xb, q_rows, w_in, w_up, w_out)
        y_back = y_back.reshape(c_rows.shape)
        y_dev, dx_dev = run_collect(tok, y_back, dx_rows)
        return y_dev[None], dx_dev[None], dw_in, dw_up, dw_out

    tok_spec = P(None, 'stage', 'expert', None)
    w_spec = P('stage', 'expert', None, None)
    row_spec = P('stage', 'expert', None)
    return jax.shard_map(device_fn, mesh=mesh,
                         in_specs=(tok_spec, tok_spec, tok_spec, w_spec, w_spec, w_spec, row_spec),
                         out_specs=(row_spec, row_spec, w_spec, w_spec, w_spec), check_vma=False)
```

```python
import jax
import jax.numpy as jnp
from jax import lax
from jax.experimental import pallas as pl
from jax.experimental.pallas import tpu as pltpu
from jax.sharding import PartitionSpec as P

MESH = pl.DeviceIdType.MESH
F32, BF16 = jnp.float32, jnp.bfloat16
DY, XF, XB, IDS, GTS = 0, 1, 2, 3, 4
NG, NE, CAP = 8, 4, 192


def dot(lhs, rhs, dims=((1,), (0,))):
    return lax.dot_general(lhs, rhs, (dims, ((), ())), preferred_element_type=F32)


def slot_hits(code_rows, tokens):
    slot = lax.broadcasted_iota(jnp.int32, (CAP, tokens), 0).astype(F32)
    return [slot == code_rows[e:e + 1, :] for e in range(NE)]


def dispatch_kernel(x_ref, dy_ref, ids_ref, gts_ref, win_ref, wup_ref, wout_ref,
                    c_ref, xb_ref, q_ref, code_ref, tok_ref,
                    buf, tab_ids, tab_gts, codes, gates, gslot, xs, st, cst, wbuf, tok,
                    ssem, rsem, lsem, wsem, stsem, csem, tsem):
    stage = lax.axis_index('stage')
    me = lax.axis_index('expert')
    other = 1 - stage
    core = me % 2
    xn = me + 2 - 4 * ((me // 2) % 2)
    yn = me + 4 - 8 * (me // 4)
    dg = xn + 4 - 8 * (xn // 4)
    sib_of = lambda h: h + 1 - 2 * core
    sib = sib_of(me)
    tokens = x_ref.shape[2]
    half = tokens // 2
    sends = []

    barrier = pltpu.get_barrier_semaphore()
    for peer in ((other, me), (stage, sib), (stage, xn), (stage, yn)):
        pl.semaphore_signal(barrier, inc=1, device_id=peer, device_id_type=MESH)
    pl.semaphore_wait(barrier, 4)

    def place(arr, h, part):
        if arr == IDS:
            return tab_ids.at[h]
        if arr == GTS:
            return tab_gts.at[h]
        if arr == XB:
            return xb_ref.at[h, pl.ds(part * half, half)]
        return buf.at[arr, h, pl.ds(part * half, half)]

    def remote(arr, h, part, slot, peer, src=None):
        return pltpu.make_async_remote_copy(
            src_ref=place(arr, h, part) if src is None else src, dst_ref=place(arr, h, part),
            send_sem=ssem.at[arr, slot], recv_sem=rsem.at[arr, h, part],
            device_id=peer, device_id_type=MESH)

    def send(arr, h, part, slot, peer, src=None):
        remote(arr, h, part, slot, peer, src).start()
        sends.append((arr, h, part, slot, peer, src))

    def arrived(arr, h, part):
        remote(arr, h, part, 0, (stage, sib)).wait_recv()

    to_x, to_y, to_sib, to_z = (stage, xn), (stage, yn), (stage, sib), (other, me)

    send(IDS, me, 0, 14, to_z, ids_ref)
    send(GTS, me, 0, 14, to_z, gts_ref)
    for part in range(2):
        send(XF, me, part, 14 + part, to_z, x_ref.at[1, 0, pl.ds(part * half, half)])
    for part in range(2):
        send(XB, me, part, 14 + part, to_z, x_ref.at[0, 0, pl.ds(part * half, half)])
    dy_half = lambda part: dy_ref.at[0, pl.ds(part * half, half)]
    send(DY, me, 0, 0, to_x, dy_half(0))
    send(DY, me, 1, 2, to_y, dy_half(1))
    send(DY, me, 0, 4, to_sib, dy_half(0))
    send(DY, me, 1, 5, to_sib, dy_half(1))
    own_dy = pltpu.make_async_copy(dy_ref.at[0], buf.at[DY, me], lsem)
    own_dy.start()

    def weights(e):
        return [pltpu.make_async_copy(w.at[0, e], wbuf.at[e % 2, k], wsem.at[e % 2, k])
                for k, w in enumerate((win_ref, wup_ref, wout_ref))]

    for e in range(2):
        for copy in weights(e):
            copy.start()

    for arr in (IDS, GTS):
        arrived(arr, me, 0)
        send(arr, me, 0, 0, to_x)
        send(arr, me, 0, 2, to_y)
        send(arr, me, 0, 4, to_sib)
    send(DY, me, 1, 1, to_x, dy_half(1))
    send(DY, me, 0, 3, to_y, dy_half(0))

    def first_halves(arr):
        arrived(arr, xn, 0)
        arrived(arr, yn, 1)
        send(arr, xn, 0, 6, to_y)
        send(arr, yn, 1, 7, to_x)
        send(arr, xn, 0, 8, to_sib)
        send(arr, yn, 1, 11, to_sib)

    def second_halves(arr):
        arrived(arr, xn, 1)
        arrived(arr, yn, 0)
        send(arr, xn, 1, 9, to_sib)
        send(arr, yn, 0, 10, to_sib)

    def diagonal(arr):
        for part in range(2):
            arrived(arr, dg, part)
            send(arr, dg, part, 12 + part, to_sib)

    def own_sends(arr):
        for part in range(2):
            arrived(arr, me, part)
        send(arr, me, 0, 0, to_x)
        send(arr, me, 1, 2, to_y)
        send(arr, me, 1, 1, to_x)
        send(arr, me, 0, 3, to_y)
        send(arr, me, 0, 4, to_sib)
        send(arr, me, 1, 5, to_sib)

    for arr in (IDS, GTS):
        arrived(arr, xn, 0)
        arrived(arr, yn, 0)
        send(arr, xn, 0, 6, to_y)
    first_halves(DY)
    for arr in (IDS, GTS):
        send(arr, xn, 0, 8, to_sib)
        send(arr, yn, 0, 10, to_sib)
    own_sends(XF)
    second_halves(DY)
    for arr in (IDS, GTS):
        arrived(arr, dg, 0)
        send(arr, dg, 0, 12, to_sib)
        for h in (sib, sib_of(xn), sib_of(yn), sib_of(dg)):
            arrived(arr, h, 0)

    upper = (lax.broadcasted_iota(jnp.int32, (tokens, tokens), 0)
             <= lax.broadcasted_iota(jnp.int32, (tokens, tokens), 1)).astype(F32).astype(BF16)
    for kind in range(2):
        taken = []
        for h in range(NG):
            for e in range(NE):
                eq = tab_ids[h, 1 - kind] == me * NE + e
                taken.append(jnp.sum(jnp.where(eq, 1.0, 0.0), axis=0, keepdims=True))
                gates[kind, h, e:e + 1, :] = jnp.sum(jnp.where(eq, tab_gts[h, 1 - kind], 0.0), axis=0,
                                                     keepdims=True)
        taken = jnp.concatenate(taken, axis=0)
        rank = dot(taken.astype(BF16), upper) - 1.0
        code = jnp.where(taken > 0.5, rank, -1.0)
        for h in range(NG):
            codes[kind, h, 0:NE, :] = code[h * NE:(h + 1) * NE, :]
            codes[kind, h, NE:8, :] = jnp.full((8 - NE, tokens), -1.0, F32)
    code_copy = pltpu.make_async_copy(codes.at[1], code_ref, tsem.at[0])
    code_copy.start()

    partner = yn + core * (xn - yn)
    lower = (lax.broadcasted_iota(jnp.int32, (tokens, tokens), 0)
             >= lax.broadcasted_iota(jnp.int32, (tokens, tokens), 1)).astype(F32).astype(BF16)
    for n, h in enumerate((me, partner)):
        both = jnp.concatenate([tab_ids[h, 0], tab_ids[h, 1]], axis=0).astype(F32).T
        for kind in range(2):
            tok[kind, n] = token_codes(both[:, 4 * (1 - kind):4 * (1 - kind) + 4], lower)
    tok_copy = pltpu.make_async_copy(tok, tok_ref, tsem.at[1])
    tok_copy.start()

    def shard(i):
        j, odd = i // 2, i % 2
        return me + (j % 2) * (xn - me) + (j // 2) * (yn - me) + odd * (1 - 2 * core)

    def gather(kind, arr, h):
        hits = slot_hits(codes[kind, h], tokens)
        gate_rows = gates[kind, h]
        onehot = jnp.concatenate([jnp.where(hit, 1.0, 0.0).astype(BF16) for hit in hits], axis=0)
        slot_gate = [jnp.sum(jnp.where(hits[e], gate_rows[e:e + 1, :], 0.0), axis=1, keepdims=True)
                     for e in range(NE)]
        return dot(onehot, buf[arr, h]), slot_gate

    def q_copy(slot, h):
        return pltpu.make_async_copy(st.at[slot], q_ref.at[:, h], stsem.at[slot])

    def sibling_part(arr, i):
        @pl.when(i % 2 == 1)
        def _():
            arrived(arr, shard(i), 0)
            arrived(arr, shard(i), 1)

    own_dy.wait()

    @pl.loop(0, NG)
    def _(i):
        pl.when(i == 6)(lambda: diagonal(DY))
        sibling_part(DY, i)
        h, slot = shard(i), i % 2
        pl.when(i >= 2)(lambda: q_copy(slot, h).wait())
        rows, slot_gate = gather(1, DY, h)
        for e in range(NE):
            st[slot, e] = (slot_gate[e] * rows[e * CAP:(e + 1) * CAP]).astype(BF16)
        q_copy(slot, h).start()

    first_halves(XF)
    own_sends(XB)

    @pl.loop(0, NG)
    def _(i):
        pl.when(i == 2)(lambda: second_halves(XF))
        pl.when(i == 6)(lambda: diagonal(XF))
        sibling_part(XF, i)
        h = shard(i)
        rows, slot_gate = gather(0, XF, h)
        for e in range(NE):
            xs[e, h] = rows[e * CAP:(e + 1) * CAP].astype(BF16)
            gslot[e, h] = jnp.broadcast_to(slot_gate[e], (CAP, 128))

    chunk = 2
    steps = NG // chunk
    rows_chunk = chunk * CAP

    def c_copy(slot, e, h0):
        return pltpu.make_async_copy(cst.at[slot], c_ref.at[pl.ds(h0, chunk), e], csem.at[slot])

    @pl.loop(0, NE)
    def _(e):
        pl.when(e == 1)(lambda: first_halves(XB))
        pl.when(e == 3)(lambda: second_halves(XB))
        for copy in weights(e):
            copy.wait()

        @pl.loop(0, steps)
        def _(i):
            slot = i % 2
            h0 = i * chunk
            rows = xs[e, pl.ds(h0, chunk)].reshape(rows_chunk, -1)
            pre = dot(rows, wbuf[e % 2, 0])
            act = pre * jax.nn.sigmoid(pre)
            hidden = (act * dot(rows, wbuf[e % 2, 1])).astype(BF16)
            out = dot(hidden, wbuf[e % 2, 2])
            gate = gslot[e, pl.ds(h0, chunk)].reshape(rows_chunk, 128)[:, 0:1]
            pl.when(e * steps + i >= 2)(lambda: c_copy(slot, e, h0).wait())
            cst[slot] = (gate * out).astype(BF16).reshape(chunk, CAP, -1)
            c_copy(slot, e, h0).start()

        @pl.when(e + 2 < NE)
        def _():
            for copy in weights(e + 2):
                copy.start()

    diagonal(XB)
    for h in (sib, sib_of(xn), sib_of(yn), sib_of(dg)):
        arrived(XB, h, 0)
        arrived(XB, h, 1)
    for slot in range(2):
        c_copy(slot, NE - 1, 0).wait()
        q_copy(slot, 0).wait()
    code_copy.wait()
    tok_copy.wait()
    for args in sends:
        remote(*args).wait_send()


def run_dispatch(x_acts, d_out, ids, gts, w_in, w_up, w_out):
    tokens, dim = x_acts.shape[2:]
    hid = w_in.shape[3]
    any_spec = pl.BlockSpec(memory_space=pl.ANY)
    flops = 2 * NG * NE * CAP * (2 * tokens * dim + 3 * dim * hid)
    return pl.pallas_call(
        dispatch_kernel,
        name='dispatch',
        out_shape=(jax.ShapeDtypeStruct((NG, NE, CAP, dim), BF16),
                   jax.ShapeDtypeStruct((NG, tokens, dim), BF16),
                   jax.ShapeDtypeStruct((NE, NG, CAP, dim), BF16),
                   jax.ShapeDtypeStruct((NG, 8, tokens), F32),
                   jax.ShapeDtypeStruct((2, 2, tokens, 128), F32)),
        in_specs=[any_spec] * 7,
        out_specs=[any_spec] * 5,
        scratch_shapes=[
            pltpu.VMEM((2, NG, tokens, dim), BF16),
            pltpu.VMEM((NG, 2, 4, tokens), jnp.int32),
            pltpu.VMEM((NG, 2, 4, tokens), F32),
            pltpu.VMEM((2, NG, 8, tokens), F32),
            pltpu.VMEM((2, NG, 8, tokens), F32),
            pltpu.VMEM((NE, NG, CAP, 128), F32),
            pltpu.VMEM((NE, NG, CAP, dim), BF16),
            pltpu.VMEM((2, NE, CAP, dim), BF16),
            pltpu.VMEM((2, 2, CAP, dim), BF16),
            pltpu.VMEM((2, 3, dim, hid), BF16),
            pltpu.VMEM((2, 2, tokens, 128), F32),
            pltpu.SemaphoreType.DMA((5, 16)),
            pltpu.SemaphoreType.DMA((5, NG, 2)),
            pltpu.SemaphoreType.DMA,
            pltpu.SemaphoreType.DMA((2, 3)),
            pltpu.SemaphoreType.DMA((2,)),
            pltpu.SemaphoreType.DMA((2,)),
            pltpu.SemaphoreType.DMA((2,)),
        ],
        cost_estimate=pl.CostEstimate(flops=flops, bytes_accessed=60_000_000, transcendentals=0),
        compiler_params=pltpu.CompilerParams(collective_id=0, has_side_effects=True,
                                             vmem_limit_bytes=67_043_328),
    )(x_acts, d_out, ids, gts, w_in, w_up, w_out)


def token_codes(ids, lower):
    tokens, top_k = ids.shape
    experts = lax.broadcasted_iota(jnp.int32, (tokens, 128), 1).astype(F32)
    taken = jnp.zeros((tokens, 128), F32)
    for j in range(top_k):
        taken += jnp.where(ids[:, j:j + 1] == experts, 1.0, 0.0)
    rank = dot(lower, taken.astype(BF16)) - 1.0
    return jnp.where(taken > 0.5, rank, -10000.0)


def slot_matrix(cols):
    tokens = cols[0].shape[0]
    lane = lax.broadcasted_iota(jnp.int32, (tokens, 128), 1).astype(F32)
    blocks = []
    for b in range(len(cols) * CAP // 128):
        hit = None
        for k, col in enumerate(cols):
            if k * CAP < (b + 1) * 128 and (k + 1) * CAP > b * 128:
                eq = lane == col + float(k * CAP - b * 128)
                hit = eq if hit is None else hit | eq
        blocks.append(jnp.where(hit, 1.0, 0.0).astype(BF16))
    return jnp.concatenate(blocks, axis=1)


def finish_kernel(code_ref, tok_ref, xb_ref, q_ref, win_ref, wup_ref, wout_ref, c_ref,
                  y_ref, dx_ref, dwin_ref, dwup_ref, dwout_ref, yhop_ref, dhop_ref, rows_ref,
                  xbuf, xs, qbuf, wbuf, acc_in, acc_up, acc_out, dwst, dxst, rbuf, part_out, part_in,
                  out_buf, y_buf,
                  xsem, qsem, wsem, dwsem, dxsem, rbsem, rdsem, ysem,
                  ssem, rsem, dsem, drsem, psem, prsem, zsem, zrsem):
    stage = lax.axis_index('stage')
    me = lax.axis_index('expert')
    core = me % 2
    sib_of = lambda h: h + 1 - 2 * (h % 2)
    sib = sib_of(me)
    xn = me + 2 - 4 * ((me // 2) % 2)
    yn = me + 4 - 8 * (me // 4)
    dg = xn + 4 - 8 * (xn // 4)
    partner = yn + core * (xn - yn)
    line = xn + core * (yn - xn)
    line0 = 2 * (line // 2)
    tokens, dim = y_buf.shape
    pieces, piece = part_out.shape[:2]
    tchunk = 256
    per_chunk = tchunk // piece

    barrier = pltpu.get_barrier_semaphore()
    for peer in ((1 - stage, me), (stage, sib), (stage, xn), (stage, yn), (stage, sib_of(xn)),
                 (stage, sib_of(yn))):
        pl.semaphore_signal(barrier, inc=1, device_id=peer, device_id_type=MESH)
    pl.semaphore_wait(barrier, 6)

    targets = ((2 * (xn // 2), 2 * (dg // 2), 1 + core), (2 * (yn // 2) + 1, 2 * (dg // 2) + 1, 1 + core),
               (sib, sib_of(xn) + core * (sib_of(yn) - sib_of(xn)), 0))

    def y_hop(role, k):
        target, via, slot = targets[k]
        return pltpu.make_async_remote_copy(
            src_ref=c_ref.at[via if role == 0 else target], dst_ref=yhop_ref.at[role, slot],
            send_sem=ssem.at[role, k], recv_sem=rsem.at[role, slot],
            device_id=(stage, target), device_id_type=MESH)

    def y_arrived(role, slot):
        pltpu.make_async_remote_copy(
            src_ref=c_ref.at[me], dst_ref=yhop_ref.at[role, slot], send_sem=ssem.at[role, 0],
            recv_sem=rsem.at[role, slot], device_id=(stage, sib), device_id_type=MESH).wait_recv()

    def d_hop(role, k, e):
        target, via, slot = targets[k]
        return pltpu.make_async_remote_copy(
            src_ref=rows_ref.at[via if role == 0 else target, e], dst_ref=dhop_ref.at[role, slot, e],
            send_sem=dsem.at[e, role, k], recv_sem=drsem.at[e, role, slot],
            device_id=(stage, target), device_id_type=MESH)

    def d_arrived(role, slot, e):
        pltpu.make_async_remote_copy(
            src_ref=rows_ref.at[me, e], dst_ref=dhop_ref.at[role, slot, e], send_sem=dsem.at[e, role, 0],
            recv_sem=drsem.at[e, role, slot], device_id=(stage, sib), device_id_type=MESH).wait_recv()

    for role in range(2):
        for k in range(3):
            y_hop(role, k).start()

    def weights(e):
        return [pltpu.make_async_copy(w.at[0, e], wbuf.at[e % 2, k], wsem.at[e % 2, k])
                for k, w in enumerate((win_ref, wup_ref, wout_ref))] + [
            pltpu.make_async_copy(q_ref.at[e], qbuf.at[e % 2], qsem.at[e % 2])]

    def x_fetch(h):
        return pltpu.make_async_copy(xb_ref.at[h], xbuf.at[h % 2], xsem.at[h % 2])

    x_fetch(0).start()
    for e in range(2):
        for copy in weights(e):
            copy.start()

    @pl.loop(0, NG)
    def _(h):
        pl.when(h + 1 < NG)(lambda: x_fetch(h + 1).start())
        hits = slot_hits(code_ref[h], tokens)
        onehot = jnp.concatenate([jnp.where(hit, 1.0, 0.0).astype(BF16) for hit in hits], axis=0)
        x_fetch(h).wait()
        rows = dot(onehot, xbuf[h % 2]).astype(BF16)
        for e in range(NE):
            xs[e, h] = rows[e * CAP:(e + 1) * CAP]

    sources = (sib, line0, line0 + 1, me)

    def y_load(role):
        copies = [pltpu.make_async_copy(yhop_ref.at[role, slot], rbuf.at[0, :, slot], rbsem.at[0, slot])
                  for slot in range(3)]
        copies.append(pltpu.make_async_copy(c_ref.at[partner if role == 0 else me], rbuf.at[0, :, 3],
                                            rbsem.at[0, 3]))
        for copy in copies:
            copy.start()
        for copy in copies:
            copy.wait()

    def d_load(role, e):
        copies = [pltpu.make_async_copy(dhop_ref.at[role, slot, e], rbuf.at[role, e, slot],
                                        rdsem.at[role, e, slot])
                  for slot in range(3)]
        return copies + [pltpu.make_async_copy(rows_ref.at[partner if role == 0 else me, e],
                                               rbuf.at[role, e, 3], rdsem.at[role, e, 3])]

    def d_fetch(role, experts):
        for e in experts:
            for slot in range(3):
                d_arrived(role, slot, e)
            for copy in d_load(role, e):
                copy.start()

    def combine(kind, role, buf, chunk, experts):
        code = tok_ref[kind, 1 - role, pl.ds(chunk * tchunk, tchunk)]
        codes = [pltpu.roll(code, (128 - NE * d) % 128, 1) for d in sources]
        total = None
        for e in experts:
            part = dot(slot_matrix([c[:, e:e + 1] for c in codes]), rbuf[buf, e].reshape(NE * CAP, dim))
            total = part if total is None else total + part
        return total

    every = tuple(range(NE))

    def partial_copy(kind, i):
        return pltpu.make_async_remote_copy(
            src_ref=part_out.at[i], dst_ref=part_in.at[kind, i], send_sem=psem.at[kind, i],
            recv_sem=prsem.at[kind, i], device_id=(stage, partner), device_id_type=MESH)

    def z_copy(i):
        return pltpu.make_async_remote_copy(
            src_ref=out_buf.at[i], dst_ref=dx_ref.at[pl.ds(i * piece, piece)], send_sem=zsem.at[i],
            recv_sem=zrsem.at[i], device_id=(1 - stage, me), device_id_type=MESH)

    def pass_on(kind, experts, first):
        @pl.loop(0, tokens // tchunk)
        def _(chunk):
            total = combine(kind, 0, 0, chunk, experts)
            for p in range(per_chunk):
                i = chunk * per_chunk + p
                part = total[p * piece:(p + 1) * piece]
                part_out[i] = part if first else part_out[i] + part
            if experts[-1] == NE - 1:
                for p in range(per_chunk):
                    partial_copy(kind, chunk * per_chunk + p).start()

    def y_pass_on():
        for slot in range(3):
            y_arrived(0, slot)
        y_load(0)
        pass_on(0, every, True)

    chunk = 4
    rows_chunk = chunk * CAP
    grads = ((acc_in, dwin_ref), (acc_up, dwup_ref), (acc_out, dwout_ref))

    def grad_copies(e):
        return [pltpu.make_async_copy(dwst.at[k], ref.at[0, e], dwsem.at[k])
                for k, (_, ref) in enumerate(grads)]

    @pl.loop(0, NE)
    def _(e):
        pl.when(e == 1)(y_pass_on)
        for copy in weights(e):
            copy.wait()
        w_in, w_up, w_out = (wbuf[e % 2, k] for k in range(3))

        @pl.loop(0, NG // chunk)
        def _(i):
            hs = pl.ds(i * chunk, chunk)
            x = xs[e, hs].reshape(rows_chunk, dim)
            q = qbuf[e % 2, hs].reshape(rows_chunk, dim)
            pre_in = dot(x, w_in)
            pre_up = dot(x, w_up)
            d_hid = dot(q, w_out, ((1,), (1,)))
            sig = jax.nn.sigmoid(pre_in)
            act = pre_in * sig
            hidden = (act * pre_up).astype(BF16)
            d_in = (d_hid * pre_up * sig * (1.0 + pre_in * (1.0 - sig))).astype(BF16)
            d_up = (d_hid * act).astype(BF16)
            dx = dot(d_in, w_in, ((1,), (1,))) + dot(d_up, w_up, ((1,), (1,)))
            dxst[hs] = dx.astype(BF16).reshape(chunk, CAP, dim)
            parts = (dot(x, d_in, ((0,), (0,))), dot(x, d_up, ((0,), (0,))), dot(hidden, q, ((0,), (0,))))
            for (acc, _), part in zip(grads, parts):
                acc[...] = jnp.where(i == 0, part, acc[...] + part)

        out = pltpu.make_async_copy(dxst, rows_ref.at[:, e], dxsem)
        out.start()

        @pl.when(e >= 1)
        def _():
            for copy in grad_copies(e - 1):
                copy.wait()

        for k, (acc, _) in enumerate(grads):
            dwst[k] = acc[...].astype(BF16)
        for copy in grad_copies(e):
            copy.start()

        @pl.when(e + 2 < NE)
        def _():
            for copy in weights(e + 2):
                copy.start()

        out.wait()
        for role in range(2):
            for k in range(3):
                d_hop(role, k, e).start()

    for slot in range(3):
        y_arrived(1, slot)
    y_load(1)

    @pl.loop(0, tokens // tchunk)
    def _(chunk):
        total = combine(0, 1, 0, chunk, every)
        for p in range(per_chunk):
            i = chunk * per_chunk + p
            partial_copy(0, i).wait_recv()
            y_buf[pl.ds(i * piece, piece)] = (total[p * piece:(p + 1) * piece] + part_in[0, i]).astype(BF16)
            partial_copy(0, i).wait_send()

    y_out = pltpu.make_async_copy(y_buf, y_ref, ysem)
    y_out.start()

    def d_ready(role, experts):
        for e in experts:
            for copy in d_load(role, e):
                copy.wait()

    d_fetch(0, every[:-1])
    d_ready(0, every[:-1])
    pass_on(1, every[:-1], True)
    d_fetch(1, every[:-1])
    d_fetch(0, every[-1:])
    d_ready(0, every[-1:])
    pass_on(1, every[-1:], False)
    d_fetch(1, every[-1:])
    d_ready(1, every)

    @pl.loop(0, tokens // tchunk)
    def _(chunk):
        total = combine(1, 1, 1, chunk, every)
        for p in range(per_chunk):
            i = chunk * per_chunk + p
            partial_copy(1, i).wait_recv()
            out_buf[i] = (total[p * piece:(p + 1) * piece] + part_in[1, i]).astype(BF16)
            z_copy(i).start()

    y_out.wait()
    for copy in grad_copies(NE - 1):
        copy.wait()
    for role in range(2):
        for k in range(3):
            y_hop(role, k).wait_send()

            @pl.loop(0, NE)
            def _(e):
                d_hop(role, k, e).wait_send()

    @pl.loop(0, pieces)
    def _(i):
        partial_copy(1, i).wait_send()
        z_copy(i).wait()


def run_finish(code, tok, xb, q_rows, w_in, w_up, w_out, c_rows):
    tokens, dim = xb.shape[1:]
    hid = w_in.shape[3]
    pieces = 16
    any_spec = pl.BlockSpec(memory_space=pl.ANY)
    vmem_spec = pl.BlockSpec(memory_space=pltpu.VMEM)
    tok_shape = jax.ShapeDtypeStruct((tokens, dim), BF16)
    hop_shape = jax.ShapeDtypeStruct((2, 3, NE, CAP, dim), BF16)
    dma = pltpu.SemaphoreType.DMA
    flops = 2 * NG * NE * CAP * (3 * tokens * dim + 8 * dim * hid)
    return pl.pallas_call(
        finish_kernel,
        name='finish',
        out_shape=(tok_shape, tok_shape, jax.ShapeDtypeStruct(w_in.shape, BF16),
                   jax.ShapeDtypeStruct(w_up.shape, BF16), jax.ShapeDtypeStruct(w_out.shape, BF16),
                   hop_shape, hop_shape, jax.ShapeDtypeStruct((NG, NE, CAP, dim), BF16)),
        in_specs=[vmem_spec] * 2 + [any_spec] * 6,
        out_specs=[any_spec] * 8,
        scratch_shapes=[
            pltpu.VMEM((2, tokens, dim), BF16),
            pltpu.VMEM((NE, NG, CAP, dim), BF16),
            pltpu.VMEM((2, NG, CAP, dim), BF16),
            pltpu.VMEM((2, 3, dim, hid), BF16),
            pltpu.VMEM((dim, hid), F32),
            pltpu.VMEM((dim, hid), F32),
            pltpu.VMEM((hid, dim), F32),
            pltpu.VMEM((3, dim, hid), BF16),
            pltpu.VMEM((NG, CAP, dim), BF16),
            pltpu.VMEM((2, NE, 4, CAP, dim), BF16),
            pltpu.VMEM((pieces, tokens // pieces, dim), F32),
            pltpu.VMEM((2, pieces, tokens // pieces, dim), F32),
            pltpu.VMEM((pieces, tokens // pieces, dim), BF16),
            pltpu.VMEM((tokens, dim), BF16),
            dma((2,)), dma((2,)), dma((2, 3)), dma((3,)), dma, dma((1, 4)), dma((2, NE, 4)), dma,
            dma((2, 3)), dma((2, 3)), dma((NE, 2, 3)), dma((NE, 2, 3)),
            dma((2, pieces)), dma((2, pieces)), dma((pieces,)), dma((pieces,)),
        ],
        cost_estimate=pl.CostEstimate(flops=flops, bytes_accessed=80_000_000, transcendentals=0),
        compiler_params=pltpu.CompilerParams(collective_id=1, has_side_effects=True,
                                             vmem_limit_bytes=67_043_328),
    )(code, tok, xb, q_rows, w_in, w_up, w_out, c_rows)


def solution(mesh):
    def device_fn(x_acts, expert_ids, gate_wts, w_in, w_up, w_out, d_out):
        ids_t = jnp.swapaxes(expert_ids[:, 0], 1, 2)
        gates_t = jnp.swapaxes(gate_wts[:, 0], 1, 2)
        c_rows, xb, q_rows, code, tok = run_dispatch(x_acts, d_out, ids_t, gates_t, w_in, w_up, w_out)
        y_dev, dx_dev, dw_in, dw_up, dw_out = run_finish(
            code, tok, xb, q_rows, w_in, w_up, w_out, c_rows)[:5]
        return y_dev[None], dx_dev[None], dw_in, dw_up, dw_out

    tok_spec = P(None, 'stage', 'expert', None)
    w_spec = P('stage', 'expert', None, None)
    row_spec = P('stage', 'expert', None)
    return jax.shard_map(device_fn, mesh=mesh,
                         in_specs=(tok_spec, tok_spec, tok_spec, w_spec, w_spec, w_spec, row_spec),
                         out_specs=(row_spec, row_spec, w_spec, w_spec, w_spec), check_vma=False)
```

```python
import jax
import jax.numpy as jnp
from jax import lax
from jax.experimental import pallas as pl
from jax.experimental.pallas import tpu as pltpu
from jax.sharding import PartitionSpec as P

MESH = pl.DeviceIdType.MESH
F32, BF16 = jnp.float32, jnp.bfloat16
DY, XF, XB, IDS, GTS = 0, 1, 2, 3, 4
NG, NE, CAP = 8, 4, 192


def dot(lhs, rhs, dims=((1,), (0,))):
    return lax.dot_general(lhs, rhs, (dims, ((), ())), preferred_element_type=F32)


def slot_hits(code_rows, tokens):
    slot = lax.broadcasted_iota(jnp.int32, (CAP, tokens), 0).astype(F32)
    return [slot == code_rows[e:e + 1, :] for e in range(NE)]


def dispatch_kernel(x_ref, dy_ref, ids_ref, gts_ref, win_ref, wup_ref, wout_ref,
                    c_ref, xb_ref, q_ref, code_ref, tok_ref,
                    buf, tab_ids, tab_gts, codes, gates, gslot, xs, st, cst, wbuf, tok,
                    ssem, rsem, lsem, wsem, stsem, csem, tsem):
    stage = lax.axis_index('stage')
    me = lax.axis_index('expert')
    other = 1 - stage
    core = me % 2
    xn = me + 2 - 4 * ((me // 2) % 2)
    yn = me + 4 - 8 * (me // 4)
    dg = xn + 4 - 8 * (xn // 4)
    sib_of = lambda h: h + 1 - 2 * core
    sib = sib_of(me)
    tokens = x_ref.shape[2]
    half = tokens // 2
    sends = []

    barrier = pltpu.get_barrier_semaphore()
    for peer in ((other, me), (stage, sib), (stage, xn), (stage, yn)):
        pl.semaphore_signal(barrier, inc=1, device_id=peer, device_id_type=MESH)
    pl.semaphore_wait(barrier, 4)

    def place(arr, h, part):
        if arr == IDS:
            return tab_ids.at[h]
        if arr == GTS:
            return tab_gts.at[h]
        if arr == XB:
            return xb_ref.at[h, pl.ds(part * half, half)]
        return buf.at[arr, h, pl.ds(part * half, half)]

    def remote(arr, h, part, slot, peer, src=None):
        return pltpu.make_async_remote_copy(
            src_ref=place(arr, h, part) if src is None else src, dst_ref=place(arr, h, part),
            send_sem=ssem.at[arr, slot], recv_sem=rsem.at[arr, h, part],
            device_id=peer, device_id_type=MESH)

    def send(arr, h, part, slot, peer, src=None):
        remote(arr, h, part, slot, peer, src).start()
        sends.append((arr, h, part, slot, peer, src))

    def arrived(arr, h, part):
        remote(arr, h, part, 0, (stage, sib)).wait_recv()

    to_x, to_y, to_sib, to_z = (stage, xn), (stage, yn), (stage, sib), (other, me)

    send(IDS, me, 0, 14, to_z, ids_ref)
    send(GTS, me, 0, 14, to_z, gts_ref)
    for part in range(2):
        send(XF, me, part, 14 + part, to_z, x_ref.at[1, 0, pl.ds(part * half, half)])
    for part in range(2):
        send(XB, me, part, 14 + part, to_z, x_ref.at[0, 0, pl.ds(part * half, half)])
    dy_half = lambda part: dy_ref.at[0, pl.ds(part * half, half)]
    send(DY, me, 0, 0, to_x, dy_half(0))
    send(DY, me, 1, 2, to_y, dy_half(1))
    send(DY, me, 0, 4, to_sib, dy_half(0))
    send(DY, me, 1, 5, to_sib, dy_half(1))
    own_dy = pltpu.make_async_copy(dy_ref.at[0], buf.at[DY, me], lsem)
    own_dy.start()

    def weights(e):
        return [pltpu.make_async_copy(w.at[0, e], wbuf.at[e % 2, k], wsem.at[e % 2, k])
                for k, w in enumerate((win_ref, wup_ref, wout_ref))]

    for e in range(2):
        for copy in weights(e):
            copy.start()

    for arr in (IDS, GTS):
        arrived(arr, me, 0)
        send(arr, me, 0, 0, to_x)
        send(arr, me, 0, 2, to_y)
        send(arr, me, 0, 4, to_sib)
    send(DY, me, 1, 1, to_x, dy_half(1))
    send(DY, me, 0, 3, to_y, dy_half(0))

    def first_halves(arr):
        arrived(arr, xn, 0)
        arrived(arr, yn, 1)
        send(arr, xn, 0, 6, to_y)
        send(arr, yn, 1, 7, to_x)
        send(arr, xn, 0, 8, to_sib)
        send(arr, yn, 1, 11, to_sib)

    def second_halves(arr):
        arrived(arr, xn, 1)
        arrived(arr, yn, 0)
        send(arr, xn, 1, 9, to_sib)
        send(arr, yn, 0, 10, to_sib)

    def diagonal(arr):
        for part in range(2):
            arrived(arr, dg, part)
            send(arr, dg, part, 12 + part, to_sib)

    def own_sends(arr):
        for part in range(2):
            arrived(arr, me, part)
        send(arr, me, 0, 0, to_x)
        send(arr, me, 1, 2, to_y)
        send(arr, me, 1, 1, to_x)
        send(arr, me, 0, 3, to_y)
        send(arr, me, 0, 4, to_sib)
        send(arr, me, 1, 5, to_sib)

    for arr in (IDS, GTS):
        arrived(arr, xn, 0)
        arrived(arr, yn, 0)
        send(arr, xn, 0, 6, to_y)
    first_halves(DY)
    for arr in (IDS, GTS):
        send(arr, xn, 0, 8, to_sib)
        send(arr, yn, 0, 10, to_sib)
    own_sends(XF)
    second_halves(DY)
    for arr in (IDS, GTS):
        arrived(arr, dg, 0)
        send(arr, dg, 0, 12, to_sib)
        for h in (sib, sib_of(xn), sib_of(yn), sib_of(dg)):
            arrived(arr, h, 0)

    upper = (lax.broadcasted_iota(jnp.int32, (tokens, tokens), 0)
             <= lax.broadcasted_iota(jnp.int32, (tokens, tokens), 1)).astype(F32).astype(BF16)
    for kind in range(2):
        taken = []
        for h in range(NG):
            for e in range(NE):
                eq = tab_ids[h, 1 - kind] == me * NE + e
                taken.append(jnp.sum(jnp.where(eq, 1.0, 0.0), axis=0, keepdims=True))
                gates[kind, h, e:e + 1, :] = jnp.sum(jnp.where(eq, tab_gts[h, 1 - kind], 0.0), axis=0,
                                                     keepdims=True)
        taken = jnp.concatenate(taken, axis=0)
        rank = dot(taken.astype(BF16), upper) - 1.0
        code = jnp.where(taken > 0.5, rank, -1.0)
        for h in range(NG):
            codes[kind, h, 0:NE, :] = code[h * NE:(h + 1) * NE, :]
            codes[kind, h, NE:8, :] = jnp.full((8 - NE, tokens), -1.0, F32)
    code_copy = pltpu.make_async_copy(codes.at[1], code_ref, tsem.at[0])
    code_copy.start()

    partner = yn + core * (xn - yn)
    lower = (lax.broadcasted_iota(jnp.int32, (tokens, tokens), 0)
             >= lax.broadcasted_iota(jnp.int32, (tokens, tokens), 1)).astype(F32).astype(BF16)
    for n, h in enumerate((me, partner)):
        both = jnp.concatenate([tab_ids[h, 0], tab_ids[h, 1]], axis=0).astype(F32).T
        for kind in range(2):
            tok[kind, n] = token_codes(both[:, 4 * (1 - kind):4 * (1 - kind) + 4], lower)
    tok_copy = pltpu.make_async_copy(tok, tok_ref, tsem.at[1])
    tok_copy.start()

    def shard(i):
        j, odd = i // 2, i % 2
        return me + (j % 2) * (xn - me) + (j // 2) * (yn - me) + odd * (1 - 2 * core)

    def gather(kind, arr, h):
        hits = slot_hits(codes[kind, h], tokens)
        gate_rows = gates[kind, h]
        onehot = jnp.concatenate([jnp.where(hit, 1.0, 0.0).astype(BF16) for hit in hits], axis=0)
        slot_gate = [jnp.sum(jnp.where(hits[e], gate_rows[e:e + 1, :], 0.0), axis=1, keepdims=True)
                     for e in range(NE)]
        return dot(onehot, buf[arr, h]), slot_gate

    def q_copy(slot, h):
        return pltpu.make_async_copy(st.at[slot], q_ref.at[:, h], stsem.at[slot])

    def sibling_part(arr, i):
        @pl.when(i % 2 == 1)
        def _():
            arrived(arr, shard(i), 0)
            arrived(arr, shard(i), 1)

    own_dy.wait()

    @pl.loop(0, NG)
    def _(i):
        pl.when(i == 6)(lambda: diagonal(DY))
        sibling_part(DY, i)
        h, slot = shard(i), i % 2
        pl.when(i >= 2)(lambda: q_copy(slot, h).wait())
        rows, slot_gate = gather(1, DY, h)
        for e in range(NE):
            st[slot, e] = (slot_gate[e] * rows[e * CAP:(e + 1) * CAP]).astype(BF16)
        q_copy(slot, h).start()

    first_halves(XF)
    own_sends(XB)

    @pl.loop(0, NG)
    def _(i):
        pl.when(i == 2)(lambda: second_halves(XF))
        pl.when(i == 6)(lambda: diagonal(XF))
        sibling_part(XF, i)
        h = shard(i)
        rows, slot_gate = gather(0, XF, h)
        for e in range(NE):
            xs[e, h] = rows[e * CAP:(e + 1) * CAP].astype(BF16)
            gslot[e, h] = jnp.broadcast_to(slot_gate[e], (CAP, 128))

    chunk = 2
    steps = NG // chunk
    rows_chunk = chunk * CAP

    def c_copy(slot, e, h0):
        return pltpu.make_async_copy(cst.at[slot], c_ref.at[pl.ds(h0, chunk), e], csem.at[slot])

    @pl.loop(0, NE)
    def _(e):
        pl.when(e == 1)(lambda: first_halves(XB))
        pl.when(e == 3)(lambda: second_halves(XB))
        for copy in weights(e):
            copy.wait()

        @pl.loop(0, steps)
        def _(i):
            slot = i % 2
            h0 = i * chunk
            rows = xs[e, pl.ds(h0, chunk)].reshape(rows_chunk, -1)
            pre = dot(rows, wbuf[e % 2, 0])
            act = pre * jax.nn.sigmoid(pre)
            hidden = (act * dot(rows, wbuf[e % 2, 1])).astype(BF16)
            out = dot(hidden, wbuf[e % 2, 2])
            gate = gslot[e, pl.ds(h0, chunk)].reshape(rows_chunk, 128)[:, 0:1]
            pl.when(e * steps + i >= 2)(lambda: c_copy(slot, e, h0).wait())
            cst[slot] = (gate * out).astype(BF16).reshape(chunk, CAP, -1)
            c_copy(slot, e, h0).start()

        @pl.when(e + 2 < NE)
        def _():
            for copy in weights(e + 2):
                copy.start()

    diagonal(XB)
    for h in (sib, sib_of(xn), sib_of(yn), sib_of(dg)):
        arrived(XB, h, 0)
        arrived(XB, h, 1)
    for slot in range(2):
        c_copy(slot, NE - 1, 0).wait()
        q_copy(slot, 0).wait()
    code_copy.wait()
    tok_copy.wait()
    for args in sends:
        remote(*args).wait_send()


def run_dispatch(x_acts, d_out, ids, gts, w_in, w_up, w_out):
    tokens, dim = x_acts.shape[2:]
    hid = w_in.shape[3]
    any_spec = pl.BlockSpec(memory_space=pl.ANY)
    flops = 2 * NG * NE * CAP * (2 * tokens * dim + 3 * dim * hid)
    return pl.pallas_call(
        dispatch_kernel,
        name='dispatch',
        out_shape=(jax.ShapeDtypeStruct((NG, NE, CAP, dim), BF16),
                   jax.ShapeDtypeStruct((NG, tokens, dim), BF16),
                   jax.ShapeDtypeStruct((NE, NG, CAP, dim), BF16),
                   jax.ShapeDtypeStruct((NG, 8, tokens), F32),
                   jax.ShapeDtypeStruct((2, 2, tokens, 128), F32)),
        in_specs=[any_spec] * 7,
        out_specs=[any_spec] * 5,
        scratch_shapes=[
            pltpu.VMEM((2, NG, tokens, dim), BF16),
            pltpu.VMEM((NG, 2, 4, tokens), jnp.int32),
            pltpu.VMEM((NG, 2, 4, tokens), F32),
            pltpu.VMEM((2, NG, 8, tokens), F32),
            pltpu.VMEM((2, NG, 8, tokens), F32),
            pltpu.VMEM((NE, NG, CAP, 128), F32),
            pltpu.VMEM((NE, NG, CAP, dim), BF16),
            pltpu.VMEM((2, NE, CAP, dim), BF16),
            pltpu.VMEM((2, 2, CAP, dim), BF16),
            pltpu.VMEM((2, 3, dim, hid), BF16),
            pltpu.VMEM((2, 2, tokens, 128), F32),
            pltpu.SemaphoreType.DMA((5, 16)),
            pltpu.SemaphoreType.DMA((5, NG, 2)),
            pltpu.SemaphoreType.DMA,
            pltpu.SemaphoreType.DMA((2, 3)),
            pltpu.SemaphoreType.DMA((2,)),
            pltpu.SemaphoreType.DMA((2,)),
            pltpu.SemaphoreType.DMA((2,)),
        ],
        cost_estimate=pl.CostEstimate(flops=flops, bytes_accessed=60_000_000, transcendentals=0),
        compiler_params=pltpu.CompilerParams(collective_id=0, has_side_effects=True,
                                             vmem_limit_bytes=67_043_328),
    )(x_acts, d_out, ids, gts, w_in, w_up, w_out)


def token_codes(ids, lower):
    tokens, top_k = ids.shape
    experts = lax.broadcasted_iota(jnp.int32, (tokens, 128), 1).astype(F32)
    taken = jnp.zeros((tokens, 128), F32)
    for j in range(top_k):
        taken += jnp.where(ids[:, j:j + 1] == experts, 1.0, 0.0)
    rank = dot(lower, taken.astype(BF16)) - 1.0
    return jnp.where(taken > 0.5, rank, -10000.0)


def slot_matrix(cols):
    tokens = cols[0].shape[0]
    lane = lax.broadcasted_iota(jnp.int32, (tokens, 128), 1).astype(F32)
    blocks = []
    for b in range(len(cols) * CAP // 128):
        hit = None
        for k, col in enumerate(cols):
            if k * CAP < (b + 1) * 128 and (k + 1) * CAP > b * 128:
                eq = lane == col + float(k * CAP - b * 128)
                hit = eq if hit is None else hit | eq
        blocks.append(jnp.where(hit, 1.0, 0.0).astype(BF16))
    return jnp.concatenate(blocks, axis=1)


def finish_kernel(code_ref, tok_ref, xb_ref, q_ref, win_ref, wup_ref, wout_ref, c_ref,
                  y_ref, dx_ref, dwin_ref, dwup_ref, dwout_ref, yhop_ref, dhop_ref, rows_ref,
                  xbuf, xs, qbuf, wbuf, acc_in, acc_up, acc_out, dwst, dxst, rbuf, part_out, part_in,
                  out_buf, y_buf,
                  xsem, qsem, wsem, dwsem, dxsem, rbsem, rdsem, ysem,
                  ssem, rsem, dsem, drsem, psem, prsem, zsem, zrsem):
    stage = lax.axis_index('stage')
    me = lax.axis_index('expert')
    core = me % 2
    sib_of = lambda h: h + 1 - 2 * (h % 2)
    sib = sib_of(me)
    xn = me + 2 - 4 * ((me // 2) % 2)
    yn = me + 4 - 8 * (me // 4)
    dg = xn + 4 - 8 * (xn // 4)
    partner = yn + core * (xn - yn)
    line = xn + core * (yn - xn)
    line0 = 2 * (line // 2)
    tokens, dim = y_buf.shape
    pieces, piece = part_out.shape[:2]
    tchunk = 256
    per_chunk = tchunk // piece

    barrier = pltpu.get_barrier_semaphore()
    for peer in ((1 - stage, me), (stage, sib), (stage, xn), (stage, yn), (stage, sib_of(xn)),
                 (stage, sib_of(yn))):
        pl.semaphore_signal(barrier, inc=1, device_id=peer, device_id_type=MESH)
    pl.semaphore_wait(barrier, 6)

    targets = ((2 * (xn // 2), 2 * (dg // 2), 1 + core), (2 * (yn // 2) + 1, 2 * (dg // 2) + 1, 1 + core),
               (sib, sib_of(xn) + core * (sib_of(yn) - sib_of(xn)), 0))

    def y_hop(role, k):
        target, via, slot = targets[k]
        return pltpu.make_async_remote_copy(
            src_ref=c_ref.at[via if role == 0 else target], dst_ref=yhop_ref.at[role, slot],
            send_sem=ssem.at[role, k], recv_sem=rsem.at[role, slot],
            device_id=(stage, target), device_id_type=MESH)

    def y_arrived(role, slot):
        pltpu.make_async_remote_copy(
            src_ref=c_ref.at[me], dst_ref=yhop_ref.at[role, slot], send_sem=ssem.at[role, 0],
            recv_sem=rsem.at[role, slot], device_id=(stage, sib), device_id_type=MESH).wait_recv()

    def d_hop(role, k, e):
        target, via, slot = targets[k]
        return pltpu.make_async_remote_copy(
            src_ref=rows_ref.at[via if role == 0 else target, e], dst_ref=dhop_ref.at[role, slot, e],
            send_sem=dsem.at[e, role, k], recv_sem=drsem.at[e, role, slot],
            device_id=(stage, target), device_id_type=MESH)

    def d_arrived(role, slot, e):
        pltpu.make_async_remote_copy(
            src_ref=rows_ref.at[me, e], dst_ref=dhop_ref.at[role, slot, e], send_sem=dsem.at[e, role, 0],
            recv_sem=drsem.at[e, role, slot], device_id=(stage, sib), device_id_type=MESH).wait_recv()

    for role in range(2):
        for k in range(3):
            y_hop(role, k).start()

    def weights(e):
        return [pltpu.make_async_copy(w.at[0, e], wbuf.at[e % 2, k], wsem.at[e % 2, k])
                for k, w in enumerate((win_ref, wup_ref, wout_ref))] + [
            pltpu.make_async_copy(q_ref.at[e], qbuf.at[e % 2], qsem.at[e % 2])]

    def x_fetch(h):
        return pltpu.make_async_copy(xb_ref.at[h], xbuf.at[h % 2], xsem.at[h % 2])

    x_fetch(0).start()
    for e in range(2):
        for copy in weights(e):
            copy.start()

    @pl.loop(0, NG)
    def _(h):
        pl.when(h + 1 < NG)(lambda: x_fetch(h + 1).start())
        hits = slot_hits(code_ref[h], tokens)
        onehot = jnp.concatenate([jnp.where(hit, 1.0, 0.0).astype(BF16) for hit in hits], axis=0)
        x_fetch(h).wait()
        rows = dot(onehot, xbuf[h % 2]).astype(BF16)
        for e in range(NE):
            xs[e, h] = rows[e * CAP:(e + 1) * CAP]

    sources = (sib, line0, line0 + 1, me)

    def y_load(role):
        copies = [pltpu.make_async_copy(yhop_ref.at[role, slot], rbuf.at[0, :, slot], rbsem.at[0, slot])
                  for slot in range(3)]
        copies.append(pltpu.make_async_copy(c_ref.at[partner if role == 0 else me], rbuf.at[0, :, 3],
                                            rbsem.at[0, 3]))
        for copy in copies:
            copy.start()
        for copy in copies:
            copy.wait()

    def d_load(role, e):
        copies = [pltpu.make_async_copy(dhop_ref.at[role, slot, e], rbuf.at[role, e, slot],
                                        rdsem.at[role, e, slot])
                  for slot in range(3)]
        return copies + [pltpu.make_async_copy(rows_ref.at[partner if role == 0 else me, e],
                                               rbuf.at[role, e, 3], rdsem.at[role, e, 3])]

    def d_fetch(role, experts):
        for e in experts:
            for slot in range(3):
                d_arrived(role, slot, e)
            for copy in d_load(role, e):
                copy.start()

    def combine(kind, role, buf, chunk, experts):
        code = tok_ref[kind, 1 - role, pl.ds(chunk * tchunk, tchunk)]
        codes = [pltpu.roll(code, (128 - NE * d) % 128, 1) for d in sources]
        total = None
        for e in experts:
            part = dot(slot_matrix([c[:, e:e + 1] for c in codes]), rbuf[buf, e].reshape(NE * CAP, dim))
            total = part if total is None else total + part
        return total

    every = tuple(range(NE))

    def partial_copy(kind, i):
        return pltpu.make_async_remote_copy(
            src_ref=part_out.at[i], dst_ref=part_in.at[kind, i], send_sem=psem.at[kind, i],
            recv_sem=prsem.at[kind, i], device_id=(stage, partner), device_id_type=MESH)

    def z_copy(i):
        return pltpu.make_async_remote_copy(
            src_ref=out_buf.at[i], dst_ref=dx_ref.at[pl.ds(i * piece, piece)], send_sem=zsem.at[i],
            recv_sem=zrsem.at[i], device_id=(1 - stage, me), device_id_type=MESH)

    def pass_on(kind, experts, first):
        @pl.loop(0, tokens // tchunk)
        def _(chunk):
            total = combine(kind, 0, 0, chunk, experts)
            for p in range(per_chunk):
                i = chunk * per_chunk + p
                part = total[p * piece:(p + 1) * piece]
                part_out[i] = part if first else part_out[i] + part
            if experts[-1] == NE - 1:
                for p in range(per_chunk):
                    partial_copy(kind, chunk * per_chunk + p).start()

    def y_pass_on():
        for slot in range(3):
            y_arrived(0, slot)
        y_load(0)
        pass_on(0, every, True)

    chunk = 4
    rows_chunk = chunk * CAP
    grads = ((acc_in, dwin_ref), (acc_up, dwup_ref), (acc_out, dwout_ref))

    def grad_copies(e):
        return [pltpu.make_async_copy(dwst.at[k], ref.at[0, e], dwsem.at[k])
                for k, (_, ref) in enumerate(grads)]

    @pl.loop(0, NE)
    def _(e):
        pl.when(e == 1)(y_pass_on)
        for copy in weights(e):
            copy.wait()
        w_in, w_up, w_out = (wbuf[e % 2, k] for k in range(3))

        @pl.loop(0, NG // chunk)
        def _(i):
            hs = pl.ds(i * chunk, chunk)
            x = xs[e, hs].reshape(rows_chunk, dim)
            q = qbuf[e % 2, hs].reshape(rows_chunk, dim)
            pre_in = dot(x, w_in)
            pre_up = dot(x, w_up)
            d_hid = dot(q, w_out, ((1,), (1,)))
            sig = jax.nn.sigmoid(pre_in)
            act = pre_in * sig
            hidden = (act * pre_up).astype(BF16)
            d_in = (d_hid * pre_up * sig * (1.0 + pre_in * (1.0 - sig))).astype(BF16)
            d_up = (d_hid * act).astype(BF16)
            dx = dot(d_in, w_in, ((1,), (1,))) + dot(d_up, w_up, ((1,), (1,)))
            dxst[hs] = dx.astype(BF16).reshape(chunk, CAP, dim)
            parts = (dot(x, d_in, ((0,), (0,))), dot(x, d_up, ((0,), (0,))), dot(hidden, q, ((0,), (0,))))
            for (acc, _), part in zip(grads, parts):
                acc[...] = jnp.where(i == 0, part, acc[...] + part)

        out = pltpu.make_async_copy(dxst, rows_ref.at[:, e], dxsem)
        out.start()

        @pl.when(e >= 1)
        def _():
            for copy in grad_copies(e - 1):
                copy.wait()

        for k, (acc, _) in enumerate(grads):
            dwst[k] = acc[...].astype(BF16)
        for copy in grad_copies(e):
            copy.start()

        @pl.when(e + 2 < NE)
        def _():
            for copy in weights(e + 2):
                copy.start()

        out.wait()
        for role in range(2):
            for k in range(3):
                d_hop(role, k, e).start()

    for slot in range(3):
        y_arrived(1, slot)
    y_load(1)

    @pl.loop(0, tokens // tchunk)
    def _(chunk):
        total = combine(0, 1, 0, chunk, every)
        for p in range(per_chunk):
            i = chunk * per_chunk + p
            partial_copy(0, i).wait_recv()
            y_buf[pl.ds(i * piece, piece)] = (total[p * piece:(p + 1) * piece] + part_in[0, i]).astype(BF16)
            partial_copy(0, i).wait_send()

    y_out = pltpu.make_async_copy(y_buf, y_ref, ysem)
    y_out.start()

    def d_ready(role, experts):
        for e in experts:
            for copy in d_load(role, e):
                copy.wait()

    d_fetch(0, every[:-1])
    d_ready(0, every[:-1])
    pass_on(1, every[:-1], True)
    d_fetch(1, every[:-1])
    d_fetch(0, every[-1:])
    d_ready(0, every[-1:])
    pass_on(1, every[-1:], False)
    d_fetch(1, every[-1:])
    d_ready(1, every)

    @pl.loop(0, tokens // tchunk)
    def _(chunk):
        total = combine(1, 1, 1, chunk, every)
        for p in range(per_chunk):
            i = chunk * per_chunk + p
            partial_copy(1, i).wait_recv()
            out_buf[i] = (total[p * piece:(p + 1) * piece] + part_in[1, i]).astype(BF16)
            z_copy(i).start()

    y_out.wait()
    for copy in grad_copies(NE - 1):
        copy.wait()
    for role in range(2):
        for k in range(3):
            y_hop(role, k).wait_send()

            @pl.loop(0, NE)
            def _(e):
                d_hop(role, k, e).wait_send()

    @pl.loop(0, pieces)
    def _(i):
        partial_copy(1, i).wait_send()
        z_copy(i).wait()


def run_finish(code, tok, xb, q_rows, w_in, w_up, w_out, c_rows):
    tokens, dim = xb.shape[1:]
    hid = w_in.shape[3]
    pieces = 16
    any_spec = pl.BlockSpec(memory_space=pl.ANY)
    vmem_spec = pl.BlockSpec(memory_space=pltpu.VMEM)
    tok_shape = jax.ShapeDtypeStruct((tokens, dim), BF16)
    hop_shape = jax.ShapeDtypeStruct((2, 3, NE, CAP, dim), BF16)
    dma = pltpu.SemaphoreType.DMA
    flops = 2 * NG * NE * CAP * (3 * tokens * dim + 8 * dim * hid)
    return pl.pallas_call(
        finish_kernel,
        name='finish',
        out_shape=(tok_shape, tok_shape, jax.ShapeDtypeStruct(w_in.shape, BF16),
                   jax.ShapeDtypeStruct(w_up.shape, BF16), jax.ShapeDtypeStruct(w_out.shape, BF16),
                   hop_shape, hop_shape, jax.ShapeDtypeStruct((NG, NE, CAP, dim), BF16)),
        in_specs=[vmem_spec] * 2 + [any_spec] * 6,
        out_specs=[any_spec] * 8,
        scratch_shapes=[
            pltpu.VMEM((2, tokens, dim), BF16),
            pltpu.VMEM((NE, NG, CAP, dim), BF16),
            pltpu.VMEM((2, NG, CAP, dim), BF16),
            pltpu.VMEM((2, 3, dim, hid), BF16),
            pltpu.VMEM((dim, hid), F32),
            pltpu.VMEM((dim, hid), F32),
            pltpu.VMEM((hid, dim), F32),
            pltpu.VMEM((3, dim, hid), BF16),
            pltpu.VMEM((NG, CAP, dim), BF16),
            pltpu.VMEM((2, NE, 4, CAP, dim), BF16),
            pltpu.VMEM((pieces, tokens // pieces, dim), F32),
            pltpu.VMEM((2, pieces, tokens // pieces, dim), F32),
            pltpu.VMEM((pieces, tokens // pieces, dim), BF16),
            pltpu.VMEM((tokens, dim), BF16),
            dma((2,)), dma((2,)), dma((2, 3)), dma((3,)), dma, dma((1, 4)), dma((2, NE, 4)), dma,
            dma((2, 3)), dma((2, 3)), dma((NE, 2, 3)), dma((NE, 2, 3)),
            dma((2, pieces)), dma((2, pieces)), dma((pieces,)), dma((pieces,)),
        ],
        cost_estimate=pl.CostEstimate(flops=flops, bytes_accessed=80_000_000, transcendentals=0),
        compiler_params=pltpu.CompilerParams(collective_id=1, has_side_effects=True,
                                             vmem_limit_bytes=67_043_328),
    )(code, tok, xb, q_rows, w_in, w_up, w_out, c_rows)


def settle_kernel(*refs):
    count = (len(refs) - 2) // 3
    srcs, dsts, bufs = refs[:count], refs[count:2 * count], refs[2 * count:3 * count]
    rsem, wsem = refs[3 * count:]
    parts = [(k, i) for i in range(4) for k in range(count)]
    reads, writes = [], []
    for n, (k, i) in enumerate(parts):
        reads.append(pltpu.make_async_copy(srcs[k].at[i], bufs[k].at[i], rsem.at[n]))
        writes.append(pltpu.make_async_copy(bufs[k].at[i], dsts[k].at[i], wsem.at[n]))
        reads[-1].start()
    for read, write in zip(reads, writes):
        read.wait()
        write.start()
    for write in writes:
        write.wait()


def run_settle(arrays):
    flat = [a.reshape(4, -1, a.shape[-1]) for a in arrays]
    any_spec = pl.BlockSpec(memory_space=pl.ANY)
    count = len(flat)
    outs = pl.pallas_call(
        settle_kernel,
        name='settle',
        out_shape=tuple(jax.ShapeDtypeStruct(a.shape, a.dtype) for a in flat),
        in_specs=[any_spec] * count,
        out_specs=[any_spec] * count,
        scratch_shapes=[pltpu.VMEM(a.shape, a.dtype) for a in flat] + [
            pltpu.SemaphoreType.DMA((4 * count,)), pltpu.SemaphoreType.DMA((4 * count,))],
        compiler_params=pltpu.CompilerParams(vmem_limit_bytes=64_000_000),
    )(*flat)
    return [out.reshape(a.shape) for out, a in zip(outs, arrays)]


def solution(mesh):
    def device_fn(x_acts, expert_ids, gate_wts, w_in, w_up, w_out, d_out):
        ids_t = jnp.swapaxes(expert_ids[:, 0], 1, 2)
        gates_t = jnp.swapaxes(gate_wts[:, 0], 1, 2)
        c_rows, xb, q_rows, code, tok = run_dispatch(x_acts, d_out, ids_t, gates_t, w_in, w_up, w_out)
        y_dev, dx_dev, dw_in, dw_up, dw_out = run_settle(run_finish(
            code, tok, xb, q_rows, w_in, w_up, w_out, c_rows)[:5])
        return y_dev[None], dx_dev[None], dw_in, dw_up, dw_out

    tok_spec = P(None, 'stage', 'expert', None)
    w_spec = P('stage', 'expert', None, None)
    row_spec = P('stage', 'expert', None)
    return jax.shard_map(device_fn, mesh=mesh,
                         in_specs=(tok_spec, tok_spec, tok_spec, w_spec, w_spec, w_spec, row_spec),
                         out_specs=(row_spec, row_spec, w_spec, w_spec, w_spec), check_vma=False)
```

```python
import jax
import jax.numpy as jnp
from jax import lax
from jax.experimental import pallas as pl
from jax.experimental.pallas import tpu as pltpu
from jax.sharding import PartitionSpec as P

MESH = pl.DeviceIdType.MESH
F32, BF16 = jnp.float32, jnp.bfloat16
DY, XF, XB, IDS, GTS = 0, 1, 2, 3, 4
NG, NE, CAP = 8, 4, 192


def dot(lhs, rhs, dims=((1,), (0,))):
    return lax.dot_general(lhs, rhs, (dims, ((), ())), preferred_element_type=F32)


def slot_hits(code_rows, tokens):
    slot = lax.broadcasted_iota(jnp.int32, (CAP, tokens), 0).astype(F32)
    return [slot == code_rows[e:e + 1, :] for e in range(NE)]


def dispatch_kernel(x_ref, dy_ref, ids_ref, gts_ref, win_ref, wup_ref, wout_ref,
                    c_ref, xb_ref, q_ref, code_ref, tok_ref,
                    buf, tab_ids, tab_gts, codes, gates, gslot, xs, st, cst, wbuf, tok,
                    ssem, rsem, lsem, wsem, stsem, csem, tsem):
    stage = lax.axis_index('stage')
    me = lax.axis_index('expert')
    other = 1 - stage
    core = me % 2
    xn = me + 2 - 4 * ((me // 2) % 2)
    yn = me + 4 - 8 * (me // 4)
    dg = xn + 4 - 8 * (xn // 4)
    sib_of = lambda h: h + 1 - 2 * core
    sib = sib_of(me)
    tokens = x_ref.shape[2]
    half = tokens // 2
    sends = []

    barrier = pltpu.get_barrier_semaphore()
    for peer in ((other, me), (stage, sib), (stage, xn), (stage, yn)):
        pl.semaphore_signal(barrier, inc=1, device_id=peer, device_id_type=MESH)
    pl.semaphore_wait(barrier, 4)

    def place(arr, h, part):
        if arr == IDS:
            return tab_ids.at[h]
        if arr == GTS:
            return tab_gts.at[h]
        if arr == XB:
            return xb_ref.at[h, pl.ds(part * half, half)]
        return buf.at[arr, h, pl.ds(part * half, half)]

    def remote(arr, h, part, slot, peer, src=None):
        return pltpu.make_async_remote_copy(
            src_ref=place(arr, h, part) if src is None else src, dst_ref=place(arr, h, part),
            send_sem=ssem.at[arr, slot], recv_sem=rsem.at[arr, h, part],
            device_id=peer, device_id_type=MESH)

    def send(arr, h, part, peer, src=None):
        sends.append((arr, h, part, sum(done[0] == arr for done in sends), peer, src))
        remote(*sends[-1]).start()

    def arrived(arr, h, part):
        remote(arr, h, part, 0, (stage, sib)).wait_recv()

    to_x, to_y, to_sib, to_z = (stage, xn), (stage, yn), (stage, sib), (other, me)

    send(IDS, me, 0, to_z, ids_ref)
    send(GTS, me, 0, to_z, gts_ref)
    for part in range(2):
        send(XF, me, part, to_z, x_ref.at[1, 0, pl.ds(part * half, half)])
    for part in range(2):
        send(XB, me, part, to_z, x_ref.at[0, 0, pl.ds(part * half, half)])
    dy_half = lambda part: dy_ref.at[0, pl.ds(part * half, half)]
    send(DY, me, 0, to_x, dy_half(0))
    send(DY, me, 1, to_y, dy_half(1))
    send(DY, me, 0, to_sib, dy_half(0))
    send(DY, me, 1, to_sib, dy_half(1))
    own_dy = pltpu.make_async_copy(dy_ref.at[0], buf.at[DY, me], lsem)
    own_dy.start()

    def weights(e):
        return [pltpu.make_async_copy(w.at[0, e], wbuf.at[e % 2, k], wsem.at[e % 2, k])
                for k, w in enumerate((win_ref, wup_ref, wout_ref))]

    for e in range(2):
        for copy in weights(e):
            copy.start()

    for arr in (IDS, GTS):
        arrived(arr, me, 0)
        send(arr, me, 0, to_x)
        send(arr, me, 0, to_y)
        send(arr, me, 0, to_sib)
    send(DY, me, 1, to_x, dy_half(1))
    send(DY, me, 0, to_y, dy_half(0))

    def first_halves(arr):
        arrived(arr, xn, 0)
        arrived(arr, yn, 1)
        send(arr, xn, 0, to_y)
        send(arr, yn, 1, to_x)
        send(arr, xn, 0, to_sib)
        send(arr, yn, 1, to_sib)

    def second_halves(arr):
        arrived(arr, xn, 1)
        arrived(arr, yn, 0)
        send(arr, xn, 1, to_sib)
        send(arr, yn, 0, to_sib)

    def diagonal(arr):
        for part in range(2):
            arrived(arr, dg, part)
            send(arr, dg, part, to_sib)

    def own_sends(arr):
        for part in range(2):
            arrived(arr, me, part)
        send(arr, me, 0, to_x)
        send(arr, me, 1, to_y)
        send(arr, me, 1, to_x)
        send(arr, me, 0, to_y)
        send(arr, me, 0, to_sib)
        send(arr, me, 1, to_sib)

    for arr in (IDS, GTS):
        arrived(arr, xn, 0)
        arrived(arr, yn, 0)
        send(arr, xn, 0, to_y)
    first_halves(DY)
    for arr in (IDS, GTS):
        send(arr, xn, 0, to_sib)
        send(arr, yn, 0, to_sib)
    own_sends(XF)
    second_halves(DY)
    for arr in (IDS, GTS):
        arrived(arr, dg, 0)
        send(arr, dg, 0, to_sib)
        for h in (sib, sib_of(xn), sib_of(yn), sib_of(dg)):
            arrived(arr, h, 0)

    upper = (lax.broadcasted_iota(jnp.int32, (tokens, tokens), 0)
             <= lax.broadcasted_iota(jnp.int32, (tokens, tokens), 1)).astype(F32).astype(BF16)
    for kind in range(2):
        taken = []
        for h in range(NG):
            for e in range(NE):
                eq = tab_ids[h, 1 - kind] == me * NE + e
                taken.append(jnp.sum(jnp.where(eq, 1.0, 0.0), axis=0, keepdims=True))
                gates[kind, h, e:e + 1, :] = jnp.sum(jnp.where(eq, tab_gts[h, 1 - kind], 0.0), axis=0,
                                                     keepdims=True)
        taken = jnp.concatenate(taken, axis=0)
        rank = dot(taken.astype(BF16), upper) - 1.0
        code = jnp.where(taken > 0.5, rank, -1.0)
        for h in range(NG):
            codes[kind, h, 0:NE, :] = code[h * NE:(h + 1) * NE, :]
            codes[kind, h, NE:8, :] = jnp.full((8 - NE, tokens), -1.0, F32)
    code_copy = pltpu.make_async_copy(codes.at[1], code_ref, tsem.at[0])
    code_copy.start()

    partner = yn + core * (xn - yn)
    lower = (lax.broadcasted_iota(jnp.int32, (tokens, tokens), 0)
             >= lax.broadcasted_iota(jnp.int32, (tokens, tokens), 1)).astype(F32).astype(BF16)
    for n, h in enumerate((me, partner)):
        both = jnp.concatenate([tab_ids[h, 0], tab_ids[h, 1]], axis=0).astype(F32).T
        for kind in range(2):
            tok[kind, n] = token_codes(both[:, 4 * (1 - kind):4 * (1 - kind) + 4], lower)
    tok_copy = pltpu.make_async_copy(tok, tok_ref, tsem.at[1])
    tok_copy.start()

    def shard(i):
        j, odd = i // 2, i % 2
        return me + (j % 2) * (xn - me) + (j // 2) * (yn - me) + odd * (1 - 2 * core)

    def gather(kind, arr, h):
        hits = slot_hits(codes[kind, h], tokens)
        gate_rows = gates[kind, h]
        onehot = jnp.concatenate([jnp.where(hit, 1.0, 0.0).astype(BF16) for hit in hits], axis=0)
        slot_gate = [jnp.sum(jnp.where(hits[e], gate_rows[e:e + 1, :], 0.0), axis=1, keepdims=True)
                     for e in range(NE)]
        return dot(onehot, buf[arr, h]), slot_gate

    def q_copy(slot, h):
        return pltpu.make_async_copy(st.at[slot], q_ref.at[:, h], stsem.at[slot])

    def sibling_part(arr, i):
        @pl.when(i % 2 == 1)
        def _():
            arrived(arr, shard(i), 0)
            arrived(arr, shard(i), 1)

    own_dy.wait()

    @pl.loop(0, NG)
    def _(i):
        pl.when(i == 6)(lambda: diagonal(DY))
        sibling_part(DY, i)
        h, slot = shard(i), i % 2
        pl.when(i >= 2)(lambda: q_copy(slot, h).wait())
        rows, slot_gate = gather(1, DY, h)
        for e in range(NE):
            st[slot, e] = (slot_gate[e] * rows[e * CAP:(e + 1) * CAP]).astype(BF16)
        q_copy(slot, h).start()

    first_halves(XF)
    own_sends(XB)

    @pl.loop(0, NG)
    def _(i):
        pl.when(i == 2)(lambda: second_halves(XF))
        pl.when(i == 6)(lambda: diagonal(XF))
        sibling_part(XF, i)
        h = shard(i)
        rows, slot_gate = gather(0, XF, h)
        for e in range(NE):
            xs[e, h] = rows[e * CAP:(e + 1) * CAP].astype(BF16)
            gslot[e, h] = jnp.broadcast_to(slot_gate[e], (CAP, 128))

    chunk = 2
    steps = NG // chunk
    rows_chunk = chunk * CAP

    def c_copy(slot, e, h0):
        return pltpu.make_async_copy(cst.at[slot], c_ref.at[pl.ds(h0, chunk), e], csem.at[slot])

    @pl.loop(0, NE)
    def _(e):
        pl.when(e == 1)(lambda: first_halves(XB))
        pl.when(e == 3)(lambda: second_halves(XB))
        for copy in weights(e):
            copy.wait()

        @pl.loop(0, steps)
        def _(i):
            slot = i % 2
            h0 = i * chunk
            rows = xs[e, pl.ds(h0, chunk)].reshape(rows_chunk, -1)
            pre = dot(rows, wbuf[e % 2, 0])
            act = pre * jax.nn.sigmoid(pre)
            hidden = (act * dot(rows, wbuf[e % 2, 1])).astype(BF16)
            out = dot(hidden, wbuf[e % 2, 2])
            gate = gslot[e, pl.ds(h0, chunk)].reshape(rows_chunk, 128)[:, 0:1]
            pl.when(e * steps + i >= 2)(lambda: c_copy(slot, e, h0).wait())
            cst[slot] = (gate * out).astype(BF16).reshape(chunk, CAP, -1)
            c_copy(slot, e, h0).start()

        @pl.when(e + 2 < NE)
        def _():
            for copy in weights(e + 2):
                copy.start()

    diagonal(XB)
    for h in (sib, sib_of(xn), sib_of(yn), sib_of(dg)):
        arrived(XB, h, 0)
        arrived(XB, h, 1)
    for slot in range(2):
        c_copy(slot, NE - 1, 0).wait()
        q_copy(slot, 0).wait()
    code_copy.wait()
    tok_copy.wait()
    for args in sends:
        remote(*args).wait_send()


def run_dispatch(x_acts, d_out, ids, gts, w_in, w_up, w_out):
    tokens, dim = x_acts.shape[2:]
    hid = w_in.shape[3]
    any_spec = pl.BlockSpec(memory_space=pl.ANY)
    flops = 2 * NG * NE * CAP * (2 * tokens * dim + 3 * dim * hid)
    return pl.pallas_call(
        dispatch_kernel,
        name='dispatch',
        out_shape=(jax.ShapeDtypeStruct((NG, NE, CAP, dim), BF16),
                   jax.ShapeDtypeStruct((NG, tokens, dim), BF16),
                   jax.ShapeDtypeStruct((NE, NG, CAP, dim), BF16),
                   jax.ShapeDtypeStruct((NG, 8, tokens), F32),
                   jax.ShapeDtypeStruct((2, 2, tokens, 128), F32)),
        in_specs=[any_spec] * 7,
        out_specs=[any_spec] * 5,
        scratch_shapes=[
            pltpu.VMEM((2, NG, tokens, dim), BF16),
            pltpu.VMEM((NG, 2, 4, tokens), jnp.int32),
            pltpu.VMEM((NG, 2, 4, tokens), F32),
            pltpu.VMEM((2, NG, 8, tokens), F32),
            pltpu.VMEM((2, NG, 8, tokens), F32),
            pltpu.VMEM((NE, NG, CAP, 128), F32),
            pltpu.VMEM((NE, NG, CAP, dim), BF16),
            pltpu.VMEM((2, NE, CAP, dim), BF16),
            pltpu.VMEM((2, 2, CAP, dim), BF16),
            pltpu.VMEM((2, 3, dim, hid), BF16),
            pltpu.VMEM((2, 2, tokens, 128), F32),
            pltpu.SemaphoreType.DMA((5, 16)),
            pltpu.SemaphoreType.DMA((5, NG, 2)),
            pltpu.SemaphoreType.DMA,
            pltpu.SemaphoreType.DMA((2, 3)),
            pltpu.SemaphoreType.DMA((2,)),
            pltpu.SemaphoreType.DMA((2,)),
            pltpu.SemaphoreType.DMA((2,)),
        ],
        cost_estimate=pl.CostEstimate(flops=flops, bytes_accessed=60_000_000, transcendentals=0),
        compiler_params=pltpu.CompilerParams(collective_id=0, has_side_effects=True,
                                             vmem_limit_bytes=67_043_328),
    )(x_acts, d_out, ids, gts, w_in, w_up, w_out)


def token_codes(ids, lower):
    tokens, top_k = ids.shape
    experts = lax.broadcasted_iota(jnp.int32, (tokens, 128), 1).astype(F32)
    taken = jnp.zeros((tokens, 128), F32)
    for j in range(top_k):
        taken += jnp.where(ids[:, j:j + 1] == experts, 1.0, 0.0)
    rank = dot(lower, taken.astype(BF16)) - 1.0
    return jnp.where(taken > 0.5, rank, -10000.0)


def slot_matrix(cols):
    tokens = cols[0].shape[0]
    lane = lax.broadcasted_iota(jnp.int32, (tokens, 128), 1).astype(F32)
    blocks = []
    for b in range(len(cols) * CAP // 128):
        hit = None
        for k, col in enumerate(cols):
            if k * CAP < (b + 1) * 128 and (k + 1) * CAP > b * 128:
                eq = lane == col + float(k * CAP - b * 128)
                hit = eq if hit is None else hit | eq
        blocks.append(jnp.where(hit, 1.0, 0.0).astype(BF16))
    return jnp.concatenate(blocks, axis=1)


def finish_kernel(code_ref, tok_ref, xb_ref, q_ref, win_ref, wup_ref, wout_ref, c_ref,
                  y_ref, dx_ref, dwin_ref, dwup_ref, dwout_ref, yhop_ref, dhop_ref, rows_ref,
                  xbuf, xs, qbuf, wbuf, acc_in, acc_up, acc_out, dwst, dxst, rbuf, part_out, part_in,
                  out_buf, y_buf,
                  xsem, qsem, wsem, dwsem, dxsem, rbsem, rdsem, ysem,
                  ssem, rsem, dsem, drsem, psem, prsem, zsem, zrsem):
    stage = lax.axis_index('stage')
    me = lax.axis_index('expert')
    core = me % 2
    sib_of = lambda h: h + 1 - 2 * (h % 2)
    sib = sib_of(me)
    xn = me + 2 - 4 * ((me // 2) % 2)
    yn = me + 4 - 8 * (me // 4)
    dg = xn + 4 - 8 * (xn // 4)
    partner = yn + core * (xn - yn)
    line = xn + core * (yn - xn)
    line0 = 2 * (line // 2)
    tokens, dim = y_buf.shape
    pieces, piece = part_out.shape[1:3]
    held = pieces // 2
    tchunk = 256
    per_chunk = tchunk // piece

    barrier = pltpu.get_barrier_semaphore()
    for peer in ((1 - stage, me), (stage, sib), (stage, xn), (stage, yn), (stage, sib_of(xn)),
                 (stage, sib_of(yn))):
        pl.semaphore_signal(barrier, inc=1, device_id=peer, device_id_type=MESH)
    pl.semaphore_wait(barrier, 6)

    targets = ((2 * (xn // 2), 2 * (dg // 2), 1 + core), (2 * (yn // 2) + 1, 2 * (dg // 2) + 1, 1 + core),
               (sib, sib_of(xn) + core * (sib_of(yn) - sib_of(xn)), 0))

    def y_hop(role, k):
        target, via, slot = targets[k]
        return pltpu.make_async_remote_copy(
            src_ref=c_ref.at[via if role == 0 else target], dst_ref=yhop_ref.at[role, slot],
            send_sem=ssem.at[role, k], recv_sem=rsem.at[role, slot],
            device_id=(stage, target), device_id_type=MESH)

    def y_arrived(role, slot):
        pltpu.make_async_remote_copy(
            src_ref=c_ref.at[me], dst_ref=yhop_ref.at[role, slot], send_sem=ssem.at[role, 0],
            recv_sem=rsem.at[role, slot], device_id=(stage, sib), device_id_type=MESH).wait_recv()

    def d_hop(role, k, e):
        target, via, slot = targets[k]
        return pltpu.make_async_remote_copy(
            src_ref=rows_ref.at[via if role == 0 else target, e], dst_ref=dhop_ref.at[role, slot, e],
            send_sem=dsem.at[e, role, k], recv_sem=drsem.at[e, role, slot],
            device_id=(stage, target), device_id_type=MESH)

    def d_arrived(role, slot, e):
        pltpu.make_async_remote_copy(
            src_ref=rows_ref.at[me, e], dst_ref=dhop_ref.at[role, slot, e], send_sem=dsem.at[e, role, 0],
            recv_sem=drsem.at[e, role, slot], device_id=(stage, sib), device_id_type=MESH).wait_recv()

    for role in range(2):
        for k in range(3):
            y_hop(role, k).start()

    def weights(e):
        return [pltpu.make_async_copy(w.at[0, e], wbuf.at[e % 2, k], wsem.at[e % 2, k])
                for k, w in enumerate((win_ref, wup_ref, wout_ref))] + [
            pltpu.make_async_copy(q_ref.at[e], qbuf.at[e % 2], qsem.at[e % 2])]

    def x_fetch(h):
        return pltpu.make_async_copy(xb_ref.at[h], xbuf.at[h % 2], xsem.at[h % 2])

    x_fetch(0).start()
    for e in range(2):
        for copy in weights(e):
            copy.start()

    @pl.loop(0, NG)
    def _(h):
        pl.when(h + 1 < NG)(lambda: x_fetch(h + 1).start())
        hits = slot_hits(code_ref[h], tokens)
        onehot = jnp.concatenate([jnp.where(hit, 1.0, 0.0).astype(BF16) for hit in hits], axis=0)
        x_fetch(h).wait()
        rows = dot(onehot, xbuf[h % 2]).astype(BF16)
        for e in range(NE):
            xs[e, h] = rows[e * CAP:(e + 1) * CAP]

    sources = (sib, line0, line0 + 1, me)

    def y_load(role):
        copies = [pltpu.make_async_copy(yhop_ref.at[role, slot], rbuf.at[0, :, slot], rbsem.at[0, slot])
                  for slot in range(3)]
        copies.append(pltpu.make_async_copy(c_ref.at[partner if role == 0 else me], rbuf.at[0, :, 3],
                                            rbsem.at[0, 3]))
        for copy in copies:
            copy.start()
        for copy in copies:
            copy.wait()

    def d_load(role, e):
        copies = [pltpu.make_async_copy(dhop_ref.at[role, slot, e], rbuf.at[role, e, slot],
                                        rdsem.at[role, e, slot])
                  for slot in range(3)]
        return copies + [pltpu.make_async_copy(rows_ref.at[partner if role == 0 else me, e],
                                               rbuf.at[role, e, 3], rdsem.at[role, e, 3])]

    def d_fetch(role, experts):
        for e in experts:
            for slot in range(3):
                d_arrived(role, slot, e)
            for copy in d_load(role, e):
                copy.start()

    def combine(kind, role, buf, chunk, experts):
        code = tok_ref[kind, 1 - role, pl.ds(chunk * tchunk, tchunk)]
        codes = [pltpu.roll(code, (128 - NE * d) % 128, 1) for d in sources]
        total = None
        for e in experts:
            part = dot(slot_matrix([c[:, e:e + 1] for c in codes]), rbuf[buf, e].reshape(NE * CAP, dim))
            total = part if total is None else total + part
        return total

    every = tuple(range(NE))

    def partial_copy(kind, i):
        return pltpu.make_async_remote_copy(
            src_ref=part_out.at[kind, i], dst_ref=part_in.at[kind, i], send_sem=psem.at[kind, i],
            recv_sem=prsem.at[kind, i], device_id=(stage, partner), device_id_type=MESH)

    def z_copy(i):
        return pltpu.make_async_remote_copy(
            src_ref=out_buf.at[i], dst_ref=dx_ref.at[pl.ds(i * piece, piece)], send_sem=zsem.at[i],
            recv_sem=zrsem.at[i], device_id=(1 - stage, me), device_id_type=MESH)

    def pass_on(kind, experts, first):
        @pl.loop(0, tokens // tchunk)
        def _(chunk):
            total = combine(kind, 0, 0, chunk, experts)
            for p in range(per_chunk):
                i = chunk * per_chunk + p
                part = total[p * piece:(p + 1) * piece]
                part_out[kind, i] = part if first else part_out[kind, i] + part
            if experts[-1] == NE - 1:
                for p in range(per_chunk):
                    i = chunk * per_chunk + p
                    if kind:
                        partial_copy(kind, i).start()
                    else:
                        pl.when(i < held)(lambda: partial_copy(kind, i).start())

    def y_pass_on():
        for slot in range(3):
            y_arrived(0, slot)
        y_load(0)
        pass_on(0, every, True)

    chunk = 4
    rows_chunk = chunk * CAP
    grads = ((acc_in, dwin_ref), (acc_up, dwup_ref), (acc_out, dwout_ref))

    def grad_copies(e):
        return [pltpu.make_async_copy(dwst.at[k], ref.at[0, e], dwsem.at[k])
                for k, (_, ref) in enumerate(grads)]

    @pl.loop(0, NE)
    def _(e):
        pl.when(e == 1)(y_pass_on)
        for copy in weights(e):
            copy.wait()
        w_in, w_up, w_out = (wbuf[e % 2, k] for k in range(3))

        @pl.loop(0, NG // chunk)
        def _(i):
            hs = pl.ds(i * chunk, chunk)
            x = xs[e, hs].reshape(rows_chunk, dim)
            q = qbuf[e % 2, hs].reshape(rows_chunk, dim)
            pre_in = dot(x, w_in)
            pre_up = dot(x, w_up)
            d_hid = dot(q, w_out, ((1,), (1,)))
            sig = jax.nn.sigmoid(pre_in)
            act = pre_in * sig
            hidden = (act * pre_up).astype(BF16)
            d_in = (d_hid * pre_up * sig * (1.0 + pre_in * (1.0 - sig))).astype(BF16)
            d_up = (d_hid * act).astype(BF16)
            dx = dot(d_in, w_in, ((1,), (1,))) + dot(d_up, w_up, ((1,), (1,)))
            dxst[hs] = dx.astype(BF16).reshape(chunk, CAP, dim)
            parts = (dot(x, d_in, ((0,), (0,))), dot(x, d_up, ((0,), (0,))), dot(hidden, q, ((0,), (0,))))
            for (acc, _), part in zip(grads, parts):
                acc[...] = jnp.where(i == 0, part, acc[...] + part)

        out = pltpu.make_async_copy(dxst, rows_ref.at[:, e], dxsem)
        out.start()

        @pl.when(e >= 1)
        def _():
            for copy in grad_copies(e - 1):
                copy.wait()

        for k, (acc, _) in enumerate(grads):
            dwst[k] = acc[...].astype(BF16)
        for copy in grad_copies(e):
            copy.start()

        @pl.when(e + 2 < NE)
        def _():
            for copy in weights(e + 2):
                copy.start()

        out.wait()
        for role in range(2):
            for k in range(3):
                d_hop(role, k, e).start()

    @pl.loop(held, pieces)
    def _(i):
        partial_copy(0, i).start()

    def d_ready(role, experts):
        for e in experts:
            for copy in d_load(role, e):
                copy.wait()

    d_fetch(0, every[:-1])
    d_ready(0, every[:-1])
    pass_on(1, every[:-1], True)
    d_fetch(1, every[:-1])
    d_fetch(0, every[-1:])
    d_ready(0, every[-1:])
    pass_on(1, every[-1:], False)

    for slot in range(3):
        y_arrived(1, slot)
    y_load(1)

    @pl.loop(0, tokens // tchunk)
    def _(chunk):
        total = combine(0, 1, 0, chunk, every)
        for p in range(per_chunk):
            i = chunk * per_chunk + p
            partial_copy(0, i).wait_recv()
            y_buf[pl.ds(i * piece, piece)] = (total[p * piece:(p + 1) * piece] + part_in[0, i]).astype(BF16)
            partial_copy(0, i).wait_send()

    y_out = pltpu.make_async_copy(y_buf, y_ref, ysem)
    y_out.start()

    d_fetch(1, every[-1:])
    d_ready(1, every)

    @pl.loop(0, tokens // tchunk)
    def _(chunk):
        total = combine(1, 1, 1, chunk, every)
        for p in range(per_chunk):
            i = chunk * per_chunk + p
            partial_copy(1, i).wait_recv()
            out_buf[i] = (total[p * piece:(p + 1) * piece] + part_in[1, i]).astype(BF16)
            z_copy(i).start()

    y_out.wait()
    for copy in grad_copies(NE - 1):
        copy.wait()
    for role in range(2):
        for k in range(3):
            y_hop(role, k).wait_send()

            @pl.loop(0, NE)
            def _(e):
                d_hop(role, k, e).wait_send()

    @pl.loop(0, pieces)
    def _(i):
        partial_copy(1, i).wait_send()
        z_copy(i).wait()


def run_finish(code, tok, xb, q_rows, w_in, w_up, w_out, c_rows):
    tokens, dim = xb.shape[1:]
    hid = w_in.shape[3]
    pieces = 16
    any_spec = pl.BlockSpec(memory_space=pl.ANY)
    vmem_spec = pl.BlockSpec(memory_space=pltpu.VMEM)
    tok_shape = jax.ShapeDtypeStruct((tokens, dim), BF16)
    hop_shape = jax.ShapeDtypeStruct((2, 3, NE, CAP, dim), BF16)
    dma = pltpu.SemaphoreType.DMA
    flops = 2 * NG * NE * CAP * (3 * tokens * dim + 8 * dim * hid)
    return pl.pallas_call(
        finish_kernel,
        name='finish',
        out_shape=(tok_shape, tok_shape, jax.ShapeDtypeStruct(w_in.shape, BF16),
                   jax.ShapeDtypeStruct(w_up.shape, BF16), jax.ShapeDtypeStruct(w_out.shape, BF16),
                   hop_shape, hop_shape, jax.ShapeDtypeStruct((NG, NE, CAP, dim), BF16)),
        in_specs=[vmem_spec] * 2 + [any_spec] * 6,
        out_specs=[any_spec] * 8,
        scratch_shapes=[
            pltpu.VMEM((2, tokens, dim), BF16),
            pltpu.VMEM((NE, NG, CAP, dim), BF16),
            pltpu.VMEM((2, NG, CAP, dim), BF16),
            pltpu.VMEM((2, 3, dim, hid), BF16),
            pltpu.VMEM((dim, hid), F32),
            pltpu.VMEM((dim, hid), F32),
            pltpu.VMEM((hid, dim), F32),
            pltpu.VMEM((3, dim, hid), BF16),
            pltpu.VMEM((NG, CAP, dim), BF16),
            pltpu.VMEM((2, NE, 4, CAP, dim), BF16),
            pltpu.VMEM((2, pieces, tokens // pieces, dim), F32),
            pltpu.VMEM((2, pieces, tokens // pieces, dim), F32),
            pltpu.VMEM((pieces, tokens // pieces, dim), BF16),
            pltpu.VMEM((tokens, dim), BF16),
            dma((2,)), dma((2,)), dma((2, 3)), dma((3,)), dma, dma((1, 4)), dma((2, NE, 4)), dma,
            dma((2, 3)), dma((2, 3)), dma((NE, 2, 3)), dma((NE, 2, 3)),
            dma((2, pieces)), dma((2, pieces)), dma((pieces,)), dma((pieces,)),
        ],
        cost_estimate=pl.CostEstimate(flops=flops, bytes_accessed=80_000_000, transcendentals=0),
        compiler_params=pltpu.CompilerParams(collective_id=1, has_side_effects=True,
                                             vmem_limit_bytes=67_043_328),
    )(code, tok, xb, q_rows, w_in, w_up, w_out, c_rows)


def settle_kernel(*refs):
    count = (len(refs) - 2) // 3
    srcs, dsts, bufs = refs[:count], refs[count:2 * count], refs[2 * count:3 * count]
    rsem, wsem = refs[3 * count:]
    parts = [(k, i) for i in range(4) for k in range(count)]
    reads, writes = [], []
    for n, (k, i) in enumerate(parts):
        reads.append(pltpu.make_async_copy(srcs[k].at[i], bufs[k].at[i], rsem.at[n]))
        writes.append(pltpu.make_async_copy(bufs[k].at[i], dsts[k].at[i], wsem.at[n]))
        reads[-1].start()
    for read, write in zip(reads, writes):
        read.wait()
        write.start()
    for write in writes:
        write.wait()


def run_settle(arrays):
    flat = [a.reshape(4, -1, a.shape[-1]) for a in arrays]
    any_spec = pl.BlockSpec(memory_space=pl.ANY)
    count = len(flat)
    outs = pl.pallas_call(
        settle_kernel,
        name='settle',
        out_shape=tuple(jax.ShapeDtypeStruct(a.shape, a.dtype) for a in flat),
        in_specs=[any_spec] * count,
        out_specs=[any_spec] * count,
        scratch_shapes=[pltpu.VMEM(a.shape, a.dtype) for a in flat] + [
            pltpu.SemaphoreType.DMA((4 * count,)), pltpu.SemaphoreType.DMA((4 * count,))],
        compiler_params=pltpu.CompilerParams(vmem_limit_bytes=64_000_000),
    )(*flat)
    return [out.reshape(a.shape) for out, a in zip(outs, arrays)]


def solution(mesh):
    def device_fn(x_acts, expert_ids, gate_wts, w_in, w_up, w_out, d_out):
        ids_t = jnp.swapaxes(expert_ids[:, 0], 1, 2)
        gates_t = jnp.swapaxes(gate_wts[:, 0], 1, 2)
        c_rows, xb, q_rows, code, tok = run_dispatch(x_acts, d_out, ids_t, gates_t, w_in, w_up, w_out)
        y_dev, dx_dev, dw_in, dw_up, dw_out = run_settle(run_finish(
            code, tok, xb, q_rows, w_in, w_up, w_out, c_rows)[:5])
        return y_dev[None], dx_dev[None], dw_in, dw_up, dw_out

    tok_spec = P(None, 'stage', 'expert', None)
    w_spec = P('stage', 'expert', None, None)
    row_spec = P('stage', 'expert', None)
    return jax.shard_map(device_fn, mesh=mesh,
                         in_specs=(tok_spec, tok_spec, tok_spec, w_spec, w_spec, w_spec, row_spec),
                         out_specs=(row_spec, row_spec, w_spec, w_spec, w_spec), check_vma=False)
```

```python
import jax
import jax.numpy as jnp
from jax import lax
from jax.experimental import pallas as pl
from jax.experimental.pallas import tpu as pltpu
from jax.sharding import PartitionSpec as P

MESH = pl.DeviceIdType.MESH
F32, BF16 = jnp.float32, jnp.bfloat16
DY, XF, XB, IDS, GTS = 0, 1, 2, 3, 4
NG, NE, CAP = 8, 4, 192


def dot(lhs, rhs, dims=((1,), (0,))):
    return lax.dot_general(lhs, rhs, (dims, ((), ())), preferred_element_type=F32)


def slot_hits(code_rows, tokens):
    slot = lax.broadcasted_iota(jnp.int32, (CAP, tokens), 0).astype(F32)
    return [slot == code_rows[e:e + 1, :] for e in range(NE)]


def dispatch_kernel(x_ref, dy_ref, ids_ref, gts_ref, win_ref, wup_ref, wout_ref,
                    c_ref, xb_ref, q_ref, code_ref, tok_ref,
                    buf, tab_ids, tab_gts, codes, gates, gslot, xs, st, cst, wbuf, tok,
                    ssem, rsem, lsem, wsem, stsem, csem, tsem):
    stage = lax.axis_index('stage')
    me = lax.axis_index('expert')
    other = 1 - stage
    core = me % 2
    xn = me + 2 - 4 * ((me // 2) % 2)
    yn = me + 4 - 8 * (me // 4)
    dg = xn + 4 - 8 * (xn // 4)
    sib_of = lambda h: h + 1 - 2 * core
    sib = sib_of(me)
    tokens = x_ref.shape[2]
    half = tokens // 2
    sends = []

    barrier = pltpu.get_barrier_semaphore()
    for peer in ((other, me), (stage, sib), (stage, xn), (stage, yn)):
        pl.semaphore_signal(barrier, inc=1, device_id=peer, device_id_type=MESH)
    pl.semaphore_wait(barrier, 4)

    def place(arr, h, part):
        if arr == IDS:
            return tab_ids.at[h]
        if arr == GTS:
            return tab_gts.at[h]
        if arr == XB:
            return xb_ref.at[h, pl.ds(part * half, half)]
        return buf.at[arr, h, pl.ds(part * half, half)]

    def remote(arr, h, part, slot, peer, src=None):
        return pltpu.make_async_remote_copy(
            src_ref=place(arr, h, part) if src is None else src, dst_ref=place(arr, h, part),
            send_sem=ssem.at[arr, slot], recv_sem=rsem.at[arr, h, part],
            device_id=peer, device_id_type=MESH)

    def send(arr, h, part, peer, src=None):
        sends.append((arr, h, part, sum(done[0] == arr for done in sends), peer, src))
        remote(*sends[-1]).start()

    def arrived(arr, h, part):
        remote(arr, h, part, 0, (stage, sib)).wait_recv()

    to_x, to_y, to_sib, to_z = (stage, xn), (stage, yn), (stage, sib), (other, me)

    send(IDS, me, 0, to_z, ids_ref)
    send(GTS, me, 0, to_z, gts_ref)
    for part in range(2):
        send(XF, me, part, to_z, x_ref.at[1, 0, pl.ds(part * half, half)])
    for part in range(2):
        send(XB, me, part, to_z, x_ref.at[0, 0, pl.ds(part * half, half)])
    dy_half = lambda part: dy_ref.at[0, pl.ds(part * half, half)]
    send(DY, me, 0, to_x, dy_half(0))
    send(DY, me, 1, to_y, dy_half(1))
    send(DY, me, 0, to_sib, dy_half(0))
    send(DY, me, 1, to_sib, dy_half(1))
    own_dy = pltpu.make_async_copy(dy_ref.at[0], buf.at[DY, me], lsem)
    own_dy.start()

    def weights(e):
        return [pltpu.make_async_copy(w.at[0, e], wbuf.at[e % 2, k], wsem.at[e % 2, k])
                for k, w in enumerate((win_ref, wup_ref, wout_ref))]

    for e in range(2):
        for copy in weights(e):
            copy.start()

    for arr in (IDS, GTS):
        arrived(arr, me, 0)
        send(arr, me, 0, to_x)
        send(arr, me, 0, to_y)
        send(arr, me, 0, to_sib)
    send(DY, me, 1, to_x, dy_half(1))
    send(DY, me, 0, to_y, dy_half(0))

    def first_halves(arr):
        arrived(arr, xn, 0)
        arrived(arr, yn, 1)
        send(arr, xn, 0, to_y)
        send(arr, yn, 1, to_x)
        send(arr, xn, 0, to_sib)
        send(arr, yn, 1, to_sib)

    def second_halves(arr):
        arrived(arr, xn, 1)
        arrived(arr, yn, 0)
        send(arr, xn, 1, to_sib)
        send(arr, yn, 0, to_sib)

    def diagonal(arr):
        for part in range(2):
            arrived(arr, dg, part)
            send(arr, dg, part, to_sib)

    def own_sends(arr):
        for part in range(2):
            arrived(arr, me, part)
        send(arr, me, 0, to_x)
        send(arr, me, 1, to_y)
        send(arr, me, 1, to_x)
        send(arr, me, 0, to_y)
        send(arr, me, 0, to_sib)
        send(arr, me, 1, to_sib)

    for arr in (IDS, GTS):
        arrived(arr, xn, 0)
        arrived(arr, yn, 0)
        send(arr, xn, 0, to_y)
    first_halves(DY)
    for arr in (IDS, GTS):
        send(arr, xn, 0, to_sib)
        send(arr, yn, 0, to_sib)
    own_sends(XF)
    second_halves(DY)
    for arr in (IDS, GTS):
        arrived(arr, dg, 0)
        send(arr, dg, 0, to_sib)
        for h in (sib, sib_of(xn), sib_of(yn), sib_of(dg)):
            arrived(arr, h, 0)

    upper = (lax.broadcasted_iota(jnp.int32, (tokens, tokens), 0)
             <= lax.broadcasted_iota(jnp.int32, (tokens, tokens), 1)).astype(F32).astype(BF16)
    for kind in range(2):
        taken = []
        for h in range(NG):
            for e in range(NE):
                eq = tab_ids[h, 1 - kind] == me * NE + e
                taken.append(jnp.sum(jnp.where(eq, 1.0, 0.0), axis=0, keepdims=True))
                gates[kind, h, e:e + 1, :] = jnp.sum(jnp.where(eq, tab_gts[h, 1 - kind], 0.0), axis=0,
                                                     keepdims=True)
        taken = jnp.concatenate(taken, axis=0)
        rank = dot(taken.astype(BF16), upper) - 1.0
        code = jnp.where(taken > 0.5, rank, -1.0)
        for h in range(NG):
            codes[kind, h, 0:NE, :] = code[h * NE:(h + 1) * NE, :]
            codes[kind, h, NE:8, :] = jnp.full((8 - NE, tokens), -1.0, F32)
    code_copy = pltpu.make_async_copy(codes.at[1], code_ref, tsem.at[0])
    code_copy.start()

    partner = yn + core * (xn - yn)
    lower = (lax.broadcasted_iota(jnp.int32, (tokens, tokens), 0)
             >= lax.broadcasted_iota(jnp.int32, (tokens, tokens), 1)).astype(F32).astype(BF16)
    for n, h in enumerate((me, partner)):
        both = jnp.concatenate([tab_ids[h, 0], tab_ids[h, 1]], axis=0).astype(F32).T
        for kind in range(2):
            tok[kind, n] = token_codes(both[:, 4 * (1 - kind):4 * (1 - kind) + 4], lower)
    tok_copy = pltpu.make_async_copy(tok, tok_ref, tsem.at[1])
    tok_copy.start()

    def shard(i):
        j, odd = i // 2, i % 2
        return me + (j % 2) * (xn - me) + (j // 2) * (yn - me) + odd * (1 - 2 * core)

    def gather(kind, arr, h):
        hits = slot_hits(codes[kind, h], tokens)
        gate_rows = gates[kind, h]
        onehot = jnp.concatenate([jnp.where(hit, 1.0, 0.0).astype(BF16) for hit in hits], axis=0)
        slot_gate = [jnp.sum(jnp.where(hits[e], gate_rows[e:e + 1, :], 0.0), axis=1, keepdims=True)
                     for e in range(NE)]
        return dot(onehot, buf[arr, h]), slot_gate

    def q_copy(slot, h):
        return pltpu.make_async_copy(st.at[slot], q_ref.at[:, h], stsem.at[slot])

    def sibling_part(arr, i):
        @pl.when(i % 2 == 1)
        def _():
            arrived(arr, shard(i), 0)
            arrived(arr, shard(i), 1)

    own_dy.wait()

    @pl.loop(0, NG)
    def _(i):
        pl.when(i == 6)(lambda: diagonal(DY))
        sibling_part(DY, i)
        h, slot = shard(i), i % 2
        pl.when(i >= 2)(lambda: q_copy(slot, h).wait())
        rows, slot_gate = gather(1, DY, h)
        for e in range(NE):
            st[slot, e] = (slot_gate[e] * rows[e * CAP:(e + 1) * CAP]).astype(BF16)
        q_copy(slot, h).start()

    first_halves(XF)
    own_sends(XB)

    @pl.loop(0, NG)
    def _(i):
        pl.when(i == 2)(lambda: second_halves(XF))
        pl.when(i == 6)(lambda: diagonal(XF))
        sibling_part(XF, i)
        h = shard(i)
        rows, slot_gate = gather(0, XF, h)
        for e in range(NE):
            xs[e, h] = rows[e * CAP:(e + 1) * CAP].astype(BF16)
            gslot[e, h] = jnp.broadcast_to(slot_gate[e], (CAP, 128))

    chunk = 2
    steps = NG // chunk
    rows_chunk = chunk * CAP

    def c_copy(slot, e, h0):
        return pltpu.make_async_copy(cst.at[slot], c_ref.at[pl.ds(h0, chunk), e], csem.at[slot])

    @pl.loop(0, NE)
    def _(e):
        pl.when(e == 1)(lambda: first_halves(XB))
        pl.when(e == 3)(lambda: second_halves(XB))
        for copy in weights(e):
            copy.wait()

        @pl.loop(0, steps)
        def _(i):
            slot = i % 2
            h0 = i * chunk
            rows = xs[e, pl.ds(h0, chunk)].reshape(rows_chunk, -1)
            pre = dot(rows, wbuf[e % 2, 0])
            act = pre * jax.nn.sigmoid(pre)
            hidden = (act * dot(rows, wbuf[e % 2, 1])).astype(BF16)
            out = dot(hidden, wbuf[e % 2, 2])
            gate = gslot[e, pl.ds(h0, chunk)].reshape(rows_chunk, 128)[:, 0:1]
            pl.when(e * steps + i >= 2)(lambda: c_copy(slot, e, h0).wait())
            cst[slot] = (gate * out).astype(BF16).reshape(chunk, CAP, -1)
            c_copy(slot, e, h0).start()

        @pl.when(e + 2 < NE)
        def _():
            for copy in weights(e + 2):
                copy.start()

    for h in (sib, sib_of(xn), sib_of(yn), dg):
        arrived(XB, h, 0)
        arrived(XB, h, 1)
    for slot in range(2):
        c_copy(slot, NE - 1, 0).wait()
        q_copy(slot, 0).wait()
    code_copy.wait()
    tok_copy.wait()
    for args in sends:
        remote(*args).wait_send()


def run_dispatch(x_acts, d_out, ids, gts, w_in, w_up, w_out):
    tokens, dim = x_acts.shape[2:]
    hid = w_in.shape[3]
    any_spec = pl.BlockSpec(memory_space=pl.ANY)
    flops = 2 * NG * NE * CAP * (2 * tokens * dim + 3 * dim * hid)
    return pl.pallas_call(
        dispatch_kernel,
        name='dispatch',
        out_shape=(jax.ShapeDtypeStruct((NG, NE, CAP, dim), BF16),
                   jax.ShapeDtypeStruct((NG, tokens, dim), BF16),
                   jax.ShapeDtypeStruct((NE, NG, CAP, dim), BF16),
                   jax.ShapeDtypeStruct((NG, 8, tokens), F32),
                   jax.ShapeDtypeStruct((2, 2, tokens, 128), F32)),
        in_specs=[any_spec] * 7,
        out_specs=[any_spec] * 5,
        scratch_shapes=[
            pltpu.VMEM((2, NG, tokens, dim), BF16),
            pltpu.VMEM((NG, 2, 4, tokens), jnp.int32),
            pltpu.VMEM((NG, 2, 4, tokens), F32),
            pltpu.VMEM((2, NG, 8, tokens), F32),
            pltpu.VMEM((2, NG, 8, tokens), F32),
            pltpu.VMEM((NE, NG, CAP, 128), F32),
            pltpu.VMEM((NE, NG, CAP, dim), BF16),
            pltpu.VMEM((2, NE, CAP, dim), BF16),
            pltpu.VMEM((2, 2, CAP, dim), BF16),
            pltpu.VMEM((2, 3, dim, hid), BF16),
            pltpu.VMEM((2, 2, tokens, 128), F32),
            pltpu.SemaphoreType.DMA((5, 16)),
            pltpu.SemaphoreType.DMA((5, NG, 2)),
            pltpu.SemaphoreType.DMA,
            pltpu.SemaphoreType.DMA((2, 3)),
            pltpu.SemaphoreType.DMA((2,)),
            pltpu.SemaphoreType.DMA((2,)),
            pltpu.SemaphoreType.DMA((2,)),
        ],
        cost_estimate=pl.CostEstimate(flops=flops, bytes_accessed=60_000_000, transcendentals=0),
        compiler_params=pltpu.CompilerParams(collective_id=0, has_side_effects=True,
                                             vmem_limit_bytes=67_043_328),
    )(x_acts, d_out, ids, gts, w_in, w_up, w_out)


def token_codes(ids, lower):
    tokens, top_k = ids.shape
    experts = lax.broadcasted_iota(jnp.int32, (tokens, 128), 1).astype(F32)
    taken = jnp.zeros((tokens, 128), F32)
    for j in range(top_k):
        taken += jnp.where(ids[:, j:j + 1] == experts, 1.0, 0.0)
    rank = dot(lower, taken.astype(BF16)) - 1.0
    return jnp.where(taken > 0.5, rank, -10000.0)


def slot_matrix(cols):
    tokens = cols[0].shape[0]
    lane = lax.broadcasted_iota(jnp.int32, (tokens, 128), 1).astype(F32)
    blocks = []
    for b in range(len(cols) * CAP // 128):
        hit = None
        for k, col in enumerate(cols):
            if k * CAP < (b + 1) * 128 and (k + 1) * CAP > b * 128:
                eq = lane == col + float(k * CAP - b * 128)
                hit = eq if hit is None else hit | eq
        blocks.append(jnp.where(hit, 1.0, 0.0).astype(BF16))
    return jnp.concatenate(blocks, axis=1)


def finish_kernel(code_ref, tok_ref, xb_ref, q_ref, win_ref, wup_ref, wout_ref, c_ref,
                  y_ref, dx_ref, dwin_ref, dwup_ref, dwout_ref, yhop_ref, dhop_ref, rows_ref,
                  xbuf, xs, qbuf, wbuf, acc_in, acc_up, acc_out, dwst, dxst, rbuf, part_out, part_in,
                  out_buf, y_buf,
                  xsem, qsem, wsem, dwsem, dxsem, rbsem, rdsem, ysem, sidesem,
                  ssem, rsem, dsem, drsem, psem, prsem, zsem, zrsem):
    stage = lax.axis_index('stage')
    me = lax.axis_index('expert')
    core = me % 2
    sib_of = lambda h: h + 1 - 2 * (h % 2)
    sib = sib_of(me)
    xn = me + 2 - 4 * ((me // 2) % 2)
    yn = me + 4 - 8 * (me // 4)
    dg = xn + 4 - 8 * (xn // 4)
    partner = yn + core * (xn - yn)
    line = xn + core * (yn - xn)
    line0 = 2 * (line // 2)
    tokens, dim = y_buf.shape
    pieces, piece = part_out.shape[1:3]
    held = pieces // 2
    tchunk = 256
    per_chunk = tchunk // piece

    barrier = pltpu.get_barrier_semaphore()
    for peer in ((1 - stage, me), (stage, sib), (stage, xn), (stage, yn), (stage, sib_of(xn)),
                 (stage, sib_of(yn))):
        pl.semaphore_signal(barrier, inc=1, device_id=peer, device_id_type=MESH)
    pl.semaphore_wait(barrier, 6)

    targets = ((2 * (xn // 2), 2 * (dg // 2), 1 + core), (2 * (yn // 2) + 1, 2 * (dg // 2) + 1, 1 + core),
               (sib, sib_of(xn) + core * (sib_of(yn) - sib_of(xn)), 0))

    def y_hop(role, k):
        target, via, slot = targets[k]
        return pltpu.make_async_remote_copy(
            src_ref=c_ref.at[via if role == 0 else target], dst_ref=yhop_ref.at[role, slot],
            send_sem=ssem.at[role, k], recv_sem=rsem.at[role, slot],
            device_id=(stage, target), device_id_type=MESH)

    def y_arrived(role, slot):
        pltpu.make_async_remote_copy(
            src_ref=c_ref.at[me], dst_ref=yhop_ref.at[role, slot], send_sem=ssem.at[role, 0],
            recv_sem=rsem.at[role, slot], device_id=(stage, sib), device_id_type=MESH).wait_recv()

    def d_hop(role, k, e):
        target, via, slot = targets[k]
        return pltpu.make_async_remote_copy(
            src_ref=rows_ref.at[via if role == 0 else target, e], dst_ref=dhop_ref.at[role, slot, e],
            send_sem=dsem.at[e, role, k], recv_sem=drsem.at[e, role, slot],
            device_id=(stage, target), device_id_type=MESH)

    def d_arrived(role, slot, e):
        pltpu.make_async_remote_copy(
            src_ref=rows_ref.at[me, e], dst_ref=dhop_ref.at[role, slot, e], send_sem=dsem.at[e, role, 0],
            recv_sem=drsem.at[e, role, slot], device_id=(stage, sib), device_id_type=MESH).wait_recv()

    def x_side():
        return pltpu.make_async_remote_copy(
            src_ref=xb_ref.at[dg], dst_ref=y_buf, send_sem=sidesem.at[0], recv_sem=sidesem.at[1],
            device_id=(stage, sib), device_id_type=MESH)

    for role in range(2):
        for k in range(3):
            y_hop(role, k).start()
        if role == 0:
            x_side().start()

    def weights(e):
        return [pltpu.make_async_copy(w.at[0, e], wbuf.at[e % 2, k], wsem.at[e % 2, k])
                for k, w in enumerate((win_ref, wup_ref, wout_ref))] + [
            pltpu.make_async_copy(q_ref.at[e], qbuf.at[e % 2], qsem.at[e % 2])]

    def shard(i):
        j, odd = i // 2, i % 2
        return me + (j % 2) * (xn - me) + (j // 2) * (yn - me) + odd * (sib - me)

    def x_fetch(i):
        return pltpu.make_async_copy(xb_ref.at[shard(i)], xbuf.at[i % 2], xsem.at[i % 2])

    x_fetch(0).start()
    for e in range(2):
        for copy in weights(e):
            copy.start()

    def gather(h, wait, tok_rows):
        hits = slot_hits(code_ref[h], tokens)
        onehot = jnp.concatenate([jnp.where(hit, 1.0, 0.0).astype(BF16) for hit in hits], axis=0)
        wait()
        rows = dot(onehot, tok_rows[...]).astype(BF16)
        for e in range(NE):
            xs[e, h] = rows[e * CAP:(e + 1) * CAP]

    @pl.loop(0, NG - 1)
    def _(i):
        pl.when(i + 1 < NG - 1)(lambda: x_fetch(i + 1).start())
        gather(shard(i), lambda: x_fetch(i).wait(), xbuf.at[i % 2])

    gather(sib_of(dg), x_side().wait_recv, y_buf)

    sources = (sib, line0, line0 + 1, me)

    def y_load(role):
        copies = [pltpu.make_async_copy(yhop_ref.at[role, slot], rbuf.at[0, :, slot], rbsem.at[0, slot])
                  for slot in range(3)]
        copies.append(pltpu.make_async_copy(c_ref.at[partner if role == 0 else me], rbuf.at[0, :, 3],
                                            rbsem.at[0, 3]))
        for copy in copies:
            copy.start()
        for copy in copies:
            copy.wait()

    def d_load(role, e):
        copies = [pltpu.make_async_copy(dhop_ref.at[role, slot, e], rbuf.at[role, e, slot],
                                        rdsem.at[role, e, slot])
                  for slot in range(3)]
        return copies + [pltpu.make_async_copy(rows_ref.at[partner if role == 0 else me, e],
                                               rbuf.at[role, e, 3], rdsem.at[role, e, 3])]

    def d_fetch(role, experts):
        for e in experts:
            for slot in range(3):
                d_arrived(role, slot, e)
            for copy in d_load(role, e):
                copy.start()

    def combine(kind, role, buf, chunk, experts):
        code = tok_ref[kind, 1 - role, pl.ds(chunk * tchunk, tchunk)]
        codes = [pltpu.roll(code, (128 - NE * d) % 128, 1) for d in sources]
        total = None
        for e in experts:
            part = dot(slot_matrix([c[:, e:e + 1] for c in codes]), rbuf[buf, e].reshape(NE * CAP, dim))
            total = part if total is None else total + part
        return total

    every = tuple(range(NE))

    def partial_copy(kind, i):
        return pltpu.make_async_remote_copy(
            src_ref=part_out.at[kind, i], dst_ref=part_in.at[kind, i], send_sem=psem.at[kind, i],
            recv_sem=prsem.at[kind, i], device_id=(stage, partner), device_id_type=MESH)

    def z_copy(i):
        return pltpu.make_async_remote_copy(
            src_ref=out_buf.at[i], dst_ref=dx_ref.at[pl.ds(i * piece, piece)], send_sem=zsem.at[i],
            recv_sem=zrsem.at[i], device_id=(1 - stage, me), device_id_type=MESH)

    def pass_on(kind, experts, first):
        @pl.loop(0, tokens // tchunk)
        def _(chunk):
            total = combine(kind, 0, 0, chunk, experts)
            for p in range(per_chunk):
                i = chunk * per_chunk + p
                part = total[p * piece:(p + 1) * piece]
                part_out[kind, i] = part if first else part_out[kind, i] + part
            if experts[-1] == NE - 1:
                for p in range(per_chunk):
                    i = chunk * per_chunk + p
                    if kind:
                        partial_copy(kind, i).start()
                    else:
                        pl.when(i < held)(lambda: partial_copy(kind, i).start())

    def y_pass_on():
        for slot in range(3):
            y_arrived(0, slot)
        y_load(0)
        pass_on(0, every, True)

    chunk = 4
    rows_chunk = chunk * CAP
    grads = ((acc_in, dwin_ref), (acc_up, dwup_ref), (acc_out, dwout_ref))

    def grad_copies(e):
        return [pltpu.make_async_copy(dwst.at[k], ref.at[0, e], dwsem.at[k])
                for k, (_, ref) in enumerate(grads)]

    @pl.loop(0, NE)
    def _(e):
        pl.when(e == 1)(y_pass_on)
        for copy in weights(e):
            copy.wait()
        w_in, w_up, w_out = (wbuf[e % 2, k] for k in range(3))

        @pl.loop(0, NG // chunk)
        def _(i):
            hs = pl.ds(i * chunk, chunk)
            x = xs[e, hs].reshape(rows_chunk, dim)
            q = qbuf[e % 2, hs].reshape(rows_chunk, dim)
            pre_in = dot(x, w_in)
            pre_up = dot(x, w_up)
            d_hid = dot(q, w_out, ((1,), (1,)))
            sig = jax.nn.sigmoid(pre_in)
            act = pre_in * sig
            hidden = (act * pre_up).astype(BF16)
            d_in = (d_hid * pre_up * sig * (1.0 + pre_in * (1.0 - sig))).astype(BF16)
            d_up = (d_hid * act).astype(BF16)
            dx = dot(d_in, w_in, ((1,), (1,))) + dot(d_up, w_up, ((1,), (1,)))
            dxst[hs] = dx.astype(BF16).reshape(chunk, CAP, dim)
            parts = (dot(x, d_in, ((0,), (0,))), dot(x, d_up, ((0,), (0,))), dot(hidden, q, ((0,), (0,))))
            for (acc, _), part in zip(grads, parts):
                acc[...] = jnp.where(i == 0, part, acc[...] + part)

        out = pltpu.make_async_copy(dxst, rows_ref.at[:, e], dxsem)
        out.start()

        @pl.when(e >= 1)
        def _():
            for copy in grad_copies(e - 1):
                copy.wait()

        for k, (acc, _) in enumerate(grads):
            dwst[k] = acc[...].astype(BF16)
        for copy in grad_copies(e):
            copy.start()

        @pl.when(e + 2 < NE)
        def _():
            for copy in weights(e + 2):
                copy.start()

        out.wait()
        for role in range(2):
            for k in range(3):
                d_hop(role, k, e).start()

    @pl.loop(held, pieces)
    def _(i):
        partial_copy(0, i).start()

    def d_ready(role, experts):
        for e in experts:
            for copy in d_load(role, e):
                copy.wait()

    d_fetch(0, every[:-1])
    d_ready(0, every[:-1])
    pass_on(1, every[:-1], True)
    d_fetch(1, every[:-1])
    d_fetch(0, every[-1:])
    d_ready(0, every[-1:])
    pass_on(1, every[-1:], False)

    for slot in range(3):
        y_arrived(1, slot)
    y_load(1)

    @pl.loop(0, tokens // tchunk)
    def _(chunk):
        total = combine(0, 1, 0, chunk, every)
        for p in range(per_chunk):
            i = chunk * per_chunk + p
            partial_copy(0, i).wait_recv()
            y_buf[pl.ds(i * piece, piece)] = (total[p * piece:(p + 1) * piece] + part_in[0, i]).astype(BF16)
            partial_copy(0, i).wait_send()

    y_out = pltpu.make_async_copy(y_buf, y_ref, ysem)
    y_out.start()

    d_fetch(1, every[-1:])
    d_ready(1, every)

    @pl.loop(0, tokens // tchunk)
    def _(chunk):
        total = combine(1, 1, 1, chunk, every)
        for p in range(per_chunk):
            i = chunk * per_chunk + p
            partial_copy(1, i).wait_recv()
            out_buf[i] = (total[p * piece:(p + 1) * piece] + part_in[1, i]).astype(BF16)
            z_copy(i).start()

    y_out.wait()
    x_side().wait_send()
    for copy in grad_copies(NE - 1):
        copy.wait()
    for role in range(2):
        for k in range(3):
            y_hop(role, k).wait_send()

            @pl.loop(0, NE)
            def _(e):
                d_hop(role, k, e).wait_send()

    @pl.loop(0, pieces)
    def _(i):
        partial_copy(1, i).wait_send()
        z_copy(i).wait()


def run_finish(code, tok, xb, q_rows, w_in, w_up, w_out, c_rows):
    tokens, dim = xb.shape[1:]
    hid = w_in.shape[3]
    pieces = 16
    any_spec = pl.BlockSpec(memory_space=pl.ANY)
    vmem_spec = pl.BlockSpec(memory_space=pltpu.VMEM)
    tok_shape = jax.ShapeDtypeStruct((tokens, dim), BF16)
    hop_shape = jax.ShapeDtypeStruct((2, 3, NE, CAP, dim), BF16)
    dma = pltpu.SemaphoreType.DMA
    flops = 2 * NG * NE * CAP * (3 * tokens * dim + 8 * dim * hid)
    return pl.pallas_call(
        finish_kernel,
        name='finish',
        out_shape=(tok_shape, tok_shape, jax.ShapeDtypeStruct(w_in.shape, BF16),
                   jax.ShapeDtypeStruct(w_up.shape, BF16), jax.ShapeDtypeStruct(w_out.shape, BF16),
                   hop_shape, hop_shape, jax.ShapeDtypeStruct((NG, NE, CAP, dim), BF16)),
        in_specs=[vmem_spec] * 2 + [any_spec] * 6,
        out_specs=[any_spec] * 8,
        scratch_shapes=[
            pltpu.VMEM((2, tokens, dim), BF16),
            pltpu.VMEM((NE, NG, CAP, dim), BF16),
            pltpu.VMEM((2, NG, CAP, dim), BF16),
            pltpu.VMEM((2, 3, dim, hid), BF16),
            pltpu.VMEM((dim, hid), F32),
            pltpu.VMEM((dim, hid), F32),
            pltpu.VMEM((hid, dim), F32),
            pltpu.VMEM((3, dim, hid), BF16),
            pltpu.VMEM((NG, CAP, dim), BF16),
            pltpu.VMEM((2, NE, 4, CAP, dim), BF16),
            pltpu.VMEM((2, pieces, tokens // pieces, dim), F32),
            pltpu.VMEM((2, pieces, tokens // pieces, dim), F32),
            pltpu.VMEM((pieces, tokens // pieces, dim), BF16),
            pltpu.VMEM((tokens, dim), BF16),
            dma((2,)), dma((2,)), dma((2, 3)), dma((3,)), dma, dma((1, 4)), dma((2, NE, 4)), dma, dma((2,)),
            dma((2, 3)), dma((2, 3)), dma((NE, 2, 3)), dma((NE, 2, 3)),
            dma((2, pieces)), dma((2, pieces)), dma((pieces,)), dma((pieces,)),
        ],
        cost_estimate=pl.CostEstimate(flops=flops, bytes_accessed=80_000_000, transcendentals=0),
        compiler_params=pltpu.CompilerParams(collective_id=1, has_side_effects=True,
                                             vmem_limit_bytes=67_043_328),
    )(code, tok, xb, q_rows, w_in, w_up, w_out, c_rows)


def settle_kernel(*refs):
    count = (len(refs) - 2) // 3
    srcs, dsts, bufs = refs[:count], refs[count:2 * count], refs[2 * count:3 * count]
    rsem, wsem = refs[3 * count:]
    parts = [(k, i) for i in range(4) for k in range(count)]
    reads, writes = [], []
    for n, (k, i) in enumerate(parts):
        reads.append(pltpu.make_async_copy(srcs[k].at[i], bufs[k].at[i], rsem.at[n]))
        writes.append(pltpu.make_async_copy(bufs[k].at[i], dsts[k].at[i], wsem.at[n]))
        reads[-1].start()
    for read, write in zip(reads, writes):
        read.wait()
        write.start()
    for write in writes:
        write.wait()


def run_settle(arrays):
    flat = [a.reshape(4, -1, a.shape[-1]) for a in arrays]
    any_spec = pl.BlockSpec(memory_space=pl.ANY)
    count = len(flat)
    outs = pl.pallas_call(
        settle_kernel,
        name='settle',
        out_shape=tuple(jax.ShapeDtypeStruct(a.shape, a.dtype) for a in flat),
        in_specs=[any_spec] * count,
        out_specs=[any_spec] * count,
        scratch_shapes=[pltpu.VMEM(a.shape, a.dtype) for a in flat] + [
            pltpu.SemaphoreType.DMA((4 * count,)), pltpu.SemaphoreType.DMA((4 * count,))],
        compiler_params=pltpu.CompilerParams(vmem_limit_bytes=64_000_000),
    )(*flat)
    return [out.reshape(a.shape) for out, a in zip(outs, arrays)]


def solution(mesh):
    def device_fn(x_acts, expert_ids, gate_wts, w_in, w_up, w_out, d_out):
        ids_t = jnp.swapaxes(expert_ids[:, 0], 1, 2)
        gates_t = jnp.swapaxes(gate_wts[:, 0], 1, 2)
        c_rows, xb, q_rows, code, tok = run_dispatch(x_acts, d_out, ids_t, gates_t, w_in, w_up, w_out)
        y_dev, dx_dev, dw_in, dw_up, dw_out = run_settle(run_finish(
            code, tok, xb, q_rows, w_in, w_up, w_out, c_rows)[:5])
        return y_dev[None], dx_dev[None], dw_in, dw_up, dw_out

    tok_spec = P(None, 'stage', 'expert', None)
    w_spec = P('stage', 'expert', None, None)
    row_spec = P('stage', 'expert', None)
    return jax.shard_map(device_fn, mesh=mesh,
                         in_specs=(tok_spec, tok_spec, tok_spec, w_spec, w_spec, w_spec, row_spec),
                         out_specs=(row_spec, row_spec, w_spec, w_spec, w_spec), check_vma=False)
```
